32 devices in a mesh: req: 8 (over z, x), seq: 4 (over y, core).
Axes of the slice: x: 2, y: 2, z: 4, core: 2. Of those that a mesh axis runs over, the one named last changes fastest.
Arguments:
- pool_states: float32 [104, 64, 64, 128], P('req', 'seq'), may hold values from -6 to 6
- inner_window: bfloat16 [104, 3, 4096], P('req', None, 'seq'), may hold values from -6 to 6
- state_window: bfloat16 [104, 3, 256], P('req', None, 'seq'), may hold values from -6 to 6
- move_plan: int32 [104, 2], P('req'), may hold values from 0 to 12, as said below
- active_mask: int32 [104], P('req'), may hold values 0 or 1
- inputs_inner: bfloat16 [8, 2048, 4096], P('req', 'seq'), may hold values from -6 to 6
- inputs_state: bfloat16 [8, 2048, 256], P('req', 'seq'), may hold values from -6 to 6
- gate_rows: bfloat16 [8, 2048, 4096], P('req', 'seq'), may hold values from -6 to 6
- step_raw: bfloat16 [8, 2048, 64], P('req', 'seq'), may hold values from -8 to 60
- lengths: int32 [8], P('req'), may hold values from 4 to 2048
- conv_weight: float32 [4, 4352], replicated, may hold values from -3 to 3
- conv_bias: float32 [4352], replicated, may hold values from -3 to 3
- step_bias: float32 [64], replicated, may hold values from -3.3 to -2.7
- decay_log: float32 [64], replicated, may hold values from -10 to 0
- skip_weight: float32 [64], replicated, may hold values from 0.5 to 1.5
- norm_weight: float32 [4096], replicated, may hold values from 0.25 to 1.75
Outputs:
- new_states: float32 [104, 64, 64, 128], P('req', 'seq')
- new_inner_window: bfloat16 [104, 3, 4096], P('req', None, 'seq')
- new_state_window: bfloat16 [104, 3, 256], P('req', None, 'seq')
- mixer_out: bfloat16 [8, 2048, 4096], P('req', 'seq')
The draws below stay inside these ranges and needn't reach their ends.
Inputs may be any that keep to these rules, and one draw needn't show every extreme that they name: `move_plan`: every pair of a destination index along req and a slot 0 .. 12 is named exactly once; the rows of one device name one destination at most 4 times, and some destination exactly 4 times.
All inputs are finite; a program needn't handle non-finite values. No bound on the sum of `active_mask` on one device may be relied on, other than what follows from the above.
Results may differ from the reference program's by a relative error of at most 0.0087.
Values may be sent and summed in bfloat16 or wider, within the bound.
No kernel may reach another device: no remote copies, remote signals or barrier semaphores. Data moves between devices by JAX's collectives and lax.ppermute only.
A program may use at most 192 MiB of HBM per device.

```python
import jax
import jax.numpy as jnp
from jax import lax

HEAD_COUNT = 64
HEAD_DIM = 64
STATE_DIM = 128
KERNEL = 4
BLOCK_LEN = 256
SLOTS_DEV = 13
PREFILLS = 1
INNER_DIM = 4096
CHANNELS = 4352
CAPACITY = 4
PROMPT_SPAN = 2048
PROMPT_TOTAL = 8
POOL_SLOTS = 104


def draw_move_plan(key, part):
    peer_count = POOL_SLOTS // SLOTS_DEV
    sampler_seeds = jax.random.split(jax.random.fold_in(key, 11), 5)
    outer_order = jax.random.permutation(sampler_seeds[0], peer_count)
    inner_order = jax.random.permutation(sampler_seeds[1], peer_count)
    slot_order = jax.random.permutation(sampler_seeds[2], SLOTS_DEV)
    rotation = jax.random.randint(sampler_seeds[3], (), 0, peer_count)
    offsets = ((jnp.arange(SLOTS_DEV) // CAPACITY + rotation) % peer_count)[slot_order]
    devices = jnp.arange(peer_count)
    target_device = outer_order[(inner_order[devices][:, None] + offsets[None, :]) % peer_count]

    def slot_table(table_key):
        return jax.random.permutation(table_key, SLOTS_DEV)
    slot_tables = jax.vmap(slot_table)(jax.random.split(sampler_seeds[4], peer_count))
    target_slot = slot_tables[target_device, jnp.arange(SLOTS_DEV)[None, :]]
    return jnp.stack([target_device, target_slot], axis=-1).reshape(POOL_SLOTS, 2).astype(jnp.int32)


def draw_step_raw(key, part):
    sampler_seeds = jax.random.split(jax.random.fold_in(key, 23), 4)
    blocks = PROMPT_SPAN // BLOCK_LEN
    offset_steps = jax.random.uniform(sampler_seeds[0], (PROMPT_TOTAL, blocks, 1, HEAD_COUNT), minval=-0.8, maxval=0.8)
    offset_steps = jnp.broadcast_to(offset_steps, (PROMPT_TOTAL, blocks, BLOCK_LEN, HEAD_COUNT)).reshape(PROMPT_TOTAL, PROMPT_SPAN, HEAD_COUNT)
    jitter_addend = 0.7 * jax.random.normal(sampler_seeds[1], (PROMPT_TOTAL, PROMPT_SPAN, HEAD_COUNT))
    arrival_tallies = jax.random.uniform(sampler_seeds[2], (PROMPT_TOTAL, PROMPT_SPAN, 1)) < 3.0 / PROMPT_SPAN
    level_entries = jax.random.uniform(sampler_seeds[3], (PROMPT_TOTAL, PROMPT_SPAN, HEAD_COUNT), minval=34.0, maxval=46.0)
    payload_array = offset_steps + jitter_addend + jnp.where(arrival_tallies, level_entries, 0.0)
    return jnp.clip(payload_array, -8.0, 60.0).astype(jnp.float32).astype(jnp.bfloat16)


def draw_decay_log(key, part):
    sampler_seeds = jax.random.split(jax.random.fold_in(key, 37), 3)
    slow_low = jnp.log(0.5 / (0.05 * PROMPT_SPAN))
    slow_high = jnp.log(2.0 / (0.05 * PROMPT_SPAN))
    fast_share = 0.5
    slow_part = jax.random.uniform(sampler_seeds[0], (HEAD_COUNT,), minval=slow_low, maxval=slow_high)
    fast_part = jax.random.uniform(sampler_seeds[1], (HEAD_COUNT,), minval=jnp.log(0.3), maxval=jnp.log(0.67))
    fast_pick = jax.random.uniform(sampler_seeds[2], (HEAD_COUNT,)) < fast_share
    return jnp.where(fast_pick, fast_part, slow_part).astype(jnp.float32)


def plant(drawn, stream_key, low, largest):
    longest = drawn.shape.index(max(drawn.shape))
    spots = []
    for shift in (0, 1):
        where = [jax.random.randint(jax.random.fold_in(stream_key, axis), (), 0, length) for axis, length in enumerate(drawn.shape)]
        where[longest] = (where[longest] + shift) % drawn.shape[longest]
        spots.append(tuple(where))
    return drawn.at[spots[0]].set(low).at[spots[1]].set(largest)


def block_scale(own_key, shape, shards, least, high):
    level = 1.0
    for dim, blocks in shards:
        draws = jax.random.uniform(jax.random.fold_in(jax.random.fold_in(own_key, 6), dim), (blocks,), jnp.float32, least / len(shards), high / len(shards))
        level = level * jnp.repeat(jnp.exp(draws), shape[dim] // blocks).reshape((-1,) + (1,) * (len(shape) - 1 - dim))
    return level


def normal_values(own_key, dims, width, limit, pieces=(), kind=jnp.bfloat16):
    entries = jax.random.normal(own_key, dims, jnp.float32) * width
    if len(pieces) > 0:
        entries = block_scale(own_key, dims, pieces, -0.22, 0.18) * entries
    return jnp.clip(entries, min=-limit, max=limit).astype(kind)


def setup_inputs(seed: int = 0) -> dict:
    streams_of = jax.random.split(jax.random.key(seed), 17)
    pool_states = normal_values(streams_of[0], (POOL_SLOTS, HEAD_COUNT, HEAD_DIM, STATE_DIM), 1.0, 6.0, ((0, 8), (1, 4)), jnp.float32)
    inner_window = normal_values(streams_of[1], (POOL_SLOTS, KERNEL - 1, INNER_DIM), 1.0, 6.0, ((0, 8), (2, 4)))
    state_window = normal_values(streams_of[2], (POOL_SLOTS, KERNEL - 1, 2 * STATE_DIM), 1.0, 6.0, ((0, 8), (2, 4)))
    move_plan = draw_move_plan(jax.random.fold_in(streams_of[16], 71), 0)
    active_mask = plant((jax.random.randint(streams_of[4], (POOL_SLOTS,), 0, 4) < 3).astype(jnp.int32), jax.random.fold_in(streams_of[4], 1), 0, 1)
    inputs_inner = normal_values(streams_of[5], (PROMPT_TOTAL, PROMPT_SPAN, INNER_DIM), 1.0, 6.0, ((0, 8), (1, 4)))
    inputs_state = normal_values(streams_of[6], (PROMPT_TOTAL, PROMPT_SPAN, 2 * STATE_DIM), 1.0, 6.0, ((0, 8), (1, 4)))
    gate_rows = normal_values(streams_of[7], (PROMPT_TOTAL, PROMPT_SPAN, INNER_DIM), 1.0, 6.0, ((0, 8), (1, 4)))
    step_raw = draw_step_raw(jax.random.fold_in(streams_of[16], 71), 0)
    lengths = plant(jax.random.randint(streams_of[9], (PROMPT_TOTAL,), KERNEL, PROMPT_SPAN + 1), jax.random.fold_in(streams_of[9], 1), KERNEL, PROMPT_SPAN).astype(jnp.int32)
    conv_weight = normal_values(streams_of[10], (KERNEL, CHANNELS), KERNEL ** -0.5, 3.0, (), jnp.float32)
    conv_bias = normal_values(streams_of[11], (CHANNELS,), 0.5, 3.0, (), jnp.float32)
    step_bias = jnp.clip(jax.random.uniform(streams_of[12], (HEAD_COUNT,), jnp.float32, -3.3, -2.7), -3.3, -2.7)
    decay_log = draw_decay_log(jax.random.fold_in(streams_of[16], 71), 0)
    skip_weight = jnp.clip(jax.random.uniform(streams_of[14], (HEAD_COUNT,), jnp.float32, 0.5, 1.5), 0.5, 1.5)
    norm_weight = jnp.clip(1.0 + 0.15 * jax.random.normal(streams_of[15], (INNER_DIM,), jnp.float32), 0.25, 1.75)
    return dict(pool_states=pool_states, inner_window=inner_window, state_window=state_window, move_plan=move_plan, active_mask=active_mask, inputs_inner=inputs_inner, inputs_state=inputs_state, gate_rows=gate_rows, step_raw=step_raw, lengths=lengths, conv_weight=conv_weight, conv_bias=conv_bias, step_bias=step_bias, decay_log=decay_log, skip_weight=skip_weight, norm_weight=norm_weight)


EPSILON = 1e-05

def conv_silu(window, new_rows, weight, bias_values):
    extended = jnp.concatenate([window, new_rows], axis=1).astype(jnp.float32)
    length = new_rows.shape[1]
    running = jnp.zeros(new_rows.shape, jnp.float32) + bias_values
    for offset in range(weight.shape[0]):
        running = running + weight[offset] * extended[:, offset:offset + length]
    return jax.nn.silu(running).astype(jnp.bfloat16)

def block_local(value_rows, write_rows, read_rows, step_rows, decay_rates):
    log_decay = step_rows * decay_rates
    running_log = jnp.cumsum(log_decay, axis=0)
    scores = jnp.dot(read_rows, write_rows.T, preferred_element_type=jnp.float32)
    log_heads = running_log.T
    log_gaps = log_heads[:, :, None] - log_heads[:, None, :]
    positions = jnp.arange(running_log.shape[0])
    causal = positions[:, None] >= positions[None, :]
    decays = jnp.where(causal, jnp.exp(jnp.where(causal, log_gaps, 0.0)), 0.0)
    weights = (scores[None] * decays * step_rows.T[:, None, :]).astype(jnp.bfloat16)
    intra_part = jnp.einsum('hts,shp->thp', weights.astype(jnp.float32), value_rows.astype(jnp.float32))
    to_end = jnp.exp(running_log[-1:] - running_log) * step_rows
    scaled = (to_end[:, :, None] * value_rows.astype(jnp.float32)).astype(jnp.bfloat16)
    block_state = jnp.einsum('shp,sn->hpn', scaled.astype(jnp.float32), write_rows.astype(jnp.float32))
    return (intra_part, block_state, running_log)

def gated_norm(payload_array, gate_part, norm_weight):
    gated_rows = payload_array.astype(jnp.float32) * jax.nn.silu(gate_part.astype(jnp.float32))
    norm_scale = lax.rsqrt(lax.optimization_barrier(jnp.mean(gated_rows * gated_rows, axis=-1, keepdims=True)) + EPSILON)
    return (gated_rows * norm_scale * norm_weight).astype(jnp.bfloat16)

def reference(pool_states, inner_window, state_window, move_plan, active_mask, inputs_inner, inputs_state, gate_rows, step_raw, lengths, conv_weight, conv_bias, step_bias, decay_log, skip_weight, norm_weight):
    keep_flag = active_mask.astype(jnp.float32)
    targets = (move_plan[:, 0] * SLOTS_DEV + move_plan[:, 1]).astype(jnp.int32)
    moved_states = jnp.zeros_like(pool_states).at[targets].set(pool_states * keep_flag[:, None, None, None])
    moved_inner = jnp.zeros_like(inner_window).at[targets].set((inner_window.astype(jnp.float32) * keep_flag[:, None, None]).astype(jnp.bfloat16))
    moved_outer = jnp.zeros_like(state_window).at[targets].set((state_window.astype(jnp.float32) * keep_flag[:, None, None]).astype(jnp.bfloat16))
    sequence_index = jnp.arange(PROMPT_TOTAL).astype(jnp.int32)
    slot_index = (sequence_index // PREFILLS * SLOTS_DEV + sequence_index % PREFILLS).astype(jnp.int32)
    decay_rates = -jnp.exp(decay_log)
    block_count = PROMPT_SPAN // BLOCK_LEN

    def split_blocks(source):
        return source.reshape((block_count, BLOCK_LEN) + source.shape[1:])

    def one_block(members):
        return block_local(members[0], members[1], members[2], members[3], decay_rates)

    def advance(carried, members):
        block_state, running_log, read_block = members
        inter_part = jnp.einsum('qn,hpn->qhp', read_block.astype(jnp.float32), carried, precision=lax.Precision.HIGHEST) * jnp.exp(running_log)[:, :, None]
        updated = jnp.exp(running_log[-1])[:, None, None] * carried + block_state
        return (updated, inter_part)

    def prefill_one(members):
        initial, head_inner, head_outer, inner_rows, outer_rows, gate_part, step_part, length_one = members
        raw_rows = jnp.concatenate([inner_rows, outer_rows], axis=1)
        window = jnp.concatenate([head_inner, head_outer], axis=1)
        mixed_rows = conv_silu(window[None], raw_rows[None], conv_weight, conv_bias)[0]
        value_rows = mixed_rows[:, :INNER_DIM].reshape(PROMPT_SPAN, HEAD_COUNT, HEAD_DIM)
        write_rows = mixed_rows[:, INNER_DIM:INNER_DIM + STATE_DIM]
        read_rows = mixed_rows[:, INNER_DIM + STATE_DIM:]
        valid_rows = (jnp.arange(PROMPT_SPAN).astype(jnp.int32) < length_one).astype(jnp.float32)
        step_sizes = jax.nn.softplus(step_part.astype(jnp.float32) + step_bias) * valid_rows[:, None]
        intra_part, block_states, running_logs = lax.map(one_block, (split_blocks(value_rows), split_blocks(write_rows), split_blocks(read_rows), split_blocks(step_sizes)))
        final_state, inter_parts = lax.scan(advance, initial, (block_states, running_logs, split_blocks(read_rows)))
        combined = (intra_part + inter_parts).reshape(PROMPT_SPAN, HEAD_COUNT, HEAD_DIM) + skip_weight[:, None] * value_rows.astype(jnp.float32)
        y_rows = (combined * valid_rows[:, None, None]).astype(jnp.bfloat16).reshape(PROMPT_SPAN, INNER_DIM)
        mixer_rows = gated_norm(y_rows, gate_part, norm_weight)
        window_pos = (length_one - (KERNEL - 1) + jnp.arange(KERNEL - 1)).astype(jnp.int32)
        last_window = jnp.take(raw_rows, window_pos, axis=0)
        return (final_state, last_window, mixer_rows)
    final_states, last_windows, mixer_out = lax.map(prefill_one, (moved_states[slot_index], moved_inner[slot_index], moved_outer[slot_index], inputs_inner, inputs_state, gate_rows, step_raw, lengths))
    new_states = moved_states.at[slot_index].set(final_states)
    new_inner = moved_inner.at[slot_index].set(last_windows[:, :, :INNER_DIM])
    new_outer = moved_outer.at[slot_index].set(last_windows[:, :, INNER_DIM:])
    return (new_states, new_inner, new_outer, mixer_out)
```

```python
import math

import jax
import jax.numpy as jnp
from jax import lax
from jax.experimental import pallas as pl
from jax.experimental.pallas import tpu as pltpu
from jax.sharding import PartitionSpec as P


HEAD_DIM = 64
STATE_DIM = 128
KERNEL = 4
BLOCK_LEN = 256
GROUP = 8
HALF = BLOCK_LEN // 2
GROUP_DIM = GROUP * HEAD_DIM
PAIR_DIM = 2 * HEAD_DIM
LANES = 128
TILE = 128
EPSILON = 1e-05
LOG2E = math.log2(math.e)
F32 = jnp.float32
BF16 = jnp.bfloat16


def dot(a, b, dims=((1,), (0,)), precision=None):
    return lax.dot_general(a, b, (dims, ((), ())), precision=precision, preferred_element_type=F32)


def silu(v):
    return v / (1.0 + jnp.exp(-v))


def conv_silu(tail, rows, weight, bias_row):
    extended = jnp.concatenate([tail, rows.astype(F32)], axis=0)
    count = rows.shape[0]
    start = tail.shape[0] - KERNEL + 1
    running = bias_row + weight[0:1] * extended[start : start + count]
    for k in range(1, KERNEL):
        running = running + weight[k : k + 1] * extended[start + k : start + k + count]
    return silu(running)


def pair_of(columns, i, low):
    return jnp.where(low, columns[:, 2 * i : 2 * i + 1], columns[:, 2 * i + 1 : 2 * i + 2])


def block_kernel(
    chain_ref,
    tail_ref,
    prev_ref,
    rows_ref,
    state_tail_ref,
    state_prev_ref,
    state_rows_ref,
    step_ref,
    rate_ref,
    weight_ref,
    bias_ref,
    state_weight_ref,
    state_bias_ref,
    skip_ref,
    part_ref,
    end_ref,
    read_ref,
    decay_ref,
    scores_scr,
    cum_scr,
    cum_t_scr,
    to_end_scr,
    decay_scr,
    write_t_scr,
    offset_scr,
    carry_scr,
):
    block = pl.program_id(0)
    group = pl.program_id(1)
    first = block == 0

    @pl.when(group == 0)
    def _():
        state_tail = jnp.where(first, state_tail_ref[...], state_prev_ref[8:16, :].astype(F32))
        mixed = conv_silu(state_tail, state_rows_ref[...], state_weight_ref[...], state_bias_ref[...])
        write = mixed[:, :STATE_DIM]
        read = mixed[:, STATE_DIM:].astype(BF16)
        read_ref[...] = read
        write_b = write.astype(BF16)
        scores_scr[...] = dot(read, write_b, ((1,), (1,)))
        write_t_scr[...] = write_b.astype(F32).T.astype(BF16)
        row = lax.broadcasted_iota(jnp.int32, (BLOCK_LEN, BLOCK_LEN), 0)
        col = lax.broadcasted_iota(jnp.int32, (BLOCK_LEN, BLOCK_LEN), 1)
        triangle = (row >= col).astype(F32)
        step = step_ref[...]
        cum = dot(triangle, step * rate_ref[...], precision=lax.Precision.HIGHEST)
        cum_scr[...] = cum
        cum_t_scr[...] = cum.T
        last = cum[BLOCK_LEN - 1 :, :]
        to_end_scr[...] = jnp.exp2(last - cum) * step
        decay_scr[...] = jnp.exp2(cum)
        offset = jnp.where(first, 0.0, offset_scr[0:1, :])
        decay_ref[...] = jnp.exp2(offset + cum)
        offset_scr[0:1, :] = offset + last

    shift = lax.rem(LANES - group * GROUP, LANES)
    cum = pltpu.roll(cum_scr[...], shift, 1)
    step = pltpu.roll(step_ref[...], shift, 1)
    to_end = pltpu.roll(to_end_scr[...], shift, 1)
    decay = pltpu.roll(decay_scr[...], shift, 1)
    cum_t = cum_t_scr[pl.ds(pl.multiple_of(group * GROUP, GROUP), GROUP), :]
    read = read_ref[...]
    write_t = write_t_scr[...]
    carry = jnp.where(first, 0.0, carry_scr[group])
    carry_b = carry.astype(BF16)
    low = lax.broadcasted_iota(jnp.int32, (1, PAIR_DIM), 1) < HEAD_DIM
    causal = lax.broadcasted_iota(jnp.int32, (HALF, HALF), 0) >= lax.broadcasted_iota(
        jnp.int32, (HALF, HALF), 1
    )
    scores_top = scores_scr[0:HALF, 0:HALF]
    scores_left = scores_scr[HALF:, 0:HALF]
    scores_right = scores_scr[HALF:, HALF:]

    def head_weights(i):
        later = cum[:, i : i + 1]
        earlier = cum_t[i : i + 1, :]
        gap_top = jnp.where(causal, later[:HALF] - earlier[:, :HALF], -1e30)
        gap_left = later[HALF:] - earlier[:, :HALF]
        gap_right = jnp.where(causal, later[HALF:] - earlier[:, HALF:], -1e30)
        top = (scores_top * jnp.exp2(gap_top)).astype(BF16)
        left = (scores_left * jnp.exp2(gap_left)).astype(BF16)
        right = (scores_right * jnp.exp2(gap_right)).astype(BF16)
        return top, jnp.concatenate([left, right], axis=1)

    for i in range(GROUP // 2):
        span = slice(i * PAIR_DIM, (i + 1) * PAIR_DIM)
        tail = jnp.where(first, tail_ref[:, span], prev_ref[8:16, span].astype(F32))
        mixed = conv_silu(tail, rows_ref[:, span], weight_ref[:, span], bias_ref[:, span])
        value = mixed.astype(BF16).astype(F32)
        stepped = (pair_of(step, i, low) * value).astype(BF16)
        scaled = (pair_of(to_end, i, low) * value).astype(BF16)
        stepped_low = jnp.where(low, stepped, jnp.zeros_like(stepped))
        stepped_high = jnp.where(low, jnp.zeros_like(stepped), stepped)
        top_0, bottom_0 = head_weights(2 * i)
        top_1, bottom_1 = head_weights(2 * i + 1)
        intra_top = dot(top_0, stepped_low[:HALF]) + dot(top_1, stepped_high[:HALF])
        intra_bottom = dot(bottom_0, stepped_low) + dot(bottom_1, stepped_high)
        inter = dot(read, carry_b[:, span]) * pair_of(decay, i, low)
        direct = inter + skip_ref[:, span] * value
        part_ref[0:HALF, span] = intra_top + direct[:HALF]
        part_ref[HALF:, span] = intra_bottom + direct[HALF:]
        kept = pair_of(decay[BLOCK_LEN - 1 :, :], i, low) * carry[:, span]
        ending = kept + dot(write_t, scaled)
        carry_scr[group, :, span] = ending
        end_ref[0, :, span] = ending.astype(BF16)


def block_parts(chain, tail, rows, state_rows, step, rate, weight, bias_row, skip_row, ends):
    length = rows.shape[0]
    channels = rows.shape[1]
    blocks = length // BLOCK_LEN
    groups = channels // GROUP_DIM
    end_groups = groups // ends
    state_dim = state_rows.shape[1]
    state_at = channels // state_dim
    per_block = BLOCK_LEN // 16

    def before(b):
        return jnp.maximum(b * per_block - 1, 0)

    def end_at(b, g, chain):
        return lax.rem(g // end_groups - chain[0] + ends, ends), 0, lax.rem(g, end_groups)

    return pl.pallas_call(
        block_kernel,
        grid_spec=pltpu.PrefetchScalarGridSpec(
        num_scalar_prefetch=1,
        grid=(blocks, groups),
        in_specs=[
            pl.BlockSpec((8, GROUP_DIM), lambda b, g, c: (0, g)),
            pl.BlockSpec((16, GROUP_DIM), lambda b, g, c: (before(b), g)),
            pl.BlockSpec((BLOCK_LEN, GROUP_DIM), lambda b, g, c: (b, g)),
            pl.BlockSpec((8, state_dim), lambda b, g, c: (0, state_at)),
            pl.BlockSpec((16, state_dim), lambda b, g, c: (before(b), 0)),
            pl.BlockSpec((BLOCK_LEN, state_dim), lambda b, g, c: (b, 0)),
            pl.BlockSpec((BLOCK_LEN, LANES), lambda b, g, c: (b, 0)),
            pl.BlockSpec((1, LANES), lambda b, g, c: (0, 0)),
            pl.BlockSpec((KERNEL, GROUP_DIM), lambda b, g, c: (0, g)),
            pl.BlockSpec((1, GROUP_DIM), lambda b, g, c: (0, g)),
            pl.BlockSpec((KERNEL, state_dim), lambda b, g, c: (0, state_at)),
            pl.BlockSpec((1, state_dim), lambda b, g, c: (0, state_at)),
            pl.BlockSpec((1, GROUP_DIM), lambda b, g, c: (0, g)),
        ],
        out_specs=[
            pl.BlockSpec((BLOCK_LEN, GROUP_DIM), lambda b, g, c: (b, g)),
            pl.BlockSpec((1, STATE_DIM, GROUP_DIM), end_at),
            pl.BlockSpec((BLOCK_LEN, STATE_DIM), lambda b, g, c: (b, 0)),
            pl.BlockSpec((BLOCK_LEN, LANES), lambda b, g, c: (b, 0)),
        ],
        scratch_shapes=[
            pltpu.VMEM((BLOCK_LEN, BLOCK_LEN), F32),
            pltpu.VMEM((BLOCK_LEN, LANES), F32),
            pltpu.VMEM((LANES, BLOCK_LEN), F32),
            pltpu.VMEM((BLOCK_LEN, LANES), F32),
            pltpu.VMEM((BLOCK_LEN, LANES), F32),
            pltpu.VMEM((STATE_DIM, BLOCK_LEN), BF16),
            pltpu.VMEM((8, LANES), F32),
            pltpu.VMEM((groups, STATE_DIM, GROUP_DIM), F32),
        ],
        ),
        out_shape=[
            jax.ShapeDtypeStruct((length, channels), F32),
            jax.ShapeDtypeStruct((ends, STATE_DIM, channels // ends), BF16),
            jax.ShapeDtypeStruct((length, STATE_DIM), BF16),
            jax.ShapeDtypeStruct((length, LANES), F32),
        ],
        compiler_params=pltpu.CompilerParams(dimension_semantics=("arbitrary", "arbitrary")),
        cost_estimate=pl.CostEstimate(
            flops=6_000_000_000, bytes_accessed=20_000_000, transcendentals=10_000_000
        ),
        name="block_parts",
    )(
        chain,
        tail,
        rows,
        rows,
        tail,
        state_rows,
        state_rows,
        step,
        rate,
        weight,
        bias_row,
        weight,
        bias_row,
        skip_row,
    )


def finish_kernel(
    place_ref, part_ref, gate_ref, read_ref, decay_ref, state_ref, norm_ref, out_ref, gated_scr
):
    tile = pl.program_id(0)
    chunks, _, width = state_ref.shape
    positions = (
        place_ref[0] + tile * TILE + lax.broadcasted_iota(jnp.int32, (TILE, PAIR_DIM), 0)
    )
    valid = (positions < place_ref[1]).astype(F32)
    low = lax.broadcasted_iota(jnp.int32, (1, PAIR_DIM), 1) < HEAD_DIM
    read = read_ref[...]
    decay = decay_ref[...]
    total = jnp.zeros((TILE, PAIR_DIM), F32)
    for chunk in range(chunks):
        from_chunk = lax.rem(place_ref[2] - chunk + chunks, chunks)
        for i in range(width // PAIR_DIM):
            pair = chunk * (width // PAIR_DIM) + i
            span = slice(pair * PAIR_DIM, (pair + 1) * PAIR_DIM)
            inter = dot(read, state_ref[from_chunk, :, i * PAIR_DIM : (i + 1) * PAIR_DIM])
            y = part_ref[:, span] + inter * pair_of(decay, pair, low)
            y = (y * valid).astype(BF16).astype(F32)
            gated = y * silu(gate_ref[:, span].astype(F32))
            gated_scr[:, span] = gated
            total = total + gated * gated
    channels = chunks * width
    mean = jnp.sum(total, axis=1, keepdims=True) * (1.0 / channels)
    scale = lax.rsqrt(mean + EPSILON)
    for pair in range(channels // PAIR_DIM):
        span = slice(pair * PAIR_DIM, (pair + 1) * PAIR_DIM)
        out_ref[:, span] = (gated_scr[:, span] * scale * norm_ref[:, span]).astype(BF16)


def finish(place, part, gate, read, decay, states, norm_row):
    length, channels = part.shape
    return pl.pallas_call(
        finish_kernel,
        grid=(length // TILE,),
        in_specs=[
            pl.BlockSpec(memory_space=pltpu.SMEM),
            pl.BlockSpec((TILE, channels), lambda t: (t, 0)),
            pl.BlockSpec((TILE, channels), lambda t: (t, 0)),
            pl.BlockSpec((TILE, STATE_DIM), lambda t: (t, 0)),
            pl.BlockSpec((TILE, LANES), lambda t: (t, 0)),
            pl.BlockSpec(states.shape, lambda t: (0, 0, 0)),
            pl.BlockSpec((1, channels), lambda t: (0, 0)),
        ],
        out_specs=pl.BlockSpec((TILE, channels), lambda t: (t, 0)),
        out_shape=jax.ShapeDtypeStruct((length, channels), BF16),
        scratch_shapes=[pltpu.VMEM((TILE, channels), F32)],
        compiler_params=pltpu.CompilerParams(dimension_semantics=("arbitrary",)),
        cost_estimate=pl.CostEstimate(
            flops=3_000_000_000, bytes_accessed=16_000_000, transcendentals=4_000_000
        ),
        name="finish",
    )(place, part, gate, read, decay, states, norm_row)


def pack_kernel(keep_ref, state_ref, out_ref):
    keep = keep_ref[pl.program_id(0)].astype(F32)
    out_ref[:, 0] = (state_ref[0] * keep).astype(BF16)


def pack(keep, states):
    slots, peers, piece, width = states.shape
    return pl.pallas_call(
        pack_kernel,
        grid=(slots,),
        in_specs=[
            pl.BlockSpec(memory_space=pltpu.SMEM),
            pl.BlockSpec((1, peers, piece, width), lambda t: (t, 0, 0, 0)),
        ],
        out_specs=pl.BlockSpec((peers, 1, piece, width), lambda t: (0, t, 0, 0)),
        out_shape=jax.ShapeDtypeStruct((peers, slots, piece, width), BF16),
        compiler_params=pltpu.CompilerParams(dimension_semantics=("arbitrary",)),
        name="pack",
    )(keep, states)


def unpack_kernel(final_ref, pieces_ref, out_ref):
    slot = pl.program_id(0)
    peers, piece = out_ref.shape[1:3]

    @pl.when(slot == 0)
    def _():
        for p in range(peers):
            out_ref[0, p] = final_ref[:, p * piece : (p + 1) * piece].T

    @pl.when(slot > 0)
    def _():
        out_ref[0] = pieces_ref[:, 0].astype(F32)


def unpack(final, pieces):
    peers, others, piece, width = pieces.shape
    slots = others + 1
    return pl.pallas_call(
        unpack_kernel,
        grid=(slots,),
        in_specs=[
            pl.BlockSpec(final.shape, lambda t: (0, 0)),
            pl.BlockSpec((peers, 1, piece, width), lambda t: (0, jnp.maximum(t - 1, 0), 0, 0)),
        ],
        out_specs=pl.BlockSpec((1, peers, piece, width), lambda t: (t, 0, 0, 0)),
        out_shape=jax.ShapeDtypeStruct((slots, peers, piece, width), F32),
        compiler_params=pltpu.CompilerParams(dimension_semantics=("arbitrary",)),
        name="unpack",
    )(final, pieces)


def combine_kernel(chain_ref, first_ref, ends_ref, decay_ref, entering_ref, final_ref):
    chain = chain_ref[0]
    count = ends_ref.shape[0]
    state = first_ref[...].astype(F32).T
    for k in range(count):
        entering_ref[lax.rem(k - chain + count, count)] = state.astype(BF16)
        end = ends_ref[lax.rem(chain - k + count, count)].astype(F32)
        state = state * decay_ref[k : k + 1, :] + end
    final_ref[...] = state


def combine(chain, first, ends, decay):
    whole = pl.BlockSpec(memory_space=pltpu.VMEM)
    return pl.pallas_call(
        combine_kernel,
        in_specs=[pl.BlockSpec(memory_space=pltpu.SMEM), whole, whole, whole],
        out_shape=[
            jax.ShapeDtypeStruct(ends.shape, BF16),
            jax.ShapeDtypeStruct(ends.shape[1:], F32),
        ],
        name="combine",
    )(chain, first, ends, decay)


def exchange(value, axis):
    return lax.all_to_all(value, axis, split_axis=0, concat_axis=0, tiled=True)


def rotate(values, axis):
    count = lax.axis_size(axis)
    got = [values[0]]
    for hop in range(1, count):
        pairs = [(source, (source + hop) % count) for source in range(count)]
        got.append(lax.ppermute(values[hop], axis, pairs))
    return jnp.stack(got)


def rows_at(source, indices):
    return source.at[indices].get(mode="promise_in_bounds")


def device_body(
    pool_states,
    inner_window,
    state_window,
    move_plan,
    active_mask,
    inputs_inner,
    inputs_state,
    gate_rows,
    step_raw,
    lengths,
    conv_weight,
    conv_bias,
    step_bias,
    decay_log,
    skip_weight,
    norm_weight,
):
    peers = lax.axis_size("req")
    own_peer = lax.axis_index("req")
    chain_size = lax.axis_size("seq")
    chain_index = lax.axis_index("seq")
    slots, local_heads = pool_states.shape[:2]
    piece = local_heads * HEAD_DIM // peers
    taps = KERNEL - 1
    keep_flag = active_mask.astype(F32)

    pieces = pack(active_mask, pool_states.reshape(slots, peers, piece, STATE_DIM))
    spread = exchange(pieces, "req").reshape(peers * slots, piece, STATE_DIM)

    inner_local = inner_window.shape[2]
    outer_local = state_window.shape[2]
    own_windows = jnp.concatenate([inner_window, state_window], axis=2).reshape(slots, -1)
    own_windows = (own_windows.astype(F32) * keep_flag[:, None]).astype(BF16)
    width = own_windows.shape[1]
    padding = jnp.zeros((slots, -(width + 2) % LANES), BF16)
    packed = jnp.concatenate([own_windows, move_plan.astype(BF16), padding], axis=1)
    every = lax.all_gather(packed, "req", axis=0, tiled=True)
    every_plan = every[:, width : width + 2].astype(F32).astype(jnp.int32)
    targets = every_plan[:, 0] * slots + every_plan[:, 1]
    order = jnp.arange(peers * slots, dtype=jnp.int32)
    sources = jnp.sum(jnp.where(targets[None, :] == order[:, None], order[None, :], 0), axis=1)
    own_sources = lax.dynamic_slice_in_dim(sources, own_peer * slots, slots)
    moved_windows = rows_at(every, own_sources)[:, :width].reshape(slots, taps, -1)

    rows = inputs_inner[0]
    state_rows = inputs_state[0]
    local_length = rows.shape[0]
    inner_dim = rows.shape[1]
    start = chain_index * local_length
    length = lengths[0]
    window_pos = length - taps + jnp.arange(taps, dtype=jnp.int32) - start
    inside = (window_pos >= 0) & (window_pos < local_length)
    safe_pos = jnp.clip(window_pos, 0, local_length - 1)
    ends = jnp.concatenate(
        [rows[local_length - taps :], state_rows[local_length - taps :]], axis=1
    )
    kept_here = jnp.concatenate([rows_at(rows, safe_pos), rows_at(state_rows, safe_pos)], axis=1)
    kept_here = jnp.where(inside[:, None], kept_here, jnp.zeros_like(kept_here))
    channels = ends.shape[1]
    window_local = inner_local + outer_local
    heads = decay_log.shape[0]
    head_pad = LANES - heads
    rate = -LOG2E * jnp.exp(decay_log)
    positions = start + jnp.arange(local_length, dtype=jnp.int32)
    valid_rows = (positions < length).astype(F32)
    step = jax.nn.softplus(step_raw[0].astype(F32) + step_bias) * valid_rows[:, None]
    device_log = jnp.sum(step * rate, axis=0)
    log_high = lax.reduce_precision(device_log, 8, 7)
    log_middle = lax.reduce_precision(device_log - log_high, 8, 7)
    log_low = lax.reduce_precision(device_log - log_high - log_middle, 8, 7)
    log_parts = jnp.stack([log_high, log_middle, log_low]).astype(BF16)
    shared = lax.all_gather(
        jnp.concatenate([log_parts, moved_windows[0], ends, kept_here], axis=1), "seq", axis=0
    )
    every_log = jnp.sum(shared[:, :, :heads].astype(F32), axis=1)
    shared = shared[:, :, heads:]
    own_log = lax.dynamic_slice_in_dim(every_log, chain_index * local_heads, local_heads, 1)
    own_decay = jnp.repeat(jnp.exp2(own_log), HEAD_DIM, axis=1)
    first_window = jnp.concatenate(
        [
            shared[:, :, :inner_local].transpose(1, 0, 2).reshape(taps, -1),
            shared[:, :, inner_local:window_local].transpose(1, 0, 2).reshape(taps, -1),
        ],
        axis=1,
    )
    earlier_rows = lax.dynamic_index_in_dim(
        shared[:, :, window_local : window_local + channels],
        jnp.maximum(chain_index - 1, 0),
        0,
        keepdims=False,
    )
    tail = jnp.where(chain_index == 0, first_window, earlier_rows).astype(F32)
    tail = jnp.concatenate([jnp.zeros((8 - taps, channels), F32), tail], axis=0)
    kept = jnp.sum(shared[:, :, window_local + channels :].astype(F32), axis=0).astype(BF16)
    kept_inner = lax.dynamic_slice_in_dim(kept, chain_index * inner_local, inner_local, 1)
    kept_outer = lax.dynamic_slice_in_dim(
        kept, inner_dim + chain_index * outer_local, outer_local, 1
    )

    chain = chain_index.astype(jnp.int32)[None]
    part, local_end, read_rows, decay = block_parts(
        chain,
        tail,
        rows,
        state_rows,
        jnp.pad(step, ((0, 0), (0, head_pad))),
        jnp.pad(rate, (0, head_pad))[None],
        conv_weight,
        conv_bias[None],
        jnp.repeat(skip_weight, HEAD_DIM)[None],
        chain_size,
    )
    own_ends = rotate(local_end, "seq")

    order_by_peer = sources.reshape(peers, slots)
    peer_order = jnp.arange(peers, dtype=jnp.int32)
    first_sources = rows_at(order_by_peer[:, 0], lax.rem(own_peer + peer_order, peers))
    first_pieces = rotate(rows_at(spread, first_sources), "req")
    first_pieces = rows_at(first_pieces, lax.rem(own_peer + peers - peer_order, peers))
    rest = rows_at(spread, order_by_peer[:, 1:].reshape(-1)).reshape(
        peers, slots - 1, piece, STATE_DIM
    )
    rest_pieces = exchange(rest, "req")

    entering, final = combine(
        chain, first_pieces.reshape(local_heads * HEAD_DIM, STATE_DIM), own_ends, own_decay
    )
    incoming = rotate(entering, "seq")

    place = jnp.stack([start, length, chain_index]).astype(jnp.int32)
    mixer_out = finish(
        place, part, gate_rows[0], read_rows, decay, incoming, norm_weight[None]
    )
    new_states = unpack(final, rest_pieces).reshape(pool_states.shape)
    new_inner = jnp.concatenate(
        [kept_inner[None], moved_windows[1:, :, :inner_local]], axis=0
    )
    new_outer = jnp.concatenate(
        [kept_outer[None], moved_windows[1:, :, inner_local:]], axis=0
    )
    return (new_states, new_inner, new_outer, mixer_out[None])


def solution(mesh):
    return jax.shard_map(
        device_body,
        mesh=mesh,
        in_specs=(
            P("req", "seq", None, None),
            P("req", None, "seq"),
            P("req", None, "seq"),
            P("req", None),
            P("req"),
            P("req", "seq", None),
            P("req", "seq", None),
            P("req", "seq", None),
            P("req", "seq", None),
            P("req"),
            P(),
            P(),
            P(),
            P(),
            P(),
            P(),
        ),
        out_specs=(
            P("req", "seq", None, None),
            P("req", None, "seq"),
            P("req", None, "seq"),
            P("req", "seq", None),
        ),
        check_vma=False,
    )
```

```python
import math

import jax
import jax.numpy as jnp
from jax import lax
from jax.experimental import pallas as pl
from jax.experimental.pallas import tpu as pltpu
from jax.sharding import PartitionSpec as P


HEAD_DIM = 64
STATE_DIM = 128
KERNEL = 4
BLOCK_LEN = 256
GROUP = 8
HALF = BLOCK_LEN // 2
GROUP_DIM = GROUP * HEAD_DIM
PAIR_DIM = 2 * HEAD_DIM
LANES = 128
TILE = 128
SLOT_TILE = 4
PEER_TILE = 2
EPSILON = 1e-05
LOG2E = math.log2(math.e)
F32 = jnp.float32
BF16 = jnp.bfloat16


def dot(a, b, dims=((1,), (0,)), precision=None):
    return lax.dot_general(a, b, (dims, ((), ())), precision=precision, preferred_element_type=F32)


def silu(v):
    return v / (1.0 + jnp.exp(-v))


def conv_silu(tail, rows, weight, bias_row):
    extended = jnp.concatenate([tail, rows.astype(F32)], axis=0)
    count = rows.shape[0]
    start = tail.shape[0] - KERNEL + 1
    running = bias_row + weight[0:1] * extended[start : start + count]
    for k in range(1, KERNEL):
        running = running + weight[k : k + 1] * extended[start + k : start + k + count]
    return silu(running)


def pair_of(columns, i, low):
    return jnp.where(low, columns[:, 2 * i : 2 * i + 1], columns[:, 2 * i + 1 : 2 * i + 2])


def block_kernel(
    chain_ref,
    tail_ref,
    prev_ref,
    rows_ref,
    state_tail_ref,
    state_prev_ref,
    state_rows_ref,
    step_ref,
    rate_ref,
    weight_ref,
    bias_ref,
    state_weight_ref,
    state_bias_ref,
    skip_ref,
    part_ref,
    end_ref,
    read_ref,
    decay_ref,
    scores_scr,
    cum_scr,
    cum_t_scr,
    to_end_scr,
    decay_scr,
    write_t_scr,
    offset_scr,
    carry_scr,
):
    block = pl.program_id(0)
    group = pl.program_id(1)
    first = block == 0

    @pl.when(group == 0)
    def _():
        state_tail = jnp.where(first, state_tail_ref[...], state_prev_ref[8:16, :].astype(F32))
        mixed = conv_silu(state_tail, state_rows_ref[...], state_weight_ref[...], state_bias_ref[...])
        write = mixed[:, :STATE_DIM]
        read = mixed[:, STATE_DIM:].astype(BF16)
        read_ref[...] = read
        write_b = write.astype(BF16)
        scores_scr[...] = dot(read, write_b, ((1,), (1,)))
        write_t_scr[...] = write_b.astype(F32).T.astype(BF16)
        row = lax.broadcasted_iota(jnp.int32, (BLOCK_LEN, BLOCK_LEN), 0)
        col = lax.broadcasted_iota(jnp.int32, (BLOCK_LEN, BLOCK_LEN), 1)
        triangle = (row >= col).astype(F32)
        step = step_ref[...]
        cum = dot(triangle, step * rate_ref[...], precision=lax.Precision.HIGHEST)
        cum_scr[...] = cum
        cum_t_scr[...] = cum.T
        last = cum[BLOCK_LEN - 1 :, :]
        to_end_scr[...] = jnp.exp2(last - cum) * step
        decay_scr[...] = jnp.exp2(cum)
        offset = jnp.where(first, 0.0, offset_scr[0:1, :])
        decay_ref[...] = jnp.exp2(offset + cum)
        offset_scr[0:1, :] = offset + last

    shift = lax.rem(LANES - group * GROUP, LANES)
    cum = pltpu.roll(cum_scr[...], shift, 1)
    step = pltpu.roll(step_ref[...], shift, 1)
    to_end = pltpu.roll(to_end_scr[...], shift, 1)
    decay = pltpu.roll(decay_scr[...], shift, 1)
    cum_t = cum_t_scr[pl.ds(pl.multiple_of(group * GROUP, GROUP), GROUP), :]
    read = read_ref[...]
    write_t = write_t_scr[...]
    carry = jnp.where(first, 0.0, carry_scr[group])
    carry_b = carry.astype(BF16)
    low = lax.broadcasted_iota(jnp.int32, (1, PAIR_DIM), 1) < HEAD_DIM
    causal = lax.broadcasted_iota(jnp.int32, (HALF, HALF), 0) >= lax.broadcasted_iota(
        jnp.int32, (HALF, HALF), 1
    )
    scores_top = scores_scr[0:HALF, 0:HALF]
    scores_left = scores_scr[HALF:, 0:HALF]
    scores_right = scores_scr[HALF:, HALF:]

    def head_weights(i):
        later = cum[:, i : i + 1]
        earlier = cum_t[i : i + 1, :]
        gap_top = jnp.where(causal, later[:HALF] - earlier[:, :HALF], -1e30)
        gap_left = later[HALF:] - earlier[:, :HALF]
        gap_right = jnp.where(causal, later[HALF:] - earlier[:, HALF:], -1e30)
        top = (scores_top * jnp.exp2(gap_top)).astype(BF16)
        left = (scores_left * jnp.exp2(gap_left)).astype(BF16)
        right = (scores_right * jnp.exp2(gap_right)).astype(BF16)
        return top, jnp.concatenate([left, right], axis=1)

    for i in range(GROUP // 2):
        span = slice(i * PAIR_DIM, (i + 1) * PAIR_DIM)
        tail = jnp.where(first, tail_ref[:, span], prev_ref[8:16, span].astype(F32))
        mixed = conv_silu(tail, rows_ref[:, span], weight_ref[:, span], bias_ref[:, span])
        value = mixed.astype(BF16).astype(F32)
        stepped = (pair_of(step, i, low) * value).astype(BF16)
        scaled = (pair_of(to_end, i, low) * value).astype(BF16)
        stepped_low = jnp.where(low, stepped, jnp.zeros_like(stepped))
        stepped_high = jnp.where(low, jnp.zeros_like(stepped), stepped)
        top_0, bottom_0 = head_weights(2 * i)
        top_1, bottom_1 = head_weights(2 * i + 1)
        intra_top = dot(top_0, stepped_low[:HALF]) + dot(top_1, stepped_high[:HALF])
        intra_bottom = dot(bottom_0, stepped_low) + dot(bottom_1, stepped_high)
        inter = dot(read, carry_b[:, span]) * pair_of(decay, i, low)
        direct = inter + skip_ref[:, span] * value
        part_ref[0:HALF, span] = intra_top + direct[:HALF]
        part_ref[HALF:, span] = intra_bottom + direct[HALF:]
        kept = pair_of(decay[BLOCK_LEN - 1 :, :], i, low) * carry[:, span]
        ending = kept + dot(write_t, scaled)
        carry_scr[group, :, span] = ending
        end_ref[0, :, span] = ending.astype(BF16)


def block_parts(chain, tail, rows, state_rows, step, rate, weight, bias_row, skip_row, ends):
    length = rows.shape[0]
    channels = rows.shape[1]
    blocks = length // BLOCK_LEN
    groups = channels // GROUP_DIM
    end_groups = groups // ends
    state_dim = state_rows.shape[1]
    state_at = channels // state_dim
    per_block = BLOCK_LEN // 16

    def before(b):
        return jnp.maximum(b * per_block - 1, 0)

    def end_at(b, g, chain):
        return lax.rem(g // end_groups - chain[0] + ends, ends), 0, lax.rem(g, end_groups)

    return pl.pallas_call(
        block_kernel,
        grid_spec=pltpu.PrefetchScalarGridSpec(
        num_scalar_prefetch=1,
        grid=(blocks, groups),
        in_specs=[
            pl.BlockSpec((8, GROUP_DIM), lambda b, g, c: (0, g)),
            pl.BlockSpec((16, GROUP_DIM), lambda b, g, c: (before(b), g)),
            pl.BlockSpec((BLOCK_LEN, GROUP_DIM), lambda b, g, c: (b, g)),
            pl.BlockSpec((8, state_dim), lambda b, g, c: (0, state_at)),
            pl.BlockSpec((16, state_dim), lambda b, g, c: (before(b), 0)),
            pl.BlockSpec((BLOCK_LEN, state_dim), lambda b, g, c: (b, 0)),
            pl.BlockSpec((BLOCK_LEN, LANES), lambda b, g, c: (b, 0)),
            pl.BlockSpec((1, LANES), lambda b, g, c: (0, 0)),
            pl.BlockSpec((KERNEL, GROUP_DIM), lambda b, g, c: (0, g)),
            pl.BlockSpec((1, GROUP_DIM), lambda b, g, c: (0, g)),
            pl.BlockSpec((KERNEL, state_dim), lambda b, g, c: (0, state_at)),
            pl.BlockSpec((1, state_dim), lambda b, g, c: (0, state_at)),
            pl.BlockSpec((1, GROUP_DIM), lambda b, g, c: (0, g)),
        ],
        out_specs=[
            pl.BlockSpec((BLOCK_LEN, GROUP_DIM), lambda b, g, c: (b, g)),
            pl.BlockSpec((1, STATE_DIM, GROUP_DIM), end_at),
            pl.BlockSpec((BLOCK_LEN, STATE_DIM), lambda b, g, c: (b, 0)),
            pl.BlockSpec((BLOCK_LEN, LANES), lambda b, g, c: (b, 0)),
        ],
        scratch_shapes=[
            pltpu.VMEM((BLOCK_LEN, BLOCK_LEN), F32),
            pltpu.VMEM((BLOCK_LEN, LANES), F32),
            pltpu.VMEM((LANES, BLOCK_LEN), F32),
            pltpu.VMEM((BLOCK_LEN, LANES), F32),
            pltpu.VMEM((BLOCK_LEN, LANES), F32),
            pltpu.VMEM((STATE_DIM, BLOCK_LEN), BF16),
            pltpu.VMEM((8, LANES), F32),
            pltpu.VMEM((groups, STATE_DIM, GROUP_DIM), F32),
        ],
        ),
        out_shape=[
            jax.ShapeDtypeStruct((length, channels), F32),
            jax.ShapeDtypeStruct((ends, STATE_DIM, channels // ends), BF16),
            jax.ShapeDtypeStruct((length, STATE_DIM), BF16),
            jax.ShapeDtypeStruct((length, LANES), F32),
        ],
        compiler_params=pltpu.CompilerParams(dimension_semantics=("arbitrary", "arbitrary")),
        cost_estimate=pl.CostEstimate(
            flops=6_000_000_000, bytes_accessed=20_000_000, transcendentals=10_000_000
        ),
        name="block_parts",
    )(
        chain,
        tail,
        rows,
        rows,
        tail,
        state_rows,
        state_rows,
        step,
        rate,
        weight,
        bias_row,
        weight,
        bias_row,
        skip_row,
    )


def finish_kernel(
    place_ref, part_ref, gate_ref, read_ref, decay_ref, norm_ref, *refs
):
    state_refs, out_ref, gated_scr, state_scr = refs[:-3], refs[-3], refs[-2], refs[-1]
    tile = pl.program_id(0)
    chunks, _, width = state_scr.shape

    @pl.when(tile == 0)
    def _():
        for hop in range(chunks):
            state_scr[lax.rem(place_ref[2] - hop + chunks, chunks)] = state_refs[hop][...]

    positions = (
        place_ref[0] + tile * TILE + lax.broadcasted_iota(jnp.int32, (TILE, PAIR_DIM), 0)
    )
    valid = (positions < place_ref[1]).astype(F32)
    low = lax.broadcasted_iota(jnp.int32, (1, PAIR_DIM), 1) < HEAD_DIM
    read = read_ref[...]
    decay = decay_ref[...]
    total = jnp.zeros((TILE, PAIR_DIM), F32)
    for chunk in range(chunks):
        for i in range(width // PAIR_DIM):
            pair = chunk * (width // PAIR_DIM) + i
            span = slice(pair * PAIR_DIM, (pair + 1) * PAIR_DIM)
            inter = dot(read, state_scr[chunk, :, i * PAIR_DIM : (i + 1) * PAIR_DIM])
            y = part_ref[:, span] + inter * pair_of(decay, pair, low)
            y = (y * valid).astype(BF16).astype(F32)
            gated = y * silu(gate_ref[:, span].astype(F32))
            gated_scr[:, span] = gated
            total = total + gated * gated
    channels = chunks * width
    mean = jnp.sum(total, axis=1, keepdims=True) * (1.0 / channels)
    scale = lax.rsqrt(mean + EPSILON)
    for pair in range(channels // PAIR_DIM):
        span = slice(pair * PAIR_DIM, (pair + 1) * PAIR_DIM)
        out_ref[:, span] = (gated_scr[:, span] * scale * norm_ref[:, span]).astype(BF16)


def finish(place, part, gate, read, decay, norm_row, states):
    length, channels = part.shape
    return pl.pallas_call(
        finish_kernel,
        grid=(length // TILE,),
        in_specs=[
            pl.BlockSpec(memory_space=pltpu.SMEM),
            pl.BlockSpec((TILE, channels), lambda t: (t, 0)),
            pl.BlockSpec((TILE, channels), lambda t: (t, 0)),
            pl.BlockSpec((TILE, STATE_DIM), lambda t: (t, 0)),
            pl.BlockSpec((TILE, LANES), lambda t: (t, 0)),
            pl.BlockSpec((1, channels), lambda t: (0, 0)),
        ]
        + [pl.BlockSpec(state.shape, lambda t: (0, 0)) for state in states],
        out_specs=pl.BlockSpec((TILE, channels), lambda t: (t, 0)),
        out_shape=jax.ShapeDtypeStruct((length, channels), BF16),
        scratch_shapes=[
            pltpu.VMEM((TILE, channels), F32),
            pltpu.VMEM((len(states),) + states[0].shape, BF16),
        ],
        compiler_params=pltpu.CompilerParams(dimension_semantics=("arbitrary",)),
        cost_estimate=pl.CostEstimate(
            flops=3_000_000_000, bytes_accessed=16_000_000, transcendentals=4_000_000
        ),
        name="finish",
    )(place, part, gate, read, decay, norm_row, *states)


def pack_kernel(place_ref, state_ref, after_ref, *out_refs):
    first_slot = pl.program_id(0) * SLOT_TILE
    peers = state_ref.shape[1]
    for j in range(SLOT_TILE):
        keep = place_ref[1 + first_slot + j].astype(F32)
        for hop in range(len(out_refs)):
            peer = lax.rem(place_ref[0] + hop, peers)
            out_refs[hop][j] = (state_ref[j, peer] * keep).astype(BF16)


def pack(place, states, after):
    slots, peers, piece, width = states.shape
    half = piece // 2
    steps = pl.cdiv(slots, SLOT_TILE)
    return pl.pallas_call(
        pack_kernel,
        grid=(steps,),
        in_specs=[
            pl.BlockSpec(memory_space=pltpu.SMEM),
            pl.BlockSpec((SLOT_TILE, peers, half, width), lambda t: (t, 0, 0, 0)),
            pl.BlockSpec(memory_space=pl.ANY),
        ],
        out_specs=[pl.BlockSpec((SLOT_TILE, half, width), lambda t: (t, 0, 0))] * peers,
        out_shape=[jax.ShapeDtypeStruct((slots, half, width), BF16)] * peers,
        compiler_params=pltpu.CompilerParams(dimension_semantics=("arbitrary",)),
        name="pack",
    )(place, states, after)


def pack_rest_kernel(place_ref, state_ref, after_ref, out_ref):
    first_slot = pl.program_id(0) * SLOT_TILE
    for j in range(SLOT_TILE):
        keep = place_ref[1 + first_slot + j].astype(F32)
        out_ref[:, j] = (state_ref[j] * keep).astype(BF16)


def pack_rest(place, states, after):
    slots, peers, piece, width = states.shape
    half = piece // 2
    steps = pl.cdiv(slots, SLOT_TILE)
    return pl.pallas_call(
        pack_rest_kernel,
        grid=(steps,),
        in_specs=[
            pl.BlockSpec(memory_space=pltpu.SMEM),
            pl.BlockSpec((SLOT_TILE, peers, half, width), lambda t: (t, 0, 1, 0)),
            pl.BlockSpec(memory_space=pl.ANY),
        ],
        out_specs=pl.BlockSpec((peers, SLOT_TILE, half, width), lambda t: (0, t, 0, 0)),
        out_shape=jax.ShapeDtypeStruct((peers, slots, half, width), BF16),
        compiler_params=pltpu.CompilerParams(dimension_semantics=("arbitrary",)),
        name="pack_rest",
    )(place, states, after)


def reorder_kernel(order_ref, *refs):
    in_refs, out_ref, sems = refs[:-2], refs[-2], refs[-1]
    slots = in_refs[0].shape[0]
    for hop in range(len(in_refs)):

        def start(i, unused):
            target = order_ref[hop * slots + i]
            pltpu.make_async_copy(in_refs[hop].at[i], out_ref.at[target], sems.at[hop]).start()
            return unused

        lax.fori_loop(0, slots, start, 0)
    for hop in range(len(in_refs)):
        span = pl.ds(hop * slots, slots)
        pltpu.make_async_copy(in_refs[hop], out_ref.at[span], sems.at[hop]).wait()


def reorder(order, pieces):
    slots, half, width = pieces[0].shape
    count = len(pieces)
    whole = pl.BlockSpec(memory_space=pltpu.HBM)
    return pl.pallas_call(
        reorder_kernel,
        in_specs=[pl.BlockSpec(memory_space=pltpu.SMEM)] + [whole] * count,
        out_specs=whole,
        out_shape=jax.ShapeDtypeStruct((count * slots, half, width), BF16),
        scratch_shapes=[pltpu.SemaphoreType.DMA((count,))],
        name="reorder",
    )(order, *pieces)


def unpack_kernel(place_ref, final_ref, *refs):
    pieces, out_ref = refs[:-1], refs[-1]
    step = pl.program_id(0)
    peers, half = out_ref.shape[1:3]
    for hop in range(peers):
        peer = lax.rem(place_ref[0] - hop + peers, peers)
        for j in range(SLOT_TILE):
            out_ref[j, peer] = pieces[hop][j].astype(F32)

    @pl.when(step == 0)
    def _():
        for p in range(peers):
            out_ref[0, p] = final_ref[2 * p * half : (2 * p + 1) * half, :]


def unpack(place, final, pieces):
    peers = len(pieces)
    slots, half, width = pieces[0].shape
    return pl.pallas_call(
        unpack_kernel,
        grid=(pl.cdiv(slots, SLOT_TILE),),
        in_specs=[
            pl.BlockSpec(memory_space=pltpu.SMEM),
            pl.BlockSpec(final.shape, lambda t: (0, 0)),
        ]
        + [pl.BlockSpec((SLOT_TILE, half, width), lambda t: (t, 0, 0))] * peers,
        out_specs=pl.BlockSpec((SLOT_TILE, peers, half, width), lambda t: (t, 0, 0, 0)),
        out_shape=jax.ShapeDtypeStruct((slots, peers, 2 * half, width), F32),
        compiler_params=pltpu.CompilerParams(dimension_semantics=("arbitrary",)),
        name="unpack",
    )(place, final, *pieces)


def unpack_rest_kernel(final_ref, pieces_ref, states_ref, out_ref):
    peers, half = pieces_ref.shape[0], pieces_ref.shape[2]
    for p in range(peers):
        out_ref[0, p] = final_ref[(2 * p + 1) * half : (2 * p + 2) * half, :]
        out_ref[1:, p] = pieces_ref[p].astype(F32)


def unpack_rest(final, pieces, states):
    slots, peers, piece, width = states.shape
    half = piece // 2
    return pl.pallas_call(
        unpack_rest_kernel,
        grid=(peers // PEER_TILE,),
        in_specs=[
            pl.BlockSpec((PEER_TILE * piece, width), lambda p: (p, 0)),
            pl.BlockSpec((PEER_TILE, slots - 1, half, width), lambda p: (p, 0, 0, 0)),
            pl.BlockSpec(memory_space=pl.ANY),
        ],
        out_specs=pl.BlockSpec((slots, PEER_TILE, half, width), lambda p: (0, p, 1, 0)),
        out_shape=jax.ShapeDtypeStruct(states.shape, F32),
        input_output_aliases={2: 0},
        compiler_params=pltpu.CompilerParams(dimension_semantics=("arbitrary",)),
        name="unpack_rest",
    )(final, pieces, states)


def combine_kernel(place_ref, decay_ref, *refs):
    peers, count = decay_ref.shape[1], decay_ref.shape[0]
    count = decay_ref.shape[0]
    scr, end_scr, enter_scr = refs[-3:]
    entering_refs = refs[-4 - count : -4]
    final_ref = refs[-4]
    inputs = refs[: -4 - count]
    end_refs = inputs[:count]
    peers = (len(inputs) - count) // 2
    upper, lower = inputs[count : count + peers], inputs[count + peers :]
    half = lower[0].shape[0]
    chain = place_ref[1]
    for hop in range(peers):
        peer = lax.rem(place_ref[0] - hop + peers, peers)
        at = pl.multiple_of(peer * 2 * half, 16)
        scr[pl.ds(at, half), :] = upper[hop][0]
        scr[pl.ds(at + half, half), :] = lower[hop][...]
    for hop in range(count):
        end_scr[lax.rem(chain - hop + count, count)] = end_refs[hop][...]
    state = scr[...].astype(F32).T
    for k in range(count):
        enter_scr[k] = state.astype(BF16)
        state = state * decay_ref[k : k + 1, :] + end_scr[k].astype(F32)
    for hop in range(count):
        entering_refs[hop][...] = enter_scr[lax.rem(chain + hop, count)]
    final_ref[...] = state.T


def combine(place, decay, ends, upper, lower):
    count = len(ends)
    whole = pl.BlockSpec(memory_space=pltpu.VMEM)
    half, width = lower[0].shape
    rows, columns = ends[0].shape
    outs = pl.pallas_call(
        combine_kernel,
        grid=(1,),
        in_specs=[
            pl.BlockSpec(memory_space=pltpu.SMEM),
            pl.BlockSpec(decay.shape, lambda t: (0, 0)),
        ]
        + [pl.BlockSpec((rows, columns), lambda t: (0, 0))] * count
        + [pl.BlockSpec((1, half, width), lambda t: (0, 0, 0))] * len(upper)
        + [pl.BlockSpec((half, width), lambda t: (0, 0))] * len(lower),
        out_specs=[pl.BlockSpec((rows, columns), lambda t: (0, 0))] * count
        + [pl.BlockSpec((columns, rows), lambda t: (0, 0))],
        out_shape=[jax.ShapeDtypeStruct((rows, columns), BF16)] * count
        + [jax.ShapeDtypeStruct((columns, rows), F32)],
        scratch_shapes=[
            pltpu.VMEM((columns, rows), BF16),
            pltpu.VMEM((count, rows, columns), BF16),
            pltpu.VMEM((count, rows, columns), BF16),
        ],
        name="combine",
    )(place, decay, *ends, *upper, *lower)
    return outs[:count], outs[count]


def share_kernel(
    place_ref,
    every_ref,
    end_ref,
    kept_ref,
    kept_next_ref,
    state_end_ref,
    state_kept_ref,
    state_next_ref,
    raw_ref,
    bias_ref,
    rate_ref,
    out_ref,
    step_ref,
):
    taps = out_ref.shape[0]
    inner = end_ref.shape[1]
    outer = state_end_ref.shape[1]
    channels = inner + outer
    first = place_ref[0]
    low_block, high_block, start, length = (
        place_ref[1],
        place_ref[2],
        place_ref[3],
        place_ref[4],
    )
    out_ref[:, :inner] = end_ref[16 - taps :, :]
    out_ref[:, inner:channels] = state_end_ref[16 - taps :, :]
    here = lax.broadcasted_iota(jnp.int32, (16, 1), 0)
    wanted = length - taps - start

    def kept_rows(low_ref, high_ref):
        low = low_ref[...].astype(F32)
        high = high_ref[...].astype(F32)
        found = []
        for i in range(taps):
            in_low = (low_block * 16 + here) == (wanted + i)
            in_high = ((high_block * 16 + here) == (wanted + i)) & (high_block > low_block)
            picked = jnp.where(in_low, low, 0.0) + jnp.where(in_high, high, 0.0)
            found.append(jnp.sum(picked, axis=0, keepdims=True))
        return jnp.concatenate(found, axis=0).astype(BF16)

    out_ref[:, channels : channels + inner] = kept_rows(kept_ref, kept_next_ref)
    out_ref[:, channels + inner : 2 * channels] = kept_rows(state_kept_ref, state_next_ref)
    window = every_ref[first].astype(F32)
    width = window.shape[1]
    keep = window[taps - 1 :, width - 1 :]
    out_ref[:, 2 * channels : 2 * channels + width] = (window * keep).astype(BF16)
    count = step_ref.shape[0]
    heads = raw_ref.shape[1]
    positions = start + lax.broadcasted_iota(jnp.int32, (count, heads), 0)
    raw = raw_ref[...].astype(F32) + bias_ref[...]
    step = jnp.maximum(raw, 0.0) + jnp.log1p(jnp.exp(-jnp.abs(raw)))
    step = jnp.where(positions < length, step, 0.0)
    step = jnp.concatenate([step, jnp.zeros((count, LANES - heads), F32)], axis=1)
    step_ref[...] = step
    total = jnp.sum(step * rate_ref[...], axis=0, keepdims=True)
    high = total.astype(BF16).astype(F32)
    middle = (total - high).astype(BF16).astype(F32)
    rest = total - high - middle
    parts = jnp.concatenate([high, middle, rest], axis=0)
    out_ref[:, 2 * channels + width :] = parts.astype(BF16)


def share(place, every, rows, state_rows, step_raw, step_bias, rate):
    taps = every.shape[1]
    width = every.shape[2]
    length, inner = rows.shape
    outer = state_rows.shape[1]
    heads = step_raw.shape[1]
    last = length // 16 - 1
    total = 2 * (inner + outer) + width + LANES
    return pl.pallas_call(
        share_kernel,
        grid_spec=pltpu.PrefetchScalarGridSpec(
            num_scalar_prefetch=1,
            grid=(1,),
            in_specs=[
                pl.BlockSpec(every.shape, lambda t, c: (0, 0, 0)),
                pl.BlockSpec((16, inner), lambda t, c: (last, 0)),
                pl.BlockSpec((16, inner), lambda t, c: (c[1], 0)),
                pl.BlockSpec((16, inner), lambda t, c: (c[2], 0)),
                pl.BlockSpec((16, outer), lambda t, c: (last, 0)),
                pl.BlockSpec((16, outer), lambda t, c: (c[1], 0)),
                pl.BlockSpec((16, outer), lambda t, c: (c[2], 0)),
                pl.BlockSpec((length, heads), lambda t, c: (0, 0)),
                pl.BlockSpec((1, heads), lambda t, c: (0, 0)),
                pl.BlockSpec((1, LANES), lambda t, c: (0, 0)),
            ],
            out_specs=[
                pl.BlockSpec((taps, total), lambda t, c: (0, 0)),
                pl.BlockSpec((length, LANES), lambda t, c: (0, 0)),
            ],
        ),
        out_shape=[
            jax.ShapeDtypeStruct((taps, total), BF16),
            jax.ShapeDtypeStruct((length, LANES), F32),
        ],
        name="share",
    )(
        place,
        every,
        rows,
        rows,
        rows,
        state_rows,
        state_rows,
        state_rows,
        step_raw,
        step_bias,
        rate,
    )


def tail_kernel(chain_ref, shared_ref, tail_ref, inner_ref, outer_ref, decay_ref):
    chain = chain_ref[0]
    count, taps = shared_ref.shape[:2]
    inner_local, outer_local = inner_ref.shape[1], outer_ref.shape[1]
    channels = tail_ref.shape[1]
    inner = count * inner_local
    at = 2 * channels
    window = jnp.concatenate(
        [shared_ref[s, :, at : at + inner_local] for s in range(count)]
        + [
            shared_ref[s, :, at + inner_local : at + inner_local + outer_local]
            for s in range(count)
        ],
        axis=1,
    ).astype(F32)
    earlier = shared_ref[jnp.maximum(chain - 1, 0), :, :channels].astype(F32)
    tail = jnp.where(chain == 0, window, earlier)
    tail_ref[...] = jnp.concatenate([jnp.zeros((8 - taps, channels), F32), tail], axis=0)
    kept = shared_ref[0, :, channels:at].astype(F32)
    for s in range(1, count):
        kept = kept + shared_ref[s, :, channels:at].astype(F32)
    own_inner = jnp.zeros((taps, inner_local), F32)
    own_outer = jnp.zeros((taps, outer_local), F32)
    for s in range(count):
        mine = chain == s
        inner_at, outer_at = s * inner_local, inner + s * outer_local
        own_inner = jnp.where(mine, kept[:, inner_at : inner_at + inner_local], own_inner)
        own_outer = jnp.where(mine, kept[:, outer_at : outer_at + outer_local], own_outer)
    inner_ref[...] = own_inner.astype(BF16)
    outer_ref[...] = own_outer.astype(BF16)
    logs = []
    for s in range(count):
        parts = shared_ref[s, :, shared_ref.shape[2] - LANES :].astype(F32)
        logs.append(jnp.sum(parts, axis=0, keepdims=True))
    logs = jnp.concatenate(logs + [jnp.zeros((8 - count, LANES), F32)] * (count < 8), axis=0)
    columns = decay_ref.shape[1]
    head = lax.broadcasted_iota(jnp.int32, (LANES, columns), 0)
    lane = lax.broadcasted_iota(jnp.int32, (LANES, columns), 1)
    local_heads = columns // HEAD_DIM
    pick = (head == chain * local_heads + lane // HEAD_DIM).astype(F32)
    spread = dot(logs, pick, precision=lax.Precision.HIGHEST)
    decay_ref[...] = jnp.exp2(spread[:count])


def tails(chain, shared, channels, inner_local, outer_local, columns):
    count, taps = shared.shape[:2]
    whole = pl.BlockSpec(memory_space=pltpu.VMEM)
    return pl.pallas_call(
        tail_kernel,
        in_specs=[pl.BlockSpec(memory_space=pltpu.SMEM), whole],
        out_shape=[
            jax.ShapeDtypeStruct((8, channels), F32),
            jax.ShapeDtypeStruct((taps, inner_local), BF16),
            jax.ShapeDtypeStruct((taps, outer_local), BF16),
            jax.ShapeDtypeStruct((count, columns), F32),
        ],
        name="tails",
    )(chain, shared)


def exchange(value, axis):
    return lax.all_to_all(value, axis, split_axis=0, concat_axis=0, tiled=True)


def rotate(values, axis):
    count = lax.axis_size(axis)
    got = [values[0]] + [None] * (count - 1)
    for hop in sorted(range(1, count), key=lambda hop: abs(2 * hop - count)):
        pairs = [(source, (source + hop) % count) for source in range(count)]
        got[hop] = lax.ppermute(values[hop], axis, pairs)
    return got


def rows_at(source, indices):
    return source.at[indices].get(mode="promise_in_bounds")


def device_body(
    pool_states,
    inner_window,
    state_window,
    move_plan,
    active_mask,
    inputs_inner,
    inputs_state,
    gate_rows,
    step_raw,
    lengths,
    conv_weight,
    conv_bias,
    step_bias,
    decay_log,
    skip_weight,
    norm_weight,
):
    peers = lax.axis_size("req")
    own_peer = lax.axis_index("req").astype(jnp.int32)
    chain_size = lax.axis_size("seq")
    chain_index = lax.axis_index("seq").astype(jnp.int32)
    slots, local_heads = pool_states.shape[:2]
    columns = local_heads * HEAD_DIM
    piece = columns // peers
    half = piece // 2
    taps = KERNEL - 1
    inner_local = inner_window.shape[2]
    outer_local = state_window.shape[2]
    width = inner_local + outer_local

    marks = jnp.stack([move_plan[:, 0], move_plan[:, 1], active_mask], axis=1).astype(BF16)
    marks = jnp.broadcast_to(marks[:, :, None], (slots, taps, (-width) % LANES))
    packed = jnp.concatenate([inner_window, state_window, marks], axis=2)
    every = lax.all_gather(packed, "req", axis=0, tiled=True)

    own = own_peer[None]
    pack_place = jnp.concatenate(
        [own, active_mask, jnp.zeros((-slots % SLOT_TILE,), jnp.int32)]
    )
    pool_pieces = pool_states.reshape(slots, peers, piece, STATE_DIM)
    spread_a = rotate(pack(pack_place, pool_pieces, every), "req")
    spread_b = exchange(pack_rest(pack_place, pool_pieces, every), "req")
    spread_b = spread_b.reshape(peers * slots, half, STATE_DIM)

    every_marks = every[:, :, width].astype(F32).astype(jnp.int32)
    target_peer = every_marks[:, 0]
    target_slot = every_marks[:, 1]
    order = jnp.arange(peers * slots, dtype=jnp.int32)
    targets = target_peer * slots + target_slot
    sources = jnp.sum(jnp.where(targets[None, :] == order[:, None], order[None, :], 0), axis=1)
    own_sources = lax.dynamic_slice_in_dim(sources, own_peer * slots, slots)
    hop_targets = lax.rem(target_peer - own_peer + peers, peers) * slots + target_slot
    peer_order = jnp.arange(peers, dtype=jnp.int32)
    by_hop = rows_at(
        hop_targets.reshape(peers, slots), lax.rem(own_peer + peers - peer_order, peers)
    ).reshape(-1)

    rows = inputs_inner[0]
    state_rows = inputs_state[0]
    local_length, inner_dim = rows.shape
    channels = inner_dim + state_rows.shape[1]
    start = chain_index * local_length
    length = lengths[0]
    last_tile = local_length // 16 - 1
    low_block = jnp.clip((length - taps - start) // 16, 0, last_tile)
    high_block = jnp.minimum(low_block + 1, last_tile)
    heads = decay_log.shape[0]
    rate = jnp.pad(-LOG2E * jnp.exp(decay_log), (0, LANES - heads))[None]
    payload, step = share(
        jnp.stack([own_sources[0], low_block, high_block, start, length]),
        every,
        rows,
        state_rows,
        step_raw[0],
        step_bias[None],
        rate,
    )
    shared = lax.all_gather(payload, "seq", axis=0)
    chain = chain_index[None]
    tail, kept_inner, kept_outer, own_decay = tails(
        chain, shared, channels, inner_local, outer_local, columns
    )

    reordered = reorder(by_hop, spread_a).reshape(peers, slots, half, STATE_DIM)
    moved_a = rotate(reordered, "req")

    part, local_end, read_rows, decay = block_parts(
        chain,
        tail,
        rows,
        state_rows,
        step,
        rate,
        conv_weight,
        conv_bias[None],
        jnp.repeat(skip_weight, HEAD_DIM)[None],
        chain_size,
    )
    own_ends = rotate(local_end, "seq")

    order_by_peer = sources.reshape(peers, slots)
    first_sources = rows_at(order_by_peer[:, 0], lax.rem(own_peer + peer_order, peers))
    first_b = rotate(rows_at(spread_b, first_sources), "req")
    rest = rows_at(spread_b, order_by_peer[:, 1:].reshape(-1))
    rest_b = exchange(rest.reshape(peers, slots - 1, half, STATE_DIM), "req")

    place = jnp.stack([own_peer, chain_index])
    entering, final = combine(place, own_decay, own_ends, moved_a, first_b)
    incoming = rotate(entering, "seq")
    mixer_out = finish(
        jnp.stack([start, length, chain_index]),
        part,
        gate_rows[0],
        read_rows,
        decay,
        norm_weight[None],
        incoming,
    )
    states = unpack(place, final, moved_a)
    new_states = unpack_rest(final, rest_b, states).reshape(pool_states.shape)

    moved = rows_at(every, own_sources).astype(F32)
    moved = (moved[1:, :, :width] * moved[1:, taps - 1 :, width:][:, :, :1]).astype(BF16)
    new_inner = jnp.concatenate([kept_inner[None], moved[:, :, :inner_local]], axis=0)
    new_outer = jnp.concatenate([kept_outer[None], moved[:, :, inner_local:]], axis=0)
    return (new_states, new_inner, new_outer, mixer_out[None])


def solution(mesh):
    return jax.shard_map(
        device_body,
        mesh=mesh,
        in_specs=(
            P("req", "seq", None, None),
            P("req", None, "seq"),
            P("req", None, "seq"),
            P("req", None),
            P("req"),
            P("req", "seq", None),
            P("req", "seq", None),
            P("req", "seq", None),
            P("req", "seq", None),
            P("req"),
            P(),
            P(),
            P(),
            P(),
            P(),
            P(),
        ),
        out_specs=(
            P("req", "seq", None, None),
            P("req", None, "seq"),
            P("req", None, "seq"),
            P("req", "seq", None),
        ),
        check_vma=False,
    )
```

```python
import math

import jax
import jax.numpy as jnp
from jax import lax
from jax.experimental import pallas as pl
from jax.experimental.pallas import tpu as pltpu
from jax.sharding import PartitionSpec as P


HEAD_DIM = 64
STATE_DIM = 128
KERNEL = 4
BLOCK_LEN = 256
GROUP = 8
HALF = BLOCK_LEN // 2
GROUP_DIM = GROUP * HEAD_DIM
PAIR_DIM = 2 * HEAD_DIM
LANES = 128
TILE = 128
SLOT_TILE = 4
SLOT_PAD = 16
PEER_TILE = 2
EPSILON = 1e-05
LOG2E = math.log2(math.e)
F32 = jnp.float32
BF16 = jnp.bfloat16


def dot(a, b, dims=((1,), (0,)), precision=None):
    return lax.dot_general(a, b, (dims, ((), ())), precision=precision, preferred_element_type=F32)


def silu(v):
    return v / (1.0 + jnp.exp(-v))


def conv_silu(tail, rows, weight, bias_row):
    extended = jnp.concatenate([tail, rows.astype(F32)], axis=0)
    count = rows.shape[0]
    start = tail.shape[0] - KERNEL + 1
    running = bias_row + weight[0:1] * extended[start : start + count]
    for k in range(1, KERNEL):
        running = running + weight[k : k + 1] * extended[start + k : start + k + count]
    return silu(running)


def pair_of(columns, i, low):
    return jnp.where(low, columns[:, 2 * i : 2 * i + 1], columns[:, 2 * i + 1 : 2 * i + 2])


def block_kernel(
    chain_ref,
    tail_ref,
    prev_ref,
    rows_ref,
    state_tail_ref,
    state_prev_ref,
    state_rows_ref,
    step_ref,
    rate_ref,
    weight_ref,
    bias_ref,
    state_weight_ref,
    state_bias_ref,
    skip_ref,
    part_ref,
    end_ref,
    read_ref,
    decay_ref,
    scores_scr,
    cum_scr,
    cum_t_scr,
    to_end_scr,
    decay_scr,
    write_t_scr,
    offset_scr,
    carry_scr,
):
    block = pl.program_id(0)
    group = pl.program_id(1)
    first = block == 0

    @pl.when(group == 0)
    def _():
        state_tail = jnp.where(first, state_tail_ref[...], state_prev_ref[8:16, :].astype(F32))
        mixed = conv_silu(state_tail, state_rows_ref[...], state_weight_ref[...], state_bias_ref[...])
        write = mixed[:, :STATE_DIM]
        read = mixed[:, STATE_DIM:].astype(BF16)
        read_ref[...] = read
        write_b = write.astype(BF16)
        scores_scr[...] = dot(read, write_b, ((1,), (1,)))
        write_t_scr[...] = write_b.astype(F32).T.astype(BF16)
        row = lax.broadcasted_iota(jnp.int32, (BLOCK_LEN, BLOCK_LEN), 0)
        col = lax.broadcasted_iota(jnp.int32, (BLOCK_LEN, BLOCK_LEN), 1)
        triangle = (row >= col).astype(F32)
        step = step_ref[...]
        cum = dot(triangle, step * rate_ref[...], precision=lax.Precision.HIGHEST)
        cum_scr[...] = cum
        cum_t_scr[...] = cum.T
        last = cum[BLOCK_LEN - 1 :, :]
        to_end_scr[...] = jnp.exp2(last - cum) * step
        decay_scr[...] = jnp.exp2(cum)
        offset = jnp.where(first, 0.0, offset_scr[0:1, :])
        decay_ref[...] = jnp.exp2(offset + cum)
        offset_scr[0:1, :] = offset + last

    shift = lax.rem(LANES - group * GROUP, LANES)
    cum = pltpu.roll(cum_scr[...], shift, 1)
    step = pltpu.roll(step_ref[...], shift, 1)
    to_end = pltpu.roll(to_end_scr[...], shift, 1)
    decay = pltpu.roll(decay_scr[...], shift, 1)
    cum_t = cum_t_scr[pl.ds(pl.multiple_of(group * GROUP, GROUP), GROUP), :]
    read = read_ref[...]
    write_t = write_t_scr[...]
    carry = jnp.where(first, 0.0, carry_scr[group])
    carry_b = carry.astype(BF16)
    low = lax.broadcasted_iota(jnp.int32, (1, PAIR_DIM), 1) < HEAD_DIM
    causal = lax.broadcasted_iota(jnp.int32, (HALF, HALF), 0) >= lax.broadcasted_iota(
        jnp.int32, (HALF, HALF), 1
    )
    scores_top = scores_scr[0:HALF, 0:HALF]
    scores_left = scores_scr[HALF:, 0:HALF]
    scores_right = scores_scr[HALF:, HALF:]

    def head_weights(i):
        later = cum[:, i : i + 1]
        earlier = cum_t[i : i + 1, :]
        gap_top = jnp.where(causal, later[:HALF] - earlier[:, :HALF], -1e30)
        gap_left = later[HALF:] - earlier[:, :HALF]
        gap_right = jnp.where(causal, later[HALF:] - earlier[:, HALF:], -1e30)
        top = (scores_top * jnp.exp2(gap_top)).astype(BF16)
        left = (scores_left * jnp.exp2(gap_left)).astype(BF16)
        right = (scores_right * jnp.exp2(gap_right)).astype(BF16)
        return top, jnp.concatenate([left, right], axis=1)

    for i in range(GROUP // 2):
        span = slice(i * PAIR_DIM, (i + 1) * PAIR_DIM)
        tail = jnp.where(first, tail_ref[:, span], prev_ref[8:16, span].astype(F32))
        mixed = conv_silu(tail, rows_ref[:, span], weight_ref[:, span], bias_ref[:, span])
        value = mixed.astype(BF16).astype(F32)
        stepped = (pair_of(step, i, low) * value).astype(BF16)
        scaled = (pair_of(to_end, i, low) * value).astype(BF16)
        stepped_low = jnp.where(low, stepped, jnp.zeros_like(stepped))
        stepped_high = jnp.where(low, jnp.zeros_like(stepped), stepped)
        top_0, bottom_0 = head_weights(2 * i)
        top_1, bottom_1 = head_weights(2 * i + 1)
        intra_top = dot(top_0, stepped_low[:HALF]) + dot(top_1, stepped_high[:HALF])
        intra_bottom = dot(bottom_0, stepped_low) + dot(bottom_1, stepped_high)
        inter = dot(read, carry_b[:, span]) * pair_of(decay, i, low)
        direct = inter + skip_ref[:, span] * value
        part_ref[0:HALF, span] = intra_top + direct[:HALF]
        part_ref[HALF:, span] = intra_bottom + direct[HALF:]
        kept = pair_of(decay[BLOCK_LEN - 1 :, :], i, low) * carry[:, span]
        ending = kept + dot(write_t, scaled)
        carry_scr[group, :, span] = ending
        end_ref[0, :, span] = ending.astype(BF16)


def block_parts(chain, tail, rows, state_rows, step, rate, weight, bias_row, skip_row, ends):
    length = rows.shape[0]
    channels = rows.shape[1]
    blocks = length // BLOCK_LEN
    groups = channels // GROUP_DIM
    end_groups = groups // ends
    state_dim = state_rows.shape[1]
    state_at = channels // state_dim
    per_block = BLOCK_LEN // 16

    def before(b):
        return jnp.maximum(b * per_block - 1, 0)

    def end_at(b, g, chain):
        return lax.rem(g // end_groups - chain[0] + ends, ends), 0, lax.rem(g, end_groups)

    return pl.pallas_call(
        block_kernel,
        grid_spec=pltpu.PrefetchScalarGridSpec(
        num_scalar_prefetch=1,
        grid=(blocks, groups),
        in_specs=[
            pl.BlockSpec((8, GROUP_DIM), lambda b, g, c: (0, g)),
            pl.BlockSpec((16, GROUP_DIM), lambda b, g, c: (before(b), g)),
            pl.BlockSpec((BLOCK_LEN, GROUP_DIM), lambda b, g, c: (b, g)),
            pl.BlockSpec((8, state_dim), lambda b, g, c: (0, state_at)),
            pl.BlockSpec((16, state_dim), lambda b, g, c: (before(b), 0)),
            pl.BlockSpec((BLOCK_LEN, state_dim), lambda b, g, c: (b, 0)),
            pl.BlockSpec((BLOCK_LEN, LANES), lambda b, g, c: (b, 0)),
            pl.BlockSpec((1, LANES), lambda b, g, c: (0, 0)),
            pl.BlockSpec((KERNEL, GROUP_DIM), lambda b, g, c: (0, g)),
            pl.BlockSpec((1, GROUP_DIM), lambda b, g, c: (0, g)),
            pl.BlockSpec((KERNEL, state_dim), lambda b, g, c: (0, state_at)),
            pl.BlockSpec((1, state_dim), lambda b, g, c: (0, state_at)),
            pl.BlockSpec((1, GROUP_DIM), lambda b, g, c: (0, g)),
        ],
        out_specs=[
            pl.BlockSpec((BLOCK_LEN, GROUP_DIM), lambda b, g, c: (b, g)),
            pl.BlockSpec((1, STATE_DIM, GROUP_DIM), end_at),
            pl.BlockSpec((BLOCK_LEN, STATE_DIM), lambda b, g, c: (b, 0)),
            pl.BlockSpec((BLOCK_LEN, LANES), lambda b, g, c: (b, 0)),
        ],
        scratch_shapes=[
            pltpu.VMEM((BLOCK_LEN, BLOCK_LEN), F32),
            pltpu.VMEM((BLOCK_LEN, LANES), F32),
            pltpu.VMEM((LANES, BLOCK_LEN), F32),
            pltpu.VMEM((BLOCK_LEN, LANES), F32),
            pltpu.VMEM((BLOCK_LEN, LANES), F32),
            pltpu.VMEM((STATE_DIM, BLOCK_LEN), BF16),
            pltpu.VMEM((8, LANES), F32),
            pltpu.VMEM((groups, STATE_DIM, GROUP_DIM), F32),
        ],
        ),
        out_shape=[
            jax.ShapeDtypeStruct((length, channels), F32),
            jax.ShapeDtypeStruct((ends, STATE_DIM, channels // ends), BF16),
            jax.ShapeDtypeStruct((length, STATE_DIM), BF16),
            jax.ShapeDtypeStruct((length, LANES), F32),
        ],
        compiler_params=pltpu.CompilerParams(dimension_semantics=("arbitrary", "arbitrary")),
        cost_estimate=pl.CostEstimate(
            flops=6_000_000_000, bytes_accessed=20_000_000, transcendentals=10_000_000
        ),
        name="block_parts",
    )(
        chain,
        tail,
        rows,
        rows,
        tail,
        state_rows,
        state_rows,
        step,
        rate,
        weight,
        bias_row,
        weight,
        bias_row,
        skip_row,
    )


def finish_kernel(
    place_ref, part_ref, gate_ref, read_ref, decay_ref, norm_ref, *refs
):
    state_refs, out_ref, gated_scr, state_scr = refs[:-3], refs[-3], refs[-2], refs[-1]
    tile = pl.program_id(0)
    chunks, _, width = state_scr.shape

    @pl.when(tile == 0)
    def _():
        for hop in range(chunks):
            state_scr[lax.rem(place_ref[2] - hop + chunks, chunks)] = state_refs[hop][...]

    positions = (
        place_ref[0] + tile * TILE + lax.broadcasted_iota(jnp.int32, (TILE, PAIR_DIM), 0)
    )
    valid = (positions < place_ref[1]).astype(F32)
    low = lax.broadcasted_iota(jnp.int32, (1, PAIR_DIM), 1) < HEAD_DIM
    read = read_ref[...]
    decay = decay_ref[...]
    total = jnp.zeros((TILE, PAIR_DIM), F32)
    for chunk in range(chunks):
        for i in range(width // PAIR_DIM):
            pair = chunk * (width // PAIR_DIM) + i
            span = slice(pair * PAIR_DIM, (pair + 1) * PAIR_DIM)
            inter = dot(read, state_scr[chunk, :, i * PAIR_DIM : (i + 1) * PAIR_DIM])
            y = part_ref[:, span] + inter * pair_of(decay, pair, low)
            y = (y * valid).astype(BF16).astype(F32)
            gated = y * silu(gate_ref[:, span].astype(F32))
            gated_scr[:, span] = gated
            total = total + gated * gated
    channels = chunks * width
    mean = jnp.sum(total, axis=1, keepdims=True) * (1.0 / channels)
    scale = lax.rsqrt(mean + EPSILON)
    for pair in range(channels // PAIR_DIM):
        span = slice(pair * PAIR_DIM, (pair + 1) * PAIR_DIM)
        out_ref[:, span] = (gated_scr[:, span] * scale * norm_ref[:, span]).astype(BF16)


def finish(place, part, gate, read, decay, norm_row, states):
    length, channels = part.shape
    return pl.pallas_call(
        finish_kernel,
        grid=(length // TILE,),
        in_specs=[
            pl.BlockSpec(memory_space=pltpu.SMEM),
            pl.BlockSpec((TILE, channels), lambda t: (t, 0)),
            pl.BlockSpec((TILE, channels), lambda t: (t, 0)),
            pl.BlockSpec((TILE, STATE_DIM), lambda t: (t, 0)),
            pl.BlockSpec((TILE, LANES), lambda t: (t, 0)),
            pl.BlockSpec((1, channels), lambda t: (0, 0)),
        ]
        + [pl.BlockSpec(state.shape, lambda t: (0, 0)) for state in states],
        out_specs=pl.BlockSpec((TILE, channels), lambda t: (t, 0)),
        out_shape=jax.ShapeDtypeStruct((length, channels), BF16),
        scratch_shapes=[
            pltpu.VMEM((TILE, channels), F32),
            pltpu.VMEM((len(states),) + states[0].shape, BF16),
        ],
        compiler_params=pltpu.CompilerParams(dimension_semantics=("arbitrary",)),
        cost_estimate=pl.CostEstimate(
            flops=3_000_000_000, bytes_accessed=16_000_000, transcendentals=4_000_000
        ),
        name="finish",
    )(place, part, gate, read, decay, norm_row, *states)


def mark_kernel(plan_ref, mask_ref, inner_ref, outer_ref, out_ref):
    peers, taps, padded, total = out_ref.shape
    slots = inner_ref.shape[1]
    width = inner_ref.shape[2] + outer_ref.shape[2]
    row = lax.broadcasted_iota(jnp.int32, (padded, total - width), 0)
    fill = jnp.zeros((padded - slots, width), F32)
    for tap in range(taps):
        marks = jnp.full((padded, total - width), -1.0, F32)
        for slot in range(slots):
            value = mask_ref[slot] if tap == 2 else plan_ref[slot, tap]
            marks = jnp.where(row == slot, value.astype(F32), marks)
        window = jnp.concatenate(
            [inner_ref[tap].astype(F32), outer_ref[tap].astype(F32)], axis=1
        )
        window = jnp.concatenate([window, fill], axis=0)
        block = jnp.concatenate([window, marks], axis=1).astype(BF16)
        for peer in range(peers):
            out_ref[peer, tap] = block


def mark(plan, mask, inner, outer, peers):
    taps, _ = inner.shape[:2]
    width = inner.shape[2] + outer.shape[2]
    whole = pl.BlockSpec(memory_space=pltpu.VMEM)
    scalar = pl.BlockSpec(memory_space=pltpu.SMEM)
    total = width + LANES - width % LANES
    return pl.pallas_call(
        mark_kernel,
        in_specs=[scalar, scalar, whole, whole],
        out_shape=jax.ShapeDtypeStruct((peers, taps, SLOT_PAD, total), BF16),
        name="mark",
    )(plan, mask, inner, outer)


def pack_kernel(own_ref, mask_ref, state_ref, *out_refs):
    first_slot = pl.program_id(0) * SLOT_TILE
    peers = state_ref.shape[1]
    for j in range(SLOT_TILE):
        keep = mask_ref[jnp.minimum(first_slot + j, mask_ref.shape[0] - 1)].astype(F32)
        for hop in range(len(out_refs)):
            peer = lax.rem(own_ref[0] + hop, peers)
            out_refs[hop][j] = (state_ref[j, peer] * keep).astype(BF16)


def pack(own, mask, states):
    slots, peers, piece, width = states.shape
    half = piece // 2
    steps = pl.cdiv(slots, SLOT_TILE)
    return pl.pallas_call(
        pack_kernel,
        grid=(steps,),
        in_specs=[
            pl.BlockSpec(memory_space=pltpu.SMEM),
            pl.BlockSpec(memory_space=pltpu.SMEM),
            pl.BlockSpec((SLOT_TILE, peers, half, width), lambda t: (t, 0, 0, 0)),
        ],
        out_specs=[pl.BlockSpec((SLOT_TILE, half, width), lambda t: (t, 0, 0))] * peers,
        out_shape=[jax.ShapeDtypeStruct((slots, half, width), BF16)] * peers,
        compiler_params=pltpu.CompilerParams(dimension_semantics=("arbitrary",)),
        name="pack",
    )(own, mask, states)


def pack_rest_kernel(mask_ref, state_ref, out_ref):
    first_slot = pl.program_id(0) * SLOT_TILE
    for j in range(SLOT_TILE):
        keep = mask_ref[jnp.minimum(first_slot + j, mask_ref.shape[0] - 1)].astype(F32)
        out_ref[:, j] = (state_ref[j] * keep).astype(BF16)


def pack_rest(mask, states):
    slots, peers, piece, width = states.shape
    half = piece // 2
    steps = pl.cdiv(slots, SLOT_TILE)
    return pl.pallas_call(
        pack_rest_kernel,
        grid=(steps,),
        in_specs=[
            pl.BlockSpec(memory_space=pltpu.SMEM),
            pl.BlockSpec((SLOT_TILE, peers, half, width), lambda t: (t, 0, 1, 0)),
        ],
        out_specs=pl.BlockSpec((peers, SLOT_TILE, half, width), lambda t: (0, t, 0, 0)),
        out_shape=jax.ShapeDtypeStruct((peers, slots, half, width), BF16),
        compiler_params=pltpu.CompilerParams(dimension_semantics=("arbitrary",)),
        name="pack_rest",
    )(mask, states)


def source_of(table_ref, target):
    code = table_ref[0, target]
    peer = lax.div(code, SLOT_PAD)
    return peer, code - peer * SLOT_PAD


def reorder_kernel(own_ref, table_ref, *refs):
    peers = (len(refs) - 1) // 2
    in_refs, out_refs, scr = refs[:peers], refs[peers:-1], refs[-1]
    slots = in_refs[0].shape[0]
    own = own_ref[0]
    for hop in range(peers):
        scr[hop] = in_refs[hop][...]
    for hop in range(peers):
        base = lax.rem(own + hop, peers) * slots

        def move(slot, unused):
            peer, index = source_of(table_ref, base + slot)
            out_refs[hop][slot] = scr[lax.rem(own - peer + peers, peers), index]
            return unused

        lax.fori_loop(0, slots, move, 0)


def reorder(own, table, pieces):
    slots, half, width = pieces[0].shape
    count = len(pieces)
    whole = pl.BlockSpec((slots, half, width), lambda t: (0, 0, 0))
    scalar = pl.BlockSpec(memory_space=pltpu.SMEM)
    return pl.pallas_call(
        reorder_kernel,
        grid=(1,),
        in_specs=[scalar, scalar] + [whole] * count,
        out_specs=[whole] * count,
        out_shape=[jax.ShapeDtypeStruct((slots, half, width), BF16)] * count,
        scratch_shapes=[pltpu.VMEM((count, slots, half, width), BF16)],
        name="reorder",
    )(own, table, *pieces)


def reorder_rest_kernel(own_ref, table_ref, in_ref, *out_refs):
    rest_ref, first_refs = out_refs[0], out_refs[1:]
    peers, slots = in_ref.shape[:2]
    own = own_ref[0]
    for hop in range(peers):
        target = lax.rem(own + hop, peers)
        peer, index = source_of(table_ref, target * slots)
        first_refs[hop][...] = in_ref[peer, index]

        def move(slot, unused):
            peer, index = source_of(table_ref, hop * slots + slot)
            rest_ref[hop, slot - 1] = in_ref[peer, index]
            return unused

        lax.fori_loop(1, slots, move, 0)


def reorder_rest(own, table, pieces):
    peers, slots, half, width = pieces.shape
    scalar = pl.BlockSpec(memory_space=pltpu.SMEM)
    outs = pl.pallas_call(
        reorder_rest_kernel,
        grid=(1,),
        in_specs=[scalar, scalar, pl.BlockSpec(pieces.shape, lambda t: (0, 0, 0, 0))],
        out_specs=[pl.BlockSpec((peers, slots - 1, half, width), lambda t: (0, 0, 0, 0))]
        + [pl.BlockSpec((half, width), lambda t: (0, 0))] * peers,
        out_shape=[jax.ShapeDtypeStruct((peers, slots - 1, half, width), BF16)]
        + [jax.ShapeDtypeStruct((half, width), BF16)] * peers,
        name="reorder_rest",
    )(own, table, pieces)
    return outs[0], outs[1:]


def unpack_kernel(place_ref, final_ref, *refs):
    pieces, out_ref = refs[:-1], refs[-1]
    step = pl.program_id(0)
    peers, half = out_ref.shape[1:3]
    for hop in range(peers):
        peer = lax.rem(place_ref[0] - hop + peers, peers)
        for j in range(SLOT_TILE):
            out_ref[j, peer] = pieces[hop][j].astype(F32)

    @pl.when(step == 0)
    def _():
        for p in range(peers):
            out_ref[0, p] = final_ref[2 * p * half : (2 * p + 1) * half, :]


def unpack(place, final, pieces):
    peers = len(pieces)
    slots, half, width = pieces[0].shape
    return pl.pallas_call(
        unpack_kernel,
        grid=(pl.cdiv(slots, SLOT_TILE),),
        in_specs=[
            pl.BlockSpec(memory_space=pltpu.SMEM),
            pl.BlockSpec(final.shape, lambda t: (0, 0)),
        ]
        + [pl.BlockSpec((SLOT_TILE, half, width), lambda t: (t, 0, 0))] * peers,
        out_specs=pl.BlockSpec((SLOT_TILE, peers, half, width), lambda t: (t, 0, 0, 0)),
        out_shape=jax.ShapeDtypeStruct((slots, peers, 2 * half, width), F32),
        compiler_params=pltpu.CompilerParams(dimension_semantics=("arbitrary",)),
        name="unpack",
    )(place, final, *pieces)


def unpack_rest_kernel(final_ref, pieces_ref, states_ref, out_ref):
    peers, half = pieces_ref.shape[0], pieces_ref.shape[2]
    for p in range(peers):
        out_ref[0, p] = final_ref[(2 * p + 1) * half : (2 * p + 2) * half, :]
        out_ref[1:, p] = pieces_ref[p].astype(F32)


def unpack_rest(final, pieces, states):
    slots, peers, piece, width = states.shape
    half = piece // 2
    return pl.pallas_call(
        unpack_rest_kernel,
        grid=(peers // PEER_TILE,),
        in_specs=[
            pl.BlockSpec((PEER_TILE * piece, width), lambda p: (p, 0)),
            pl.BlockSpec((PEER_TILE, slots - 1, half, width), lambda p: (p, 0, 0, 0)),
            pl.BlockSpec(memory_space=pl.ANY),
        ],
        out_specs=pl.BlockSpec((slots, PEER_TILE, half, width), lambda p: (0, p, 1, 0)),
        out_shape=jax.ShapeDtypeStruct(states.shape, F32),
        input_output_aliases={2: 0},
        compiler_params=pltpu.CompilerParams(dimension_semantics=("arbitrary",)),
        name="unpack_rest",
    )(final, pieces, states)


def combine_kernel(place_ref, decay_ref, *refs):
    peers, count = decay_ref.shape[1], decay_ref.shape[0]
    count = decay_ref.shape[0]
    scr, end_scr, enter_scr = refs[-3:]
    entering_refs = refs[-4 - count : -4]
    final_ref = refs[-4]
    inputs = refs[: -4 - count]
    end_refs = inputs[:count]
    peers = (len(inputs) - count) // 2
    upper, lower = inputs[count : count + peers], inputs[count + peers :]
    half = lower[0].shape[0]
    chain = place_ref[1]
    for hop in range(peers):
        peer = lax.rem(place_ref[0] - hop + peers, peers)
        at = pl.multiple_of(peer * 2 * half, 16)
        scr[pl.ds(at, half), :] = upper[hop][0]
        scr[pl.ds(at + half, half), :] = lower[hop][...]
    for hop in range(count):
        end_scr[lax.rem(chain - hop + count, count)] = end_refs[hop][...]
    state = scr[...].astype(F32).T
    for k in range(count):
        enter_scr[k] = state.astype(BF16)
        state = state * decay_ref[k : k + 1, :] + end_scr[k].astype(F32)
    for hop in range(count):
        entering_refs[hop][...] = enter_scr[lax.rem(chain + hop, count)]
    final_ref[...] = state.T


def combine(place, decay, ends, upper, lower):
    count = len(ends)
    whole = pl.BlockSpec(memory_space=pltpu.VMEM)
    half, width = lower[0].shape
    rows, columns = ends[0].shape
    outs = pl.pallas_call(
        combine_kernel,
        grid=(1,),
        in_specs=[
            pl.BlockSpec(memory_space=pltpu.SMEM),
            pl.BlockSpec(decay.shape, lambda t: (0, 0)),
        ]
        + [pl.BlockSpec((rows, columns), lambda t: (0, 0))] * count
        + [pl.BlockSpec((1, half, width), lambda t: (0, 0, 0))] * len(upper)
        + [pl.BlockSpec((half, width), lambda t: (0, 0))] * len(lower),
        out_specs=[pl.BlockSpec((rows, columns), lambda t: (0, 0))] * count
        + [pl.BlockSpec((columns, rows), lambda t: (0, 0))],
        out_shape=[jax.ShapeDtypeStruct((rows, columns), BF16)] * count
        + [jax.ShapeDtypeStruct((columns, rows), F32)],
        scratch_shapes=[
            pltpu.VMEM((columns, rows), BF16),
            pltpu.VMEM((count, rows, columns), BF16),
            pltpu.VMEM((count, rows, columns), BF16),
        ],
        name="combine",
    )(place, decay, *ends, *upper, *lower)
    return outs[:count], outs[count]


def share_kernel(
    place_ref,
    every_ref,
    end_ref,
    kept_ref,
    kept_next_ref,
    state_end_ref,
    state_kept_ref,
    state_next_ref,
    raw_ref,
    bias_ref,
    rate_ref,
    out_ref,
    step_ref,
    moved_ref,
    table_ref,
):
    taps = out_ref.shape[0]
    inner = end_ref.shape[1]
    outer = state_end_ref.shape[1]
    channels = inner + outer
    own, slots = place_ref[0], place_ref[5]
    peers, _, padded, width = every_ref.shape
    rows = peers * padded
    mark_at = width - width % LANES - LANES
    marks = []
    for tap in range(taps):
        lanes = every_ref[:, tap, :, mark_at:].astype(F32).reshape(rows, width - mark_at)
        marks.append(lanes[:, width - mark_at - 1 :])
    target = marks[0] * slots.astype(F32) + marks[1]
    columns = table_ref.shape[1]
    lane = lax.broadcasted_iota(jnp.int32, (rows, columns), 1).astype(F32)
    source = lax.broadcasted_iota(jnp.int32, (rows, columns), 0).astype(F32)
    found = jnp.sum(jnp.where(target == lane, source, 0.0), axis=0, keepdims=True)
    table_ref[...] = jnp.broadcast_to(found, table_ref.shape).astype(jnp.int32)
    lane = lax.broadcasted_iota(jnp.int32, (rows, LANES), 1)
    mine = (target == (own * slots + lane).astype(F32)) & (lane < slots)
    pick = jnp.where(mine, marks[2], 0.0).astype(BF16)
    firsts = []
    for tap in range(taps):
        source_rows = every_ref[:, tap].astype(F32).reshape(rows, width).astype(BF16)
        moved = dot(pick, source_rows, ((0,), (0,)))[:padded]
        moved_ref[tap] = moved.astype(BF16)
        firsts.append(moved[:1])
    low_block, high_block, start, length = (
        place_ref[1],
        place_ref[2],
        place_ref[3],
        place_ref[4],
    )
    out_ref[:, :inner] = end_ref[16 - taps :, :]
    out_ref[:, inner:channels] = state_end_ref[16 - taps :, :]
    here = lax.broadcasted_iota(jnp.int32, (16, 1), 0)
    wanted = length - taps - start

    def kept_rows(low_ref, high_ref):
        low = low_ref[...].astype(F32)
        high = high_ref[...].astype(F32)
        found = []
        for i in range(taps):
            in_low = (low_block * 16 + here) == (wanted + i)
            in_high = ((high_block * 16 + here) == (wanted + i)) & (high_block > low_block)
            picked = jnp.where(in_low, low, 0.0) + jnp.where(in_high, high, 0.0)
            found.append(jnp.sum(picked, axis=0, keepdims=True))
        return jnp.concatenate(found, axis=0).astype(BF16)

    out_ref[:, channels : channels + inner] = kept_rows(kept_ref, kept_next_ref)
    out_ref[:, channels + inner : 2 * channels] = kept_rows(state_kept_ref, state_next_ref)
    out_ref[:, 2 * channels : 2 * channels + width] = jnp.concatenate(firsts, axis=0).astype(BF16)
    count = step_ref.shape[0]
    heads = raw_ref.shape[1]
    positions = start + lax.broadcasted_iota(jnp.int32, (count, heads), 0)
    raw = raw_ref[...].astype(F32) + bias_ref[...]
    step = jnp.maximum(raw, 0.0) + jnp.log1p(jnp.exp(-jnp.abs(raw)))
    step = jnp.where(positions < length, step, 0.0)
    step = jnp.concatenate([step, jnp.zeros((count, LANES - heads), F32)], axis=1)
    step_ref[...] = step
    total = jnp.sum(step * rate_ref[...], axis=0, keepdims=True)
    high = total.astype(BF16).astype(F32)
    middle = (total - high).astype(BF16).astype(F32)
    rest = total - high - middle
    parts = jnp.concatenate([high, middle, rest], axis=0)
    out_ref[:, 2 * channels + width :] = parts.astype(BF16)


def share(place, slots, every, rows, state_rows, step_raw, step_bias, rate):
    peers, taps, padded, width = every.shape
    length, inner = rows.shape
    outer = state_rows.shape[1]
    heads = step_raw.shape[1]
    last = length // 16 - 1
    total = 2 * (inner + outer) + width + LANES
    lanes = pl.cdiv(peers * slots, LANES) * LANES
    return pl.pallas_call(
        share_kernel,
        grid_spec=pltpu.PrefetchScalarGridSpec(
            num_scalar_prefetch=1,
            grid=(1,),
            in_specs=[
                pl.BlockSpec(every.shape, lambda t, c: (0, 0, 0, 0)),
                pl.BlockSpec((16, inner), lambda t, c: (last, 0)),
                pl.BlockSpec((16, inner), lambda t, c: (c[1], 0)),
                pl.BlockSpec((16, inner), lambda t, c: (c[2], 0)),
                pl.BlockSpec((16, outer), lambda t, c: (last, 0)),
                pl.BlockSpec((16, outer), lambda t, c: (c[1], 0)),
                pl.BlockSpec((16, outer), lambda t, c: (c[2], 0)),
                pl.BlockSpec((length, heads), lambda t, c: (0, 0)),
                pl.BlockSpec((1, heads), lambda t, c: (0, 0)),
                pl.BlockSpec((1, LANES), lambda t, c: (0, 0)),
            ],
            out_specs=[
                pl.BlockSpec((taps, total), lambda t, c: (0, 0)),
                pl.BlockSpec((length, LANES), lambda t, c: (0, 0)),
                pl.BlockSpec((taps, padded, width), lambda t, c: (0, 0, 0)),
                pl.BlockSpec((8, lanes), lambda t, c: (0, 0)),
            ],
        ),
        out_shape=[
            jax.ShapeDtypeStruct((taps, total), BF16),
            jax.ShapeDtypeStruct((length, LANES), F32),
            jax.ShapeDtypeStruct((taps, padded, width), BF16),
            jax.ShapeDtypeStruct((8, lanes), jnp.int32),
        ],
        name="share",
    )(
        place,
        every,
        rows,
        rows,
        rows,
        state_rows,
        state_rows,
        state_rows,
        step_raw,
        step_bias,
        rate,
    )


def tail_kernel(
    chain_ref, shared_ref, moved_ref, tail_ref, inner_ref, outer_ref, decay_ref
):
    chain = chain_ref[0]
    count, taps = shared_ref.shape[:2]
    slots, inner_local = inner_ref.shape[1:]
    outer_local = outer_ref.shape[2]
    channels = tail_ref.shape[1]
    inner = count * inner_local
    at = 2 * channels
    window = jnp.concatenate(
        [shared_ref[s, :, at : at + inner_local] for s in range(count)]
        + [
            shared_ref[s, :, at + inner_local : at + inner_local + outer_local]
            for s in range(count)
        ],
        axis=1,
    ).astype(F32)
    earlier = shared_ref[jnp.maximum(chain - 1, 0), :, :channels].astype(F32)
    tail = jnp.where(chain == 0, window, earlier)
    tail_ref[...] = jnp.concatenate([jnp.zeros((8 - taps, channels), F32), tail], axis=0)
    kept = shared_ref[0, :, channels:at].astype(F32)
    for s in range(1, count):
        kept = kept + shared_ref[s, :, channels:at].astype(F32)
    own_inner = jnp.zeros((taps, inner_local), F32)
    own_outer = jnp.zeros((taps, outer_local), F32)
    for s in range(count):
        mine = chain == s
        inner_at, outer_at = s * inner_local, inner + s * outer_local
        own_inner = jnp.where(mine, kept[:, inner_at : inner_at + inner_local], own_inner)
        own_outer = jnp.where(mine, kept[:, outer_at : outer_at + outer_local], own_outer)
    width = inner_local + outer_local
    top = lax.broadcasted_iota(jnp.int32, (moved_ref.shape[1], 1), 0) == 0
    for tap in range(taps):
        moved = moved_ref[tap].astype(F32)
        both = jnp.where(top, own_inner[tap : tap + 1], moved[:, :inner_local])
        inner_ref[tap] = both.astype(BF16)[:slots]
        both = jnp.where(top, own_outer[tap : tap + 1], moved[:, inner_local:width])
        outer_ref[tap] = both.astype(BF16)[:slots]
    logs = []
    for s in range(count):
        parts = shared_ref[s, :, shared_ref.shape[2] - LANES :].astype(F32)
        logs.append(jnp.sum(parts, axis=0, keepdims=True))
    logs = jnp.concatenate(logs + [jnp.zeros((8 - count, LANES), F32)] * (count < 8), axis=0)
    columns = decay_ref.shape[1]
    head = lax.broadcasted_iota(jnp.int32, (LANES, columns), 0)
    lane = lax.broadcasted_iota(jnp.int32, (LANES, columns), 1)
    local_heads = columns // HEAD_DIM
    pick = (head == chain * local_heads + lane // HEAD_DIM).astype(F32)
    spread = dot(logs, pick, precision=lax.Precision.HIGHEST)
    decay_ref[...] = jnp.exp2(spread[:count])


def tails(chain, shared, moved, slots, channels, inner_local, outer_local, columns):
    count, taps = shared.shape[:2]
    whole = pl.BlockSpec(memory_space=pltpu.VMEM)
    return pl.pallas_call(
        tail_kernel,
        in_specs=[pl.BlockSpec(memory_space=pltpu.SMEM), whole, whole],
        out_shape=[
            jax.ShapeDtypeStruct((8, channels), F32),
            jax.ShapeDtypeStruct((taps, slots, inner_local), BF16),
            jax.ShapeDtypeStruct((taps, slots, outer_local), BF16),
            jax.ShapeDtypeStruct((count, columns), F32),
        ],
        name="tails",
    )(chain, shared, moved)


def exchange(value, axis):
    return lax.all_to_all(value, axis, split_axis=0, concat_axis=0, tiled=True)


def rotate(values, axis):
    count = lax.axis_size(axis)
    got = [values[0]] + [None] * (count - 1)
    for hop in sorted(range(1, count), key=lambda hop: abs(2 * hop - count)):
        pairs = [(source, (source + hop) % count) for source in range(count)]
        got[hop] = lax.ppermute(values[hop], axis, pairs)
    return got


def device_body(
    pool_states,
    inner_window,
    state_window,
    move_plan,
    active_mask,
    inputs_inner,
    inputs_state,
    gate_rows,
    step_raw,
    lengths,
    conv_weight,
    conv_bias,
    step_bias,
    decay_log,
    skip_weight,
    norm_weight,
):
    peers = lax.axis_size("req")
    own_peer = lax.axis_index("req").astype(jnp.int32)
    chain_size = lax.axis_size("seq")
    chain_index = lax.axis_index("seq").astype(jnp.int32)
    slots, local_heads = pool_states.shape[:2]
    columns = local_heads * HEAD_DIM
    piece = columns // peers
    taps = KERNEL - 1
    inner_local = inner_window.shape[2]
    outer_local = state_window.shape[2]

    own = own_peer[None]
    packed = mark(
        move_plan,
        active_mask,
        inner_window.transpose(1, 0, 2),
        state_window.transpose(1, 0, 2),
        peers,
    )
    every = exchange(packed, "req")
    pool_pieces = pool_states.reshape(slots, peers, piece, STATE_DIM)
    spread_a = rotate(pack(own, active_mask, pool_pieces), "req")
    spread_b = exchange(pack_rest(active_mask, pool_pieces), "req")

    rows = inputs_inner[0]
    state_rows = inputs_state[0]
    local_length, inner_dim = rows.shape
    channels = inner_dim + state_rows.shape[1]
    start = chain_index * local_length
    length = lengths[0]
    last_tile = local_length // 16 - 1
    low_block = jnp.clip((length - taps - start) // 16, 0, last_tile)
    high_block = jnp.minimum(low_block + 1, last_tile)
    heads = decay_log.shape[0]
    rate = jnp.pad(-LOG2E * jnp.exp(decay_log), (0, LANES - heads))[None]
    payload, step, moved, table = share(
        jnp.stack([own_peer, low_block, high_block, start, length, jnp.int32(slots)]),
        slots,
        every,
        rows,
        state_rows,
        step_raw[0],
        step_bias[None],
        rate,
    )
    shared = lax.all_gather(payload, "seq", axis=0)
    chain = chain_index[None]
    tail, new_inner, new_outer, own_decay = tails(
        chain, shared, moved, slots, channels, inner_local, outer_local, columns
    )

    moved_a = rotate(reorder(own, table, spread_a), "req")

    part, local_end, read_rows, decay = block_parts(
        chain,
        tail,
        rows,
        state_rows,
        step,
        rate,
        conv_weight,
        conv_bias[None],
        jnp.repeat(skip_weight, HEAD_DIM)[None],
        chain_size,
    )
    own_ends = rotate(local_end, "seq")

    rest, first = reorder_rest(own, table, spread_b)
    first_b = rotate(first, "req")
    rest_b = exchange(rest, "req")

    place = jnp.stack([own_peer, chain_index])
    entering, final = combine(place, own_decay, own_ends, moved_a, first_b)
    incoming = rotate(entering, "seq")
    finish_place = jnp.stack([start, length, chain_index])
    mixer_out = finish(
        finish_place,
        part,
        gate_rows[0],
        read_rows,
        decay,
        norm_weight[None],
        incoming,
    )
    states = unpack(place, final, moved_a)
    new_states = unpack_rest(final, rest_b, states).reshape(pool_states.shape)

    return (
        new_states,
        new_inner.transpose(1, 0, 2),
        new_outer.transpose(1, 0, 2),
        mixer_out[None],
    )


def solution(mesh):
    return jax.shard_map(
        device_body,
        mesh=mesh,
        in_specs=(
            P("req", "seq", None, None),
            P("req", None, "seq"),
            P("req", None, "seq"),
            P("req", None),
            P("req"),
            P("req", "seq", None),
            P("req", "seq", None),
            P("req", "seq", None),
            P("req", "seq", None),
            P("req"),
            P(),
            P(),
            P(),
            P(),
            P(),
            P(),
        ),
        out_specs=(
            P("req", "seq", None, None),
            P("req", None, "seq"),
            P("req", None, "seq"),
            P("req", "seq", None),
        ),
        check_vma=False,
    )
```

```python
import functools
import math

import jax
import jax.numpy as jnp
from jax import lax
from jax.experimental import pallas as pl
from jax.experimental.pallas import tpu as pltpu
from jax.sharding import PartitionSpec as P


HEAD_DIM = 64
STATE_DIM = 128
KERNEL = 4
BLOCK_LEN = 256
GROUP = 8
HALF = BLOCK_LEN // 2
GROUP_DIM = GROUP * HEAD_DIM
PAIR_DIM = 2 * HEAD_DIM
LANES = 128
TILE = 128
SLOT_TILE = 4
SLOT_PAD = 16
PEER_TILE = 2
EPSILON = 1e-05
LOG2E = math.log2(math.e)
F32 = jnp.float32
BF16 = jnp.bfloat16


def dot(a, b, dims=((1,), (0,)), precision=None):
    return lax.dot_general(a, b, (dims, ((), ())), precision=precision, preferred_element_type=F32)


def silu(v):
    return v / (1.0 + jnp.exp(-v))


def conv_silu(tail, rows, weight, bias_row):
    extended = jnp.concatenate([tail, rows.astype(F32)], axis=0)
    count = rows.shape[0]
    start = tail.shape[0] - KERNEL + 1
    running = bias_row + weight[0:1] * extended[start : start + count]
    for k in range(1, KERNEL):
        running = running + weight[k : k + 1] * extended[start + k : start + k + count]
    return silu(running)


def pair_of(columns, i, low):
    return jnp.where(low, columns[:, 2 * i : 2 * i + 1], columns[:, 2 * i + 1 : 2 * i + 2])


def block_kernel(
    chain_ref,
    tail_ref,
    prev_ref,
    rows_ref,
    state_tail_ref,
    state_prev_ref,
    state_rows_ref,
    step_ref,
    rate_ref,
    weight_ref,
    bias_ref,
    state_weight_ref,
    state_bias_ref,
    skip_ref,
    part_ref,
    end_ref,
    read_ref,
    decay_ref,
    scores_scr,
    cum_scr,
    cum_t_scr,
    to_end_scr,
    decay_scr,
    write_t_scr,
    offset_scr,
    carry_scr,
):
    block = pl.program_id(0)
    group = pl.program_id(1)
    first = block == 0

    @pl.when(group == 0)
    def _():
        state_tail = jnp.where(first, state_tail_ref[...], state_prev_ref[8:16, :].astype(F32))
        mixed = conv_silu(state_tail, state_rows_ref[...], state_weight_ref[...], state_bias_ref[...])
        write = mixed[:, :STATE_DIM]
        read = mixed[:, STATE_DIM:].astype(BF16)
        read_ref[...] = read
        write_b = write.astype(BF16)
        scores_scr[...] = dot(read, write_b, ((1,), (1,)))
        write_t_scr[...] = write_b.astype(F32).T.astype(BF16)
        row = lax.broadcasted_iota(jnp.int32, (BLOCK_LEN, BLOCK_LEN), 0)
        col = lax.broadcasted_iota(jnp.int32, (BLOCK_LEN, BLOCK_LEN), 1)
        triangle = (row >= col).astype(F32)
        step = step_ref[...]
        cum = dot(triangle, step * rate_ref[...], precision=lax.Precision.HIGHEST)
        cum_scr[...] = cum
        cum_t_scr[...] = cum.T
        last = cum[BLOCK_LEN - 1 :, :]
        to_end_scr[...] = jnp.exp2(last - cum) * step
        decay_scr[...] = jnp.exp2(cum)
        offset = jnp.where(first, 0.0, offset_scr[0:1, :])
        decay_ref[...] = jnp.exp2(offset + cum)
        offset_scr[0:1, :] = offset + last

    shift = lax.rem(LANES - group * GROUP, LANES)
    cum = pltpu.roll(cum_scr[...], shift, 1)
    step = pltpu.roll(step_ref[...], shift, 1)
    to_end = pltpu.roll(to_end_scr[...], shift, 1)
    decay = pltpu.roll(decay_scr[...], shift, 1)
    cum_t = cum_t_scr[pl.ds(pl.multiple_of(group * GROUP, GROUP), GROUP), :]
    read = read_ref[...]
    write_t = write_t_scr[...]
    carry = jnp.where(first, 0.0, carry_scr[group])
    carry_b = carry.astype(BF16)
    low = lax.broadcasted_iota(jnp.int32, (1, PAIR_DIM), 1) < HEAD_DIM
    causal = lax.broadcasted_iota(jnp.int32, (HALF, HALF), 0) >= lax.broadcasted_iota(
        jnp.int32, (HALF, HALF), 1
    )
    scores_top = scores_scr[0:HALF, 0:HALF]
    scores_left = scores_scr[HALF:, 0:HALF]
    scores_right = scores_scr[HALF:, HALF:]

    def head_weights(i):
        later = cum[:, i : i + 1]
        earlier = cum_t[i : i + 1, :]
        gap_top = jnp.where(causal, later[:HALF] - earlier[:, :HALF], -1e30)
        gap_left = later[HALF:] - earlier[:, :HALF]
        gap_right = jnp.where(causal, later[HALF:] - earlier[:, HALF:], -1e30)
        top = (scores_top * jnp.exp2(gap_top)).astype(BF16)
        left = (scores_left * jnp.exp2(gap_left)).astype(BF16)
        right = (scores_right * jnp.exp2(gap_right)).astype(BF16)
        return top, jnp.concatenate([left, right], axis=1)

    for i in range(GROUP // 2):
        span = slice(i * PAIR_DIM, (i + 1) * PAIR_DIM)
        tail = jnp.where(first, tail_ref[:, span], prev_ref[8:16, span].astype(F32))
        mixed = conv_silu(tail, rows_ref[:, span], weight_ref[:, span], bias_ref[:, span])
        value = mixed.astype(BF16).astype(F32)
        stepped = (pair_of(step, i, low) * value).astype(BF16)
        scaled = (pair_of(to_end, i, low) * value).astype(BF16)
        stepped_low = jnp.where(low, stepped, jnp.zeros_like(stepped))
        stepped_high = jnp.where(low, jnp.zeros_like(stepped), stepped)
        top_0, bottom_0 = head_weights(2 * i)
        top_1, bottom_1 = head_weights(2 * i + 1)
        intra_top = dot(top_0, stepped_low[:HALF]) + dot(top_1, stepped_high[:HALF])
        intra_bottom = dot(bottom_0, stepped_low) + dot(bottom_1, stepped_high)
        inter = dot(read, carry_b[:, span]) * pair_of(decay, i, low)
        direct = inter + skip_ref[:, span] * value
        part_ref[0:HALF, span] = intra_top + direct[:HALF]
        part_ref[HALF:, span] = intra_bottom + direct[HALF:]
        kept = pair_of(decay[BLOCK_LEN - 1 :, :], i, low) * carry[:, span]
        ending = kept + dot(write_t, scaled)
        carry_scr[group, :, span] = ending
        end_ref[0, :, span] = ending.astype(BF16)


def block_parts(chain, tail, rows, state_rows, step, rate, weight, bias_row, skip_row, ends):
    length = rows.shape[0]
    channels = rows.shape[1]
    blocks = length // BLOCK_LEN
    groups = channels // GROUP_DIM
    end_groups = groups // ends
    state_dim = state_rows.shape[1]
    state_at = channels // state_dim
    per_block = BLOCK_LEN // 16

    def before(b):
        return jnp.maximum(b * per_block - 1, 0)

    def end_at(b, g, chain):
        return lax.rem(g // end_groups - chain[0] + ends, ends), 0, lax.rem(g, end_groups)

    return pl.pallas_call(
        block_kernel,
        grid_spec=pltpu.PrefetchScalarGridSpec(
        num_scalar_prefetch=1,
        grid=(blocks, groups),
        in_specs=[
            pl.BlockSpec((8, GROUP_DIM), lambda b, g, c: (0, g)),
            pl.BlockSpec((16, GROUP_DIM), lambda b, g, c: (before(b), g)),
            pl.BlockSpec((BLOCK_LEN, GROUP_DIM), lambda b, g, c: (b, g)),
            pl.BlockSpec((8, state_dim), lambda b, g, c: (0, state_at)),
            pl.BlockSpec((16, state_dim), lambda b, g, c: (before(b), 0)),
            pl.BlockSpec((BLOCK_LEN, state_dim), lambda b, g, c: (b, 0)),
            pl.BlockSpec((BLOCK_LEN, LANES), lambda b, g, c: (b, 0)),
            pl.BlockSpec((1, LANES), lambda b, g, c: (0, 0)),
            pl.BlockSpec((KERNEL, GROUP_DIM), lambda b, g, c: (0, g)),
            pl.BlockSpec((1, GROUP_DIM), lambda b, g, c: (0, g)),
            pl.BlockSpec((KERNEL, state_dim), lambda b, g, c: (0, state_at)),
            pl.BlockSpec((1, state_dim), lambda b, g, c: (0, state_at)),
            pl.BlockSpec((1, GROUP_DIM), lambda b, g, c: (0, g)),
        ],
        out_specs=[
            pl.BlockSpec((BLOCK_LEN, GROUP_DIM), lambda b, g, c: (b, g)),
            pl.BlockSpec((1, STATE_DIM, GROUP_DIM), end_at),
            pl.BlockSpec((BLOCK_LEN, STATE_DIM), lambda b, g, c: (b, 0)),
            pl.BlockSpec((BLOCK_LEN, LANES), lambda b, g, c: (b, 0)),
        ],
        scratch_shapes=[
            pltpu.VMEM((BLOCK_LEN, BLOCK_LEN), F32),
            pltpu.VMEM((BLOCK_LEN, LANES), F32),
            pltpu.VMEM((LANES, BLOCK_LEN), F32),
            pltpu.VMEM((BLOCK_LEN, LANES), F32),
            pltpu.VMEM((BLOCK_LEN, LANES), F32),
            pltpu.VMEM((STATE_DIM, BLOCK_LEN), BF16),
            pltpu.VMEM((8, LANES), F32),
            pltpu.VMEM((groups, STATE_DIM, GROUP_DIM), F32),
        ],
        ),
        out_shape=[
            jax.ShapeDtypeStruct((length, channels), F32),
            jax.ShapeDtypeStruct((ends, STATE_DIM, channels // ends), BF16),
            jax.ShapeDtypeStruct((length, STATE_DIM), BF16),
            jax.ShapeDtypeStruct((length, LANES), F32),
        ],
        compiler_params=pltpu.CompilerParams(dimension_semantics=("arbitrary", "arbitrary")),
        cost_estimate=pl.CostEstimate(
            flops=6_000_000_000, bytes_accessed=20_000_000, transcendentals=10_000_000
        ),
        name="block_parts",
    )(
        chain,
        tail,
        rows,
        rows,
        tail,
        state_rows,
        state_rows,
        step,
        rate,
        weight,
        bias_row,
        weight,
        bias_row,
        skip_row,
    )


def finish_kernel(
    place_ref, part_ref, gate_ref, read_ref, decay_ref, norm_ref, *refs
):
    state_refs, out_ref, gated_scr, state_scr = refs[:-3], refs[-3], refs[-2], refs[-1]
    tile = pl.program_id(0)
    chunks, _, width = state_scr.shape

    @pl.when(tile == 0)
    def _():
        for hop in range(chunks):
            state_scr[lax.rem(place_ref[2] - hop + chunks, chunks)] = state_refs[hop][...]

    positions = (
        place_ref[0] + tile * TILE + lax.broadcasted_iota(jnp.int32, (TILE, PAIR_DIM), 0)
    )
    valid = (positions < place_ref[1]).astype(F32)
    low = lax.broadcasted_iota(jnp.int32, (1, PAIR_DIM), 1) < HEAD_DIM
    read = read_ref[...]
    decay = decay_ref[...]
    total = jnp.zeros((TILE, PAIR_DIM), F32)
    for chunk in range(chunks):
        for i in range(width // PAIR_DIM):
            pair = chunk * (width // PAIR_DIM) + i
            span = slice(pair * PAIR_DIM, (pair + 1) * PAIR_DIM)
            inter = dot(read, state_scr[chunk, :, i * PAIR_DIM : (i + 1) * PAIR_DIM])
            y = part_ref[:, span] + inter * pair_of(decay, pair, low)
            y = (y * valid).astype(BF16).astype(F32)
            gated = y * silu(gate_ref[:, span].astype(F32))
            gated_scr[:, span] = gated
            total = total + gated * gated
    channels = chunks * width
    mean = jnp.sum(total, axis=1, keepdims=True) * (1.0 / channels)
    scale = lax.rsqrt(mean + EPSILON)
    for pair in range(channels // PAIR_DIM):
        span = slice(pair * PAIR_DIM, (pair + 1) * PAIR_DIM)
        out_ref[:, span] = (gated_scr[:, span] * scale * norm_ref[:, span]).astype(BF16)


def finish(place, part, gate, read, decay, norm_row, states):
    length, channels = part.shape
    return pl.pallas_call(
        finish_kernel,
        grid=(length // TILE,),
        in_specs=[
            pl.BlockSpec(memory_space=pltpu.SMEM),
            pl.BlockSpec((TILE, channels), lambda t: (t, 0)),
            pl.BlockSpec((TILE, channels), lambda t: (t, 0)),
            pl.BlockSpec((TILE, STATE_DIM), lambda t: (t, 0)),
            pl.BlockSpec((TILE, LANES), lambda t: (t, 0)),
            pl.BlockSpec((1, channels), lambda t: (0, 0)),
        ]
        + [pl.BlockSpec(state.shape, lambda t: (0, 0)) for state in states],
        out_specs=pl.BlockSpec((TILE, channels), lambda t: (t, 0)),
        out_shape=jax.ShapeDtypeStruct((length, channels), BF16),
        scratch_shapes=[
            pltpu.VMEM((TILE, channels), F32),
            pltpu.VMEM((len(states),) + states[0].shape, BF16),
        ],
        compiler_params=pltpu.CompilerParams(dimension_semantics=("arbitrary",)),
        cost_estimate=pl.CostEstimate(
            flops=3_000_000_000, bytes_accessed=16_000_000, transcendentals=4_000_000
        ),
        name="finish",
    )(place, part, gate, read, decay, norm_row, *states)


def mark_kernel(plan_ref, mask_ref, inner_ref, outer_ref, out_ref, scr):
    peers, padded, total = out_ref.shape
    taps, slots = inner_ref.shape[:2]
    width = inner_ref.shape[2] + outer_ref.shape[2]
    capacity = most_per_pair(slots, peers)
    scr[:, :width] = jnp.zeros((peers * padded, width), F32)
    scr[:, width:] = jnp.full((peers * padded, total - width), -1.0, F32)
    windows = []
    for tap in range(taps):
        both = [inner_ref[tap].astype(F32), outer_ref[tap].astype(F32)]
        windows.append(jnp.concatenate(both, axis=1))
    lane = lax.broadcasted_iota(jnp.int32, (1, LANES), 1)
    peer_marks = jnp.zeros((1, LANES), F32)
    slot_marks = jnp.zeros((1, LANES), F32)
    for slot in range(slots):
        peer, target = plan_ref[slot, 0], plan_ref[slot, 1]
        rank = jnp.int32(0)
        for earlier in range(slot):
            rank = rank + (plan_ref[earlier, 0] == peer).astype(jnp.int32)
        keep = mask_ref[slot].astype(F32)
        for tap in range(taps):
            tag = jnp.full((1, total - width), (target + tap * SLOT_PAD).astype(F32))
            row = jnp.concatenate([windows[tap][slot : slot + 1] * keep, tag], axis=1)
            scr[pl.ds(peer * padded + tap * capacity + rank, 1), :] = row
        peer_marks = jnp.where(lane == slot, peer.astype(F32), peer_marks)
        slot_marks = jnp.where(lane == slot, target.astype(F32), slot_marks)
    for peer in range(peers):
        at = peer * padded + taps * capacity
        scr[at : at + 1, :LANES] = peer_marks
        scr[at + 1 : at + 2, :LANES] = slot_marks
        out_ref[peer] = scr[peer * padded : (peer + 1) * padded, :].astype(BF16)


def most_per_pair(slots, peers):
    return (2 * slots + peers - 1) // peers


def mark(plan, mask, inner, outer, peers):
    taps, slots = inner.shape[:2]
    width = inner.shape[2] + outer.shape[2]
    whole = pl.BlockSpec(memory_space=pltpu.VMEM)
    scalar = pl.BlockSpec(memory_space=pltpu.SMEM)
    total = width + LANES - width % LANES
    padded = pl.cdiv(taps * most_per_pair(slots, peers) + 2, 16) * 16
    return pl.pallas_call(
        mark_kernel,
        in_specs=[scalar, scalar, whole, whole],
        out_shape=jax.ShapeDtypeStruct((peers, padded, total), BF16),
        scratch_shapes=[pltpu.VMEM((peers * padded, total), F32)],
        name="mark",
    )(plan, mask, inner, outer)


def pack_kernel(own_ref, mask_ref, state_ref, *out_refs):
    first_slot = pl.program_id(0) * SLOT_TILE
    peers = state_ref.shape[1]
    for j in range(SLOT_TILE):
        keep = mask_ref[jnp.minimum(first_slot + j, mask_ref.shape[0] - 1)].astype(F32)
        for hop in range(len(out_refs)):
            peer = lax.rem(own_ref[0] + hop, peers)
            out_refs[hop][j] = (state_ref[j, peer] * keep).astype(BF16)


def pack(own, mask, states):
    slots, peers, piece, width = states.shape
    half = piece // 2
    steps = pl.cdiv(slots, SLOT_TILE)
    return pl.pallas_call(
        pack_kernel,
        grid=(steps,),
        in_specs=[
            pl.BlockSpec(memory_space=pltpu.SMEM),
            pl.BlockSpec(memory_space=pltpu.SMEM),
            pl.BlockSpec((SLOT_TILE, peers, half, width), lambda t: (t, 0, 0, 0)),
        ],
        out_specs=[pl.BlockSpec((SLOT_TILE, half, width), lambda t: (t, 0, 0))] * peers,
        out_shape=[jax.ShapeDtypeStruct((slots, half, width), BF16)] * peers,
        compiler_params=pltpu.CompilerParams(dimension_semantics=("arbitrary",)),
        name="pack",
    )(own, mask, states)


def pack_rest_kernel(mask_ref, state_ref, out_ref):
    first_slot = pl.program_id(0) * SLOT_TILE
    for j in range(SLOT_TILE):
        keep = mask_ref[jnp.minimum(first_slot + j, mask_ref.shape[0] - 1)].astype(F32)
        out_ref[:, j] = (state_ref[j] * keep).astype(BF16)


def pack_rest(mask, states):
    slots, peers, piece, width = states.shape
    half = piece // 2
    steps = pl.cdiv(slots, SLOT_TILE)
    return pl.pallas_call(
        pack_rest_kernel,
        grid=(steps,),
        in_specs=[
            pl.BlockSpec(memory_space=pltpu.SMEM),
            pl.BlockSpec((SLOT_TILE, peers, half, width), lambda t: (t, 0, 1, 0)),
        ],
        out_specs=pl.BlockSpec((peers, SLOT_TILE, half, width), lambda t: (0, t, 0, 0)),
        out_shape=jax.ShapeDtypeStruct((peers, slots, half, width), BF16),
        compiler_params=pltpu.CompilerParams(dimension_semantics=("arbitrary",)),
        name="pack_rest",
    )(mask, states)


def source_of(table_ref, target):
    code = table_ref[0, target]
    peer = lax.div(code, SLOT_PAD)
    return peer, code - peer * SLOT_PAD


def reorder_kernel(own_ref, table_ref, *refs):
    peers = (len(refs) - 1) // 2
    in_refs, out_refs, scr = refs[:peers], refs[peers:-1], refs[-1]
    slots = in_refs[0].shape[0]
    own = own_ref[0]
    for hop in range(peers):
        scr[hop] = in_refs[hop][...]
    for hop in range(peers):
        base = lax.rem(own + hop, peers) * slots

        def move(slot, unused):
            peer, index = source_of(table_ref, base + slot)
            out_refs[hop][slot] = scr[lax.rem(own - peer + peers, peers), index]
            return unused

        lax.fori_loop(0, slots, move, 0)


def reorder(own, table, pieces):
    slots, half, width = pieces[0].shape
    count = len(pieces)
    whole = pl.BlockSpec((slots, half, width), lambda t: (0, 0, 0))
    scalar = pl.BlockSpec(memory_space=pltpu.SMEM)
    return pl.pallas_call(
        reorder_kernel,
        grid=(1,),
        in_specs=[scalar, scalar] + [whole] * count,
        out_specs=[whole] * count,
        out_shape=[jax.ShapeDtypeStruct((slots, half, width), BF16)] * count,
        scratch_shapes=[pltpu.VMEM((count, slots, half, width), BF16)],
        name="reorder",
    )(own, table, *pieces)


def reorder_rest_kernel(own_ref, table_ref, in_ref, *out_refs):
    rest_ref, first_refs = out_refs[0], out_refs[1:]
    peers, slots = in_ref.shape[:2]
    own = own_ref[0]
    for hop in range(peers):
        target = lax.rem(own + hop, peers)
        peer, index = source_of(table_ref, target * slots)
        first_refs[hop][...] = in_ref[peer, index]

        def move(slot, unused):
            peer, index = source_of(table_ref, hop * slots + slot)
            rest_ref[hop, slot - 1] = in_ref[peer, index]
            return unused

        lax.fori_loop(1, slots, move, 0)


def reorder_rest(own, table, pieces):
    peers, slots, half, width = pieces.shape
    scalar = pl.BlockSpec(memory_space=pltpu.SMEM)
    outs = pl.pallas_call(
        reorder_rest_kernel,
        grid=(1,),
        in_specs=[scalar, scalar, pl.BlockSpec(pieces.shape, lambda t: (0, 0, 0, 0))],
        out_specs=[pl.BlockSpec((peers, slots - 1, half, width), lambda t: (0, 0, 0, 0))]
        + [pl.BlockSpec((half, width), lambda t: (0, 0))] * peers,
        out_shape=[jax.ShapeDtypeStruct((peers, slots - 1, half, width), BF16)]
        + [jax.ShapeDtypeStruct((half, width), BF16)] * peers,
        name="reorder_rest",
    )(own, table, pieces)
    return outs[0], outs[1:]


def unpack_kernel(place_ref, final_ref, *refs):
    pieces, out_ref = refs[:-1], refs[-1]
    step = pl.program_id(0)
    peers, half = out_ref.shape[1:3]
    for hop in range(peers):
        peer = lax.rem(place_ref[0] - hop + peers, peers)
        for j in range(SLOT_TILE):
            out_ref[j, peer] = pieces[hop][j].astype(F32)

    @pl.when(step == 0)
    def _():
        for p in range(peers):
            out_ref[0, p] = final_ref[2 * p * half : (2 * p + 1) * half, :]


def unpack(place, final, pieces):
    peers = len(pieces)
    slots, half, width = pieces[0].shape
    return pl.pallas_call(
        unpack_kernel,
        grid=(pl.cdiv(slots, SLOT_TILE),),
        in_specs=[
            pl.BlockSpec(memory_space=pltpu.SMEM),
            pl.BlockSpec(final.shape, lambda t: (0, 0)),
        ]
        + [pl.BlockSpec((SLOT_TILE, half, width), lambda t: (t, 0, 0))] * peers,
        out_specs=pl.BlockSpec((SLOT_TILE, peers, half, width), lambda t: (t, 0, 0, 0)),
        out_shape=jax.ShapeDtypeStruct((slots, peers, 2 * half, width), F32),
        compiler_params=pltpu.CompilerParams(dimension_semantics=("arbitrary",)),
        name="unpack",
    )(place, final, *pieces)


def unpack_rest_kernel(final_ref, pieces_ref, states_ref, out_ref):
    peers, half = pieces_ref.shape[0], pieces_ref.shape[2]
    for p in range(peers):
        out_ref[0, p] = final_ref[(2 * p + 1) * half : (2 * p + 2) * half, :]
        out_ref[1:, p] = pieces_ref[p].astype(F32)


def unpack_rest(final, pieces, states):
    slots, peers, piece, width = states.shape
    half = piece // 2
    return pl.pallas_call(
        unpack_rest_kernel,
        grid=(peers // PEER_TILE,),
        in_specs=[
            pl.BlockSpec((PEER_TILE * piece, width), lambda p: (p, 0)),
            pl.BlockSpec((PEER_TILE, slots - 1, half, width), lambda p: (p, 0, 0, 0)),
            pl.BlockSpec(memory_space=pl.ANY),
        ],
        out_specs=pl.BlockSpec((slots, PEER_TILE, half, width), lambda p: (0, p, 1, 0)),
        out_shape=jax.ShapeDtypeStruct(states.shape, F32),
        input_output_aliases={2: 0},
        compiler_params=pltpu.CompilerParams(dimension_semantics=("arbitrary",)),
        name="unpack_rest",
    )(final, pieces, states)


def combine_kernel(place_ref, decay_ref, *refs):
    peers, count = decay_ref.shape[1], decay_ref.shape[0]
    count = decay_ref.shape[0]
    scr, end_scr, enter_scr = refs[-3:]
    entering_refs = refs[-4 - count : -4]
    final_ref = refs[-4]
    inputs = refs[: -4 - count]
    end_refs = inputs[:count]
    peers = (len(inputs) - count) // 2
    upper, lower = inputs[count : count + peers], inputs[count + peers :]
    half = lower[0].shape[0]
    chain = place_ref[1]
    for hop in range(peers):
        peer = lax.rem(place_ref[0] - hop + peers, peers)
        at = pl.multiple_of(peer * 2 * half, 16)
        scr[pl.ds(at, half), :] = upper[hop][0]
        scr[pl.ds(at + half, half), :] = lower[hop][...]
    for hop in range(count):
        end_scr[lax.rem(chain - hop + count, count)] = end_refs[hop][...]
    state = scr[...].astype(F32).T
    for k in range(count):
        enter_scr[k] = state.astype(BF16)
        state = state * decay_ref[k : k + 1, :] + end_scr[k].astype(F32)
    for hop in range(count):
        entering_refs[hop][...] = enter_scr[lax.rem(chain + hop, count)]
    final_ref[...] = state.T


def combine(place, decay, ends, upper, lower):
    count = len(ends)
    whole = pl.BlockSpec(memory_space=pltpu.VMEM)
    half, width = lower[0].shape
    rows, columns = ends[0].shape
    outs = pl.pallas_call(
        combine_kernel,
        grid=(1,),
        in_specs=[
            pl.BlockSpec(memory_space=pltpu.SMEM),
            pl.BlockSpec(decay.shape, lambda t: (0, 0)),
        ]
        + [pl.BlockSpec((rows, columns), lambda t: (0, 0))] * count
        + [pl.BlockSpec((1, half, width), lambda t: (0, 0, 0))] * len(upper)
        + [pl.BlockSpec((half, width), lambda t: (0, 0))] * len(lower),
        out_specs=[pl.BlockSpec((rows, columns), lambda t: (0, 0))] * count
        + [pl.BlockSpec((columns, rows), lambda t: (0, 0))],
        out_shape=[jax.ShapeDtypeStruct((rows, columns), BF16)] * count
        + [jax.ShapeDtypeStruct((columns, rows), F32)],
        scratch_shapes=[
            pltpu.VMEM((columns, rows), BF16),
            pltpu.VMEM((count, rows, columns), BF16),
            pltpu.VMEM((count, rows, columns), BF16),
        ],
        name="combine",
    )(place, decay, *ends, *upper, *lower)
    return outs[:count], outs[count]


def share_kernel(
    slot_count,
    place_ref,
    every_ref,
    end_ref,
    kept_ref,
    kept_next_ref,
    state_end_ref,
    state_kept_ref,
    state_next_ref,
    raw_ref,
    bias_ref,
    rate_ref,
    out_ref,
    step_ref,
    moved_ref,
    table_ref,
):
    taps = out_ref.shape[0]
    inner = end_ref.shape[1]
    outer = state_end_ref.shape[1]
    channels = inner + outer
    peers, packet, width = every_ref.shape
    padded = moved_ref.shape[1]
    slots = float(slot_count)
    rows = peers * packet
    everything = every_ref[...].astype(F32).reshape(rows, width)
    tags = everything[:, width - 1 :]
    lane = lax.broadcasted_iota(jnp.int32, (rows, LANES), 1).astype(F32)
    pick = (tags == lane).astype(BF16)
    moved = dot(pick, everything.astype(BF16), ((0,), (0,)))
    firsts = []
    for tap in range(taps):
        moved_ref[tap] = moved[tap * padded : (tap + 1) * padded].astype(BF16)
        firsts.append(moved[tap * padded : tap * padded + 1])
    at = taps * most_per_pair(slot_count, peers)
    peer_marks = [every_ref[p, at : at + 1, :LANES].astype(F32) for p in range(peers)]
    slot_marks = [every_ref[p, at + 1 : at + 2, :LANES].astype(F32) for p in range(peers)]
    target = jnp.concatenate(peer_marks, axis=0) * slots + jnp.concatenate(slot_marks, axis=0)
    columns = table_ref.shape[1]
    lane = lax.broadcasted_iota(jnp.int32, (peers, columns), 1).astype(F32)
    code = lax.broadcasted_iota(jnp.int32, (peers, columns), 0).astype(F32) * SLOT_PAD
    found = jnp.zeros((peers, columns), F32)
    for slot in range(slot_count):
        found = found + jnp.where(target[:, slot : slot + 1] == lane, code + slot, 0.0)
    found = jnp.sum(found, axis=0, keepdims=True)
    table_ref[...] = jnp.broadcast_to(found, table_ref.shape).astype(jnp.int32)
    low_block, high_block, start, length = (
        place_ref[0],
        place_ref[1],
        place_ref[2],
        place_ref[3],
    )
    out_ref[:, :inner] = end_ref[16 - taps :, :]
    out_ref[:, inner:channels] = state_end_ref[16 - taps :, :]
    here = lax.broadcasted_iota(jnp.int32, (16, 1), 0)
    wanted = length - taps - start

    def kept_rows(low_ref, high_ref):
        low = low_ref[...].astype(F32)
        high = high_ref[...].astype(F32)
        found = []
        for i in range(taps):
            in_low = (low_block * 16 + here) == (wanted + i)
            in_high = ((high_block * 16 + here) == (wanted + i)) & (high_block > low_block)
            picked = jnp.where(in_low, low, 0.0) + jnp.where(in_high, high, 0.0)
            found.append(jnp.sum(picked, axis=0, keepdims=True))
        return jnp.concatenate(found, axis=0).astype(BF16)

    out_ref[:, channels : channels + inner] = kept_rows(kept_ref, kept_next_ref)
    out_ref[:, channels + inner : 2 * channels] = kept_rows(state_kept_ref, state_next_ref)
    out_ref[:, 2 * channels : 2 * channels + width] = jnp.concatenate(firsts, axis=0).astype(BF16)
    count = step_ref.shape[0]
    heads = raw_ref.shape[1]
    positions = start + lax.broadcasted_iota(jnp.int32, (count, heads), 0)
    raw = raw_ref[...].astype(F32) + bias_ref[...]
    step = jnp.maximum(raw, 0.0) + jnp.log1p(jnp.exp(-jnp.abs(raw)))
    step = jnp.where(positions < length, step, 0.0)
    step = jnp.concatenate([step, jnp.zeros((count, LANES - heads), F32)], axis=1)
    step_ref[...] = step
    total = jnp.sum(step * rate_ref[...], axis=0, keepdims=True)
    high = total.astype(BF16).astype(F32)
    middle = (total - high).astype(BF16).astype(F32)
    rest = total - high - middle
    parts = jnp.concatenate([high, middle, rest], axis=0)
    out_ref[:, 2 * channels + width :] = parts.astype(BF16)


def share(place, slots, every, rows, state_rows, step_raw, step_bias, rate):
    peers, _, width = every.shape
    taps, padded = KERNEL - 1, SLOT_PAD
    length, inner = rows.shape
    outer = state_rows.shape[1]
    heads = step_raw.shape[1]
    last = length // 16 - 1
    total = 2 * (inner + outer) + width + LANES
    lanes = pl.cdiv(peers * slots, LANES) * LANES
    return pl.pallas_call(
        functools.partial(share_kernel, slots),
        grid_spec=pltpu.PrefetchScalarGridSpec(
            num_scalar_prefetch=1,
            grid=(1,),
            in_specs=[
                pl.BlockSpec(every.shape, lambda t, c: (0, 0, 0)),
                pl.BlockSpec((16, inner), lambda t, c: (last, 0)),
                pl.BlockSpec((16, inner), lambda t, c: (c[0], 0)),
                pl.BlockSpec((16, inner), lambda t, c: (c[1], 0)),
                pl.BlockSpec((16, outer), lambda t, c: (last, 0)),
                pl.BlockSpec((16, outer), lambda t, c: (c[0], 0)),
                pl.BlockSpec((16, outer), lambda t, c: (c[1], 0)),
                pl.BlockSpec((length, heads), lambda t, c: (0, 0)),
                pl.BlockSpec((1, heads), lambda t, c: (0, 0)),
                pl.BlockSpec((1, LANES), lambda t, c: (0, 0)),
            ],
            out_specs=[
                pl.BlockSpec((taps, total), lambda t, c: (0, 0)),
                pl.BlockSpec((length, LANES), lambda t, c: (0, 0)),
                pl.BlockSpec((taps, padded, width), lambda t, c: (0, 0, 0)),
                pl.BlockSpec((8, lanes), lambda t, c: (0, 0)),
            ],
        ),
        out_shape=[
            jax.ShapeDtypeStruct((taps, total), BF16),
            jax.ShapeDtypeStruct((length, LANES), F32),
            jax.ShapeDtypeStruct((taps, padded, width), BF16),
            jax.ShapeDtypeStruct((8, lanes), jnp.int32),
        ],
        name="share",
    )(
        place,
        every,
        rows,
        rows,
        rows,
        state_rows,
        state_rows,
        state_rows,
        step_raw,
        step_bias,
        rate,
    )


def tail_kernel(
    chain_ref, shared_ref, moved_ref, tail_ref, inner_ref, outer_ref, decay_ref
):
    chain = chain_ref[0]
    count, taps = shared_ref.shape[:2]
    slots, inner_local = inner_ref.shape[1:]
    outer_local = outer_ref.shape[2]
    channels = tail_ref.shape[1]
    inner = count * inner_local
    at = 2 * channels
    window = jnp.concatenate(
        [shared_ref[s, :, at : at + inner_local] for s in range(count)]
        + [
            shared_ref[s, :, at + inner_local : at + inner_local + outer_local]
            for s in range(count)
        ],
        axis=1,
    ).astype(F32)
    earlier = shared_ref[jnp.maximum(chain - 1, 0), :, :channels].astype(F32)
    tail = jnp.where(chain == 0, window, earlier)
    tail_ref[...] = jnp.concatenate([jnp.zeros((8 - taps, channels), F32), tail], axis=0)
    kept = shared_ref[0, :, channels:at].astype(F32)
    for s in range(1, count):
        kept = kept + shared_ref[s, :, channels:at].astype(F32)
    own_inner = jnp.zeros((taps, inner_local), F32)
    own_outer = jnp.zeros((taps, outer_local), F32)
    for s in range(count):
        mine = chain == s
        inner_at, outer_at = s * inner_local, inner + s * outer_local
        own_inner = jnp.where(mine, kept[:, inner_at : inner_at + inner_local], own_inner)
        own_outer = jnp.where(mine, kept[:, outer_at : outer_at + outer_local], own_outer)
    width = inner_local + outer_local
    top = lax.broadcasted_iota(jnp.int32, (moved_ref.shape[1], 1), 0) == 0
    for tap in range(taps):
        moved = moved_ref[tap].astype(F32)
        both = jnp.where(top, own_inner[tap : tap + 1], moved[:, :inner_local])
        inner_ref[tap] = both.astype(BF16)[:slots]
        both = jnp.where(top, own_outer[tap : tap + 1], moved[:, inner_local:width])
        outer_ref[tap] = both.astype(BF16)[:slots]
    logs = []
    for s in range(count):
        parts = shared_ref[s, :, shared_ref.shape[2] - LANES :].astype(F32)
        logs.append(jnp.sum(parts, axis=0, keepdims=True))
    logs = jnp.concatenate(logs + [jnp.zeros((8 - count, LANES), F32)] * (count < 8), axis=0)
    columns = decay_ref.shape[1]
    head = lax.broadcasted_iota(jnp.int32, (LANES, columns), 0)
    lane = lax.broadcasted_iota(jnp.int32, (LANES, columns), 1)
    local_heads = columns // HEAD_DIM
    pick = (head == chain * local_heads + lane // HEAD_DIM).astype(F32)
    spread = dot(logs, pick, precision=lax.Precision.HIGHEST)
    decay_ref[...] = jnp.exp2(spread[:count])


def tails(chain, shared, moved, slots, channels, inner_local, outer_local, columns):
    count, taps = shared.shape[:2]
    whole = pl.BlockSpec(memory_space=pltpu.VMEM)
    return pl.pallas_call(
        tail_kernel,
        in_specs=[pl.BlockSpec(memory_space=pltpu.SMEM), whole, whole],
        out_shape=[
            jax.ShapeDtypeStruct((8, channels), F32),
            jax.ShapeDtypeStruct((taps, slots, inner_local), BF16),
            jax.ShapeDtypeStruct((taps, slots, outer_local), BF16),
            jax.ShapeDtypeStruct((count, columns), F32),
        ],
        name="tails",
    )(chain, shared, moved)


def exchange(value, axis):
    return lax.all_to_all(value, axis, split_axis=0, concat_axis=0, tiled=True)


def rotate(values, axis):
    count = lax.axis_size(axis)
    got = [values[0]] + [None] * (count - 1)
    for hop in sorted(range(1, count), key=lambda hop: abs(2 * hop - count)):
        pairs = [(source, (source + hop) % count) for source in range(count)]
        got[hop] = lax.ppermute(values[hop], axis, pairs)
    return got


def device_body(
    pool_states,
    inner_window,
    state_window,
    move_plan,
    active_mask,
    inputs_inner,
    inputs_state,
    gate_rows,
    step_raw,
    lengths,
    conv_weight,
    conv_bias,
    step_bias,
    decay_log,
    skip_weight,
    norm_weight,
):
    peers = lax.axis_size("req")
    own_peer = lax.axis_index("req").astype(jnp.int32)
    chain_size = lax.axis_size("seq")
    chain_index = lax.axis_index("seq").astype(jnp.int32)
    slots, local_heads = pool_states.shape[:2]
    columns = local_heads * HEAD_DIM
    piece = columns // peers
    taps = KERNEL - 1
    inner_local = inner_window.shape[2]
    outer_local = state_window.shape[2]

    own = own_peer[None]
    packed = mark(
        move_plan,
        active_mask,
        inner_window.transpose(1, 0, 2),
        state_window.transpose(1, 0, 2),
        peers,
    )
    every = exchange(packed, "req")
    pool_pieces = pool_states.reshape(slots, peers, piece, STATE_DIM)
    spread_a = rotate(pack(own, active_mask, pool_pieces), "req")
    spread_b = exchange(pack_rest(active_mask, pool_pieces), "req")

    rows = inputs_inner[0]
    state_rows = inputs_state[0]
    local_length, inner_dim = rows.shape
    channels = inner_dim + state_rows.shape[1]
    start = chain_index * local_length
    length = lengths[0]
    last_tile = local_length // 16 - 1
    low_block = jnp.clip((length - taps - start) // 16, 0, last_tile)
    high_block = jnp.minimum(low_block + 1, last_tile)
    heads = decay_log.shape[0]
    rate = jnp.pad(-LOG2E * jnp.exp(decay_log), (0, LANES - heads))[None]
    payload, step, moved, table = share(
        jnp.stack([low_block, high_block, start, length]),
        slots,
        every,
        rows,
        state_rows,
        step_raw[0],
        step_bias[None],
        rate,
    )
    shared = lax.all_gather(payload, "seq", axis=0)
    chain = chain_index[None]
    tail, new_inner, new_outer, own_decay = tails(
        chain, shared, moved, slots, channels, inner_local, outer_local, columns
    )

    moved_a = rotate(reorder(own, table, spread_a), "req")

    part, local_end, read_rows, decay = block_parts(
        chain,
        tail,
        rows,
        state_rows,
        step,
        rate,
        conv_weight,
        conv_bias[None],
        jnp.repeat(skip_weight, HEAD_DIM)[None],
        chain_size,
    )
    own_ends = rotate(local_end, "seq")

    rest, first = reorder_rest(own, table, spread_b)
    first_b = rotate(first, "req")
    rest_b = exchange(rest, "req")

    place = jnp.stack([own_peer, chain_index])
    entering, final = combine(place, own_decay, own_ends, moved_a, first_b)
    incoming = rotate(entering, "seq")
    finish_place = jnp.stack([start, length, chain_index])
    mixer_out = finish(
        finish_place,
        part,
        gate_rows[0],
        read_rows,
        decay,
        norm_weight[None],
        incoming,
    )
    states = unpack(place, final, moved_a)
    new_states = unpack_rest(final, rest_b, states).reshape(pool_states.shape)

    return (
        new_states,
        new_inner.transpose(1, 0, 2),
        new_outer.transpose(1, 0, 2),
        mixer_out[None],
    )


def solution(mesh):
    return jax.shard_map(
        device_body,
        mesh=mesh,
        in_specs=(
            P("req", "seq", None, None),
            P("req", None, "seq"),
            P("req", None, "seq"),
            P("req", None),
            P("req"),
            P("req", "seq", None),
            P("req", "seq", None),
            P("req", "seq", None),
            P("req", "seq", None),
            P("req"),
            P(),
            P(),
            P(),
            P(),
            P(),
            P(),
        ),
        out_specs=(
            P("req", "seq", None, None),
            P("req", None, "seq"),
            P("req", None, "seq"),
            P("req", "seq", None),
        ),
        check_vma=False,
    )
```

```python
import functools
import math

import jax
import jax.numpy as jnp
from jax import lax
from jax.experimental import pallas as pl
from jax.experimental.pallas import tpu as pltpu
from jax.sharding import PartitionSpec as P


HEAD_DIM = 64
STATE_DIM = 128
KERNEL = 4
BLOCK_LEN = 256
GROUP = 8
HALF = BLOCK_LEN // 2
GROUP_DIM = GROUP * HEAD_DIM
PAIR_DIM = 2 * HEAD_DIM
LANES = 128
TILE = 128
SLOT_TILE = 4
SLOT_PAD = 16
PEER_TILE = 2
EPSILON = 1e-05
LOG2E = math.log2(math.e)
F32 = jnp.float32
BF16 = jnp.bfloat16


def dot(a, b, dims=((1,), (0,)), precision=None):
    return lax.dot_general(a, b, (dims, ((), ())), precision=precision, preferred_element_type=F32)


def silu(v):
    return v / (1.0 + jnp.exp(-v))


def conv_silu(tail, rows, weight, bias_row):
    extended = jnp.concatenate([tail, rows.astype(F32)], axis=0)
    count = rows.shape[0]
    start = tail.shape[0] - KERNEL + 1
    running = bias_row + weight[0:1] * extended[start : start + count]
    for k in range(1, KERNEL):
        running = running + weight[k : k + 1] * extended[start + k : start + k + count]
    return silu(running)


def pair_of(columns, i, low):
    return jnp.where(low, columns[:, 2 * i : 2 * i + 1], columns[:, 2 * i + 1 : 2 * i + 2])


def block_kernel(
    chain_ref,
    tail_ref,
    prev_ref,
    rows_ref,
    state_tail_ref,
    state_prev_ref,
    state_rows_ref,
    step_ref,
    rate_ref,
    weight_ref,
    bias_ref,
    state_weight_ref,
    state_bias_ref,
    skip_ref,
    part_ref,
    end_ref,
    read_ref,
    decay_ref,
    scores_scr,
    cum_scr,
    cum_t_scr,
    to_end_scr,
    decay_scr,
    write_t_scr,
    offset_scr,
    carry_scr,
):
    block = pl.program_id(0)
    group = pl.program_id(1)
    first = block == 0

    @pl.when(group == 0)
    def _():
        state_tail = jnp.where(first, state_tail_ref[...], state_prev_ref[8:16, :].astype(F32))
        mixed = conv_silu(state_tail, state_rows_ref[...], state_weight_ref[...], state_bias_ref[...])
        write = mixed[:, :STATE_DIM]
        read = mixed[:, STATE_DIM:].astype(BF16)
        read_ref[...] = read
        write_b = write.astype(BF16)
        scores_scr[...] = dot(read, write_b, ((1,), (1,)))
        write_t_scr[...] = write_b.astype(F32).T.astype(BF16)
        row = lax.broadcasted_iota(jnp.int32, (BLOCK_LEN, BLOCK_LEN), 0)
        col = lax.broadcasted_iota(jnp.int32, (BLOCK_LEN, BLOCK_LEN), 1)
        triangle = (row >= col).astype(F32)
        step = step_ref[...]
        cum = dot(triangle, step * rate_ref[...], precision=lax.Precision.HIGHEST)
        cum_scr[...] = cum
        cum_t_scr[...] = cum.T
        last = cum[BLOCK_LEN - 1 :, :]
        to_end_scr[...] = jnp.exp2(last - cum) * step
        decay_scr[...] = jnp.exp2(cum)
        offset = jnp.where(first, 0.0, offset_scr[0:1, :])
        decay_ref[...] = jnp.exp2(offset + cum)
        offset_scr[0:1, :] = offset + last

    shift = lax.rem(LANES - group * GROUP, LANES)
    cum = pltpu.roll(cum_scr[...], shift, 1)
    step = pltpu.roll(step_ref[...], shift, 1)
    to_end = pltpu.roll(to_end_scr[...], shift, 1)
    decay = pltpu.roll(decay_scr[...], shift, 1)
    cum_t = cum_t_scr[pl.ds(pl.multiple_of(group * GROUP, GROUP), GROUP), :]
    read = read_ref[...]
    write_t = write_t_scr[...]
    carry = jnp.where(first, 0.0, carry_scr[group])
    carry_b = carry.astype(BF16)
    low = lax.broadcasted_iota(jnp.int32, (1, PAIR_DIM), 1) < HEAD_DIM
    causal = lax.broadcasted_iota(jnp.int32, (HALF, HALF), 0) >= lax.broadcasted_iota(
        jnp.int32, (HALF, HALF), 1
    )
    scores_top = scores_scr[0:HALF, 0:HALF]
    scores_left = scores_scr[HALF:, 0:HALF]
    scores_right = scores_scr[HALF:, HALF:]

    def head_weights(i):
        later = cum[:, i : i + 1]
        earlier = cum_t[i : i + 1, :]
        gap_top = jnp.where(causal, later[:HALF] - earlier[:, :HALF], -1e30)
        gap_left = later[HALF:] - earlier[:, :HALF]
        gap_right = jnp.where(causal, later[HALF:] - earlier[:, HALF:], -1e30)
        top = (scores_top * jnp.exp2(gap_top)).astype(BF16)
        left = (scores_left * jnp.exp2(gap_left)).astype(BF16)
        right = (scores_right * jnp.exp2(gap_right)).astype(BF16)
        return top, jnp.concatenate([left, right], axis=1)

    for i in range(GROUP // 2):
        span = slice(i * PAIR_DIM, (i + 1) * PAIR_DIM)
        tail = jnp.where(first, tail_ref[:, span], prev_ref[8:16, span].astype(F32))
        mixed = conv_silu(tail, rows_ref[:, span], weight_ref[:, span], bias_ref[:, span])
        value = mixed.astype(BF16).astype(F32)
        stepped = (pair_of(step, i, low) * value).astype(BF16)
        scaled = (pair_of(to_end, i, low) * value).astype(BF16)
        stepped_low = jnp.where(low, stepped, jnp.zeros_like(stepped))
        stepped_high = jnp.where(low, jnp.zeros_like(stepped), stepped)
        top_0, bottom_0 = head_weights(2 * i)
        top_1, bottom_1 = head_weights(2 * i + 1)
        intra_top = dot(top_0, stepped_low[:HALF]) + dot(top_1, stepped_high[:HALF])
        intra_bottom = dot(bottom_0, stepped_low) + dot(bottom_1, stepped_high)
        inter = dot(read, carry_b[:, span]) * pair_of(decay, i, low)
        direct = inter + skip_ref[:, span] * value
        part_ref[0:HALF, span] = intra_top + direct[:HALF]
        part_ref[HALF:, span] = intra_bottom + direct[HALF:]
        kept = pair_of(decay[BLOCK_LEN - 1 :, :], i, low) * carry[:, span]
        ending = kept + dot(write_t, scaled)
        carry_scr[group, :, span] = ending
        end_ref[0, :, span] = ending.astype(BF16)


def block_parts(chain, tail, rows, state_rows, step, rate, weight, bias_row, skip_row, ends):
    length = rows.shape[0]
    channels = rows.shape[1]
    blocks = length // BLOCK_LEN
    groups = channels // GROUP_DIM
    end_groups = groups // ends
    state_dim = state_rows.shape[1]
    state_at = channels // state_dim
    per_block = BLOCK_LEN // 16

    def before(b):
        return jnp.maximum(b * per_block - 1, 0)

    def end_at(b, g, chain):
        return lax.rem(g // end_groups - chain[0] + ends, ends), 0, lax.rem(g, end_groups)

    return pl.pallas_call(
        block_kernel,
        grid_spec=pltpu.PrefetchScalarGridSpec(
        num_scalar_prefetch=1,
        grid=(blocks, groups),
        in_specs=[
            pl.BlockSpec((8, GROUP_DIM), lambda b, g, c: (0, g)),
            pl.BlockSpec((16, GROUP_DIM), lambda b, g, c: (before(b), g)),
            pl.BlockSpec((BLOCK_LEN, GROUP_DIM), lambda b, g, c: (b, g)),
            pl.BlockSpec((8, state_dim), lambda b, g, c: (0, state_at)),
            pl.BlockSpec((16, state_dim), lambda b, g, c: (before(b), 0)),
            pl.BlockSpec((BLOCK_LEN, state_dim), lambda b, g, c: (b, 0)),
            pl.BlockSpec((BLOCK_LEN, LANES), lambda b, g, c: (b, 0)),
            pl.BlockSpec((1, LANES), lambda b, g, c: (0, 0)),
            pl.BlockSpec((KERNEL, GROUP_DIM), lambda b, g, c: (0, g)),
            pl.BlockSpec((1, GROUP_DIM), lambda b, g, c: (0, g)),
            pl.BlockSpec((KERNEL, state_dim), lambda b, g, c: (0, state_at)),
            pl.BlockSpec((1, state_dim), lambda b, g, c: (0, state_at)),
            pl.BlockSpec((1, GROUP_DIM), lambda b, g, c: (0, g)),
        ],
        out_specs=[
            pl.BlockSpec((BLOCK_LEN, GROUP_DIM), lambda b, g, c: (b, g)),
            pl.BlockSpec((1, STATE_DIM, GROUP_DIM), end_at),
            pl.BlockSpec((BLOCK_LEN, STATE_DIM), lambda b, g, c: (b, 0)),
            pl.BlockSpec((BLOCK_LEN, LANES), lambda b, g, c: (b, 0)),
        ],
        scratch_shapes=[
            pltpu.VMEM((BLOCK_LEN, BLOCK_LEN), F32),
            pltpu.VMEM((BLOCK_LEN, LANES), F32),
            pltpu.VMEM((LANES, BLOCK_LEN), F32),
            pltpu.VMEM((BLOCK_LEN, LANES), F32),
            pltpu.VMEM((BLOCK_LEN, LANES), F32),
            pltpu.VMEM((STATE_DIM, BLOCK_LEN), BF16),
            pltpu.VMEM((8, LANES), F32),
            pltpu.VMEM((groups, STATE_DIM, GROUP_DIM), F32),
        ],
        ),
        out_shape=[
            jax.ShapeDtypeStruct((length, channels), F32),
            jax.ShapeDtypeStruct((ends, STATE_DIM, channels // ends), BF16),
            jax.ShapeDtypeStruct((length, STATE_DIM), BF16),
            jax.ShapeDtypeStruct((length, LANES), F32),
        ],
        compiler_params=pltpu.CompilerParams(dimension_semantics=("arbitrary", "arbitrary")),
        cost_estimate=pl.CostEstimate(
            flops=6_000_000_000, bytes_accessed=20_000_000, transcendentals=10_000_000
        ),
        name="block_parts",
    )(
        chain,
        tail,
        rows,
        rows,
        tail,
        state_rows,
        state_rows,
        step,
        rate,
        weight,
        bias_row,
        weight,
        bias_row,
        skip_row,
    )


def finish_kernel(
    place_ref, part_ref, gate_ref, read_ref, decay_ref, norm_ref, *refs
):
    state_refs, out_ref, gated_scr, state_scr = refs[:-3], refs[-3], refs[-2], refs[-1]
    tile = pl.program_id(0)
    chunks, _, width = state_scr.shape

    @pl.when(tile == 0)
    def _():
        for hop in range(chunks):
            state_scr[lax.rem(place_ref[2] - hop + chunks, chunks)] = state_refs[hop][...]

    positions = (
        place_ref[0] + tile * TILE + lax.broadcasted_iota(jnp.int32, (TILE, PAIR_DIM), 0)
    )
    valid = (positions < place_ref[1]).astype(F32)
    low = lax.broadcasted_iota(jnp.int32, (1, PAIR_DIM), 1) < HEAD_DIM
    read = read_ref[...]
    decay = decay_ref[...]
    total = jnp.zeros((TILE, PAIR_DIM), F32)
    for chunk in range(chunks):
        for i in range(width // PAIR_DIM):
            pair = chunk * (width // PAIR_DIM) + i
            span = slice(pair * PAIR_DIM, (pair + 1) * PAIR_DIM)
            inter = dot(read, state_scr[chunk, :, i * PAIR_DIM : (i + 1) * PAIR_DIM])
            y = part_ref[:, span] + inter * pair_of(decay, pair, low)
            y = (y * valid).astype(BF16).astype(F32)
            gated = y * silu(gate_ref[:, span].astype(F32))
            gated_scr[:, span] = gated
            total = total + gated * gated
    channels = chunks * width
    mean = jnp.sum(total, axis=1, keepdims=True) * (1.0 / channels)
    scale = lax.rsqrt(mean + EPSILON)
    for pair in range(channels // PAIR_DIM):
        span = slice(pair * PAIR_DIM, (pair + 1) * PAIR_DIM)
        out_ref[:, span] = (gated_scr[:, span] * scale * norm_ref[:, span]).astype(BF16)


def finish(place, part, gate, read, decay, norm_row, states):
    length, channels = part.shape
    return pl.pallas_call(
        finish_kernel,
        grid=(length // TILE,),
        in_specs=[
            pl.BlockSpec(memory_space=pltpu.SMEM),
            pl.BlockSpec((TILE, channels), lambda t: (t, 0)),
            pl.BlockSpec((TILE, channels), lambda t: (t, 0)),
            pl.BlockSpec((TILE, STATE_DIM), lambda t: (t, 0)),
            pl.BlockSpec((TILE, LANES), lambda t: (t, 0)),
            pl.BlockSpec((1, channels), lambda t: (0, 0)),
        ]
        + [pl.BlockSpec(state.shape, lambda t: (0, 0)) for state in states],
        out_specs=pl.BlockSpec((TILE, channels), lambda t: (t, 0)),
        out_shape=jax.ShapeDtypeStruct((length, channels), BF16),
        scratch_shapes=[
            pltpu.VMEM((TILE, channels), F32),
            pltpu.VMEM((len(states),) + states[0].shape, BF16),
        ],
        compiler_params=pltpu.CompilerParams(dimension_semantics=("arbitrary",)),
        cost_estimate=pl.CostEstimate(
            flops=3_000_000_000, bytes_accessed=16_000_000, transcendentals=4_000_000
        ),
        name="finish",
    )(place, part, gate, read, decay, norm_row, *states)


def mark_kernel(plan_ref, mask_ref, inner_ref, outer_ref, out_ref, scr):
    peers, padded, total = out_ref.shape
    taps, slots = inner_ref.shape[:2]
    width = inner_ref.shape[2] + outer_ref.shape[2]
    capacity = most_per_pair(slots, peers)
    scr[:, :width] = jnp.zeros((peers * padded, width), F32)
    scr[:, width:] = jnp.full((peers * padded, total - width), -1.0, F32)
    windows = []
    for tap in range(taps):
        both = [inner_ref[tap].astype(F32), outer_ref[tap].astype(F32)]
        windows.append(jnp.concatenate(both, axis=1))
    lane = lax.broadcasted_iota(jnp.int32, (1, LANES), 1)
    peer_marks = jnp.zeros((1, LANES), F32)
    slot_marks = jnp.zeros((1, LANES), F32)
    for slot in range(slots):
        peer, target = plan_ref[0, slot], plan_ref[1, slot]
        rank = jnp.int32(0)
        for earlier in range(slot):
            rank = rank + (plan_ref[0, earlier] == peer).astype(jnp.int32)
        keep = mask_ref[slot].astype(F32)
        for tap in range(taps):
            tag = jnp.full((1, total - width), (target + tap * SLOT_PAD).astype(F32))
            row = jnp.concatenate([windows[tap][slot : slot + 1] * keep, tag], axis=1)
            scr[pl.ds(peer * padded + tap * capacity + rank, 1), :] = row
        peer_marks = jnp.where(lane == slot, peer.astype(F32), peer_marks)
        slot_marks = jnp.where(lane == slot, target.astype(F32), slot_marks)
    for peer in range(peers):
        at = peer * padded + taps * capacity
        scr[at : at + 1, :LANES] = peer_marks
        scr[at + 1 : at + 2, :LANES] = slot_marks
        out_ref[peer] = scr[peer * padded : (peer + 1) * padded, :].astype(BF16)


def most_per_pair(slots, peers):
    return (2 * slots + peers - 1) // peers


def mark(plan, mask, inner, outer, peers):
    taps, slots = inner.shape[:2]
    width = inner.shape[2] + outer.shape[2]
    whole = pl.BlockSpec(memory_space=pltpu.VMEM)
    scalar = pl.BlockSpec(memory_space=pltpu.SMEM)
    total = width + LANES - width % LANES
    padded = pl.cdiv(taps * most_per_pair(slots, peers) + 2, 16) * 16
    return pl.pallas_call(
        mark_kernel,
        in_specs=[scalar, scalar, whole, whole],
        out_shape=jax.ShapeDtypeStruct((peers, padded, total), BF16),
        scratch_shapes=[pltpu.VMEM((peers * padded, total), F32)],
        name="mark",
    )(plan, mask, inner, outer)


def pack_kernel(own_ref, mask_ref, state_ref, *out_refs):
    first_slot = pl.program_id(0) * SLOT_TILE
    peers = state_ref.shape[1]
    for j in range(SLOT_TILE):
        keep = mask_ref[jnp.minimum(first_slot + j, mask_ref.shape[0] - 1)].astype(F32)
        for hop in range(len(out_refs)):
            peer = lax.rem(own_ref[0] + hop, peers)
            out_refs[hop][j] = (state_ref[j, peer] * keep).astype(BF16)


def pack(own, mask, states):
    slots, peers, piece, width = states.shape
    half = piece // 2
    steps = pl.cdiv(slots, SLOT_TILE)
    return pl.pallas_call(
        pack_kernel,
        grid=(steps,),
        in_specs=[
            pl.BlockSpec(memory_space=pltpu.SMEM),
            pl.BlockSpec(memory_space=pltpu.SMEM),
            pl.BlockSpec((SLOT_TILE, peers, half, width), lambda t: (t, 0, 0, 0)),
        ],
        out_specs=[pl.BlockSpec((SLOT_TILE, half, width), lambda t: (t, 0, 0))] * peers,
        out_shape=[jax.ShapeDtypeStruct((slots, half, width), BF16)] * peers,
        compiler_params=pltpu.CompilerParams(dimension_semantics=("arbitrary",)),
        name="pack",
    )(own, mask, states)


def pack_rest_kernel(mask_ref, state_ref, out_ref):
    first_slot = pl.program_id(0) * SLOT_TILE
    for j in range(SLOT_TILE):
        keep = mask_ref[jnp.minimum(first_slot + j, mask_ref.shape[0] - 1)].astype(F32)
        out_ref[:, j] = (state_ref[j] * keep).astype(BF16)


def pack_rest(mask, states):
    slots, peers, piece, width = states.shape
    half = piece // 2
    steps = pl.cdiv(slots, SLOT_TILE)
    return pl.pallas_call(
        pack_rest_kernel,
        grid=(steps,),
        in_specs=[
            pl.BlockSpec(memory_space=pltpu.SMEM),
            pl.BlockSpec((SLOT_TILE, peers, half, width), lambda t: (t, 0, 1, 0)),
        ],
        out_specs=pl.BlockSpec((peers, SLOT_TILE, half, width), lambda t: (0, t, 0, 0)),
        out_shape=jax.ShapeDtypeStruct((peers, slots, half, width), BF16),
        compiler_params=pltpu.CompilerParams(dimension_semantics=("arbitrary",)),
        name="pack_rest",
    )(mask, states)


def source_of(table_ref, target):
    code = table_ref[0, target]
    peer = lax.div(code, SLOT_PAD)
    return peer, code - peer * SLOT_PAD


def reorder_kernel(own_ref, table_ref, *refs):
    peers = (len(refs) - 2) // 2
    in_refs, rest_ref, first_refs, scr = (
        refs[:peers],
        refs[peers],
        refs[peers + 1 : -1],
        refs[-1],
    )
    slots = in_refs[0].shape[0]
    own = own_ref[0]
    for hop in range(peers):
        scr[lax.rem(own - hop + peers, peers)] = in_refs[hop][...]
    for hop in range(peers):
        peer, index = source_of(table_ref, lax.rem(own + hop, peers) * slots)
        first_refs[hop][...] = scr[peer, index]

        def move(slot, unused):
            peer, index = source_of(table_ref, hop * slots + slot)
            rest_ref[hop, slot - 1] = scr[peer, index]
            return unused

        lax.fori_loop(1, slots, move, 0)


def reorder(own, table, pieces):
    slots, half, width = pieces[0].shape
    peers = len(pieces)
    scalar = pl.BlockSpec(memory_space=pltpu.SMEM)
    outs = pl.pallas_call(
        reorder_kernel,
        grid=(1,),
        in_specs=[scalar, scalar]
        + [pl.BlockSpec((slots, half, width), lambda t: (0, 0, 0))] * peers,
        out_specs=[pl.BlockSpec((peers, slots - 1, half, width), lambda t: (0, 0, 0, 0))]
        + [pl.BlockSpec((half, width), lambda t: (0, 0))] * peers,
        out_shape=[jax.ShapeDtypeStruct((peers, slots - 1, half, width), BF16)]
        + [jax.ShapeDtypeStruct((half, width), BF16)] * peers,
        scratch_shapes=[pltpu.VMEM((peers, slots, half, width), BF16)],
        name="reorder",
    )(own, table, *pieces)
    return outs[0], outs[1:]


def reorder_rest_kernel(own_ref, table_ref, in_ref, *refs):
    peers, slots, half, _ = in_ref.shape
    upper_refs, first_refs, rest_refs = (
        refs[:peers],
        refs[peers : 2 * peers],
        refs[2 * peers :],
    )
    own = own_ref[0]
    for hop in range(peers):
        base = lax.rem(own + hop, peers) * slots
        peer, index = source_of(table_ref, base)
        first_refs[hop][:half, :] = upper_refs[hop][...]
        first_refs[hop][half:, :] = in_ref[peer, index]

        def move(slot, unused):
            peer, index = source_of(table_ref, base + slot)
            rest_refs[hop][slot - 1] = in_ref[peer, index]
            return unused

        lax.fori_loop(1, slots, move, 0)


def reorder_rest(own, table, pieces, upper):
    peers, slots, half, width = pieces.shape
    scalar = pl.BlockSpec(memory_space=pltpu.SMEM)
    outs = pl.pallas_call(
        reorder_rest_kernel,
        grid=(1,),
        in_specs=[scalar, scalar, pl.BlockSpec(pieces.shape, lambda t: (0, 0, 0, 0))]
        + [pl.BlockSpec((half, width), lambda t: (0, 0))] * peers,
        out_specs=[pl.BlockSpec((2 * half, width), lambda t: (0, 0))] * peers
        + [pl.BlockSpec((slots - 1, half, width), lambda t: (0, 0, 0))] * peers,
        out_shape=[jax.ShapeDtypeStruct((2 * half, width), BF16)] * peers
        + [jax.ShapeDtypeStruct((slots - 1, half, width), BF16)] * peers,
        name="reorder_rest",
    )(own, table, pieces, *upper)
    return outs[:peers], outs[peers:]


def unpack_kernel(final_ref, pieces_ref, out_ref):
    peers, half = pieces_ref.shape[0], pieces_ref.shape[2]
    for p in range(peers):
        out_ref[0, p] = final_ref[2 * p * half : (2 * p + 1) * half, :]
        out_ref[1:, p] = pieces_ref[p].astype(F32)


def unpack(final, pieces):
    peers, others, half, width = pieces.shape
    slots, piece = others + 1, 2 * half
    return pl.pallas_call(
        unpack_kernel,
        grid=(peers // PEER_TILE,),
        in_specs=[
            pl.BlockSpec((PEER_TILE * piece, width), lambda p: (p, 0)),
            pl.BlockSpec((PEER_TILE, others, half, width), lambda p: (p, 0, 0, 0)),
        ],
        out_specs=pl.BlockSpec((slots, PEER_TILE, half, width), lambda p: (0, p, 0, 0)),
        out_shape=jax.ShapeDtypeStruct((slots, peers, piece, width), F32),
        compiler_params=pltpu.CompilerParams(dimension_semantics=("arbitrary",)),
        name="unpack",
    )(final, pieces)


def unpack_rest_kernel(own_ref, final_ref, states_ref, *refs):
    piece_refs, out_ref = refs[:-1], refs[-1]
    step = pl.program_id(0)
    half = out_ref.shape[2]
    out_ref[0, 0] = final_ref[half:, :]
    for hop in range(len(piece_refs)):

        @pl.when(step == hop)
        def _():
            out_ref[1:, 0] = piece_refs[hop][...].astype(F32)


def unpack_rest(own, final, pieces, states):
    slots, peers, piece, width = states.shape
    half = piece // 2

    def from_peer(hop, own):
        return lax.rem(own[0] - hop + peers, peers)

    return pl.pallas_call(
        unpack_rest_kernel,
        grid_spec=pltpu.PrefetchScalarGridSpec(
            num_scalar_prefetch=1,
            grid=(peers,),
            in_specs=[
                pl.BlockSpec((piece, width), lambda h, own: (from_peer(h, own), 0)),
                pl.BlockSpec(memory_space=pl.ANY),
            ]
            + [pl.BlockSpec((slots - 1, half, width), lambda h, own: (0, 0, 0))] * peers,
            out_specs=pl.BlockSpec(
                (slots, 1, half, width), lambda h, own: (0, from_peer(h, own), 1, 0)
            ),
        ),
        out_shape=jax.ShapeDtypeStruct(states.shape, F32),
        input_output_aliases={2: 0},
        compiler_params=pltpu.CompilerParams(dimension_semantics=("arbitrary",)),
        name="unpack_rest",
    )(own, final, states, *pieces)


def combine_kernel(place_ref, decay_ref, *refs):
    count = decay_ref.shape[0]
    scr, end_scr, enter_scr = refs[-3:]
    entering_refs = refs[-4 - count : -4]
    final_ref = refs[-4]
    inputs = refs[: -4 - count]
    end_refs = inputs[:count]
    peers = len(inputs) - count
    first_refs = inputs[count:]
    piece = first_refs[0].shape[0]
    chain = place_ref[1]
    for hop in range(peers):
        peer = lax.rem(place_ref[0] - hop + peers, peers)
        scr[pl.ds(pl.multiple_of(peer * piece, 16), piece), :] = first_refs[hop][...]
    for hop in range(count):
        end_scr[lax.rem(chain - hop + count, count)] = end_refs[hop][...]
    state = scr[...].astype(F32).T
    for k in range(count):
        enter_scr[k] = state.astype(BF16)
        state = state * decay_ref[k : k + 1, :] + end_scr[k].astype(F32)
    for hop in range(count):
        entering_refs[hop][...] = enter_scr[lax.rem(chain + hop, count)]
    final_ref[...] = state.T


def combine(place, decay, ends, first):
    count = len(ends)
    whole = pl.BlockSpec(memory_space=pltpu.VMEM)
    rows, columns = ends[0].shape
    outs = pl.pallas_call(
        combine_kernel,
        grid=(1,),
        in_specs=[
            pl.BlockSpec(memory_space=pltpu.SMEM),
            pl.BlockSpec(decay.shape, lambda t: (0, 0)),
        ]
        + [pl.BlockSpec((rows, columns), lambda t: (0, 0))] * count
        + [pl.BlockSpec(first[0].shape, lambda t: (0, 0))] * len(first),
        out_specs=[pl.BlockSpec((rows, columns), lambda t: (0, 0))] * count
        + [pl.BlockSpec((columns, rows), lambda t: (0, 0))],
        out_shape=[jax.ShapeDtypeStruct((rows, columns), BF16)] * count
        + [jax.ShapeDtypeStruct((columns, rows), F32)],
        scratch_shapes=[
            pltpu.VMEM((columns, rows), BF16),
            pltpu.VMEM((count, rows, columns), BF16),
            pltpu.VMEM((count, rows, columns), BF16),
        ],
        name="combine",
    )(place, decay, *ends, *first)
    return outs[:count], outs[count]


def share_kernel(
    slot_count,
    place_ref,
    every_ref,
    end_ref,
    kept_ref,
    kept_next_ref,
    state_end_ref,
    state_kept_ref,
    state_next_ref,
    raw_ref,
    bias_ref,
    rate_ref,
    out_ref,
    step_ref,
    moved_ref,
    table_ref,
):
    taps = out_ref.shape[0]
    inner = end_ref.shape[1]
    outer = state_end_ref.shape[1]
    channels = inner + outer
    peers, packet, width = every_ref.shape
    padded = moved_ref.shape[1]
    slots = float(slot_count)
    rows = peers * packet
    everything = every_ref[...].astype(F32).reshape(rows, width)
    tags = everything[:, width - 1 :]
    lane = lax.broadcasted_iota(jnp.int32, (rows, LANES), 1).astype(F32)
    pick = (tags == lane).astype(BF16)
    moved = dot(pick, everything.astype(BF16), ((0,), (0,)))
    firsts = []
    for tap in range(taps):
        moved_ref[tap] = moved[tap * padded : (tap + 1) * padded].astype(BF16)
        firsts.append(moved[tap * padded : tap * padded + 1])
    at = taps * most_per_pair(slot_count, peers)
    peer_marks = [every_ref[p, at : at + 1, :LANES].astype(F32) for p in range(peers)]
    slot_marks = [every_ref[p, at + 1 : at + 2, :LANES].astype(F32) for p in range(peers)]
    target = jnp.concatenate(peer_marks, axis=0) * slots + jnp.concatenate(slot_marks, axis=0)
    columns = table_ref.shape[1]
    lane = lax.broadcasted_iota(jnp.int32, (peers, columns), 1).astype(F32)
    code = lax.broadcasted_iota(jnp.int32, (peers, columns), 0).astype(F32) * SLOT_PAD
    found = jnp.zeros((peers, columns), F32)
    for slot in range(slot_count):
        found = found + jnp.where(target[:, slot : slot + 1] == lane, code + slot, 0.0)
    found = jnp.sum(found, axis=0, keepdims=True)
    table_ref[...] = jnp.broadcast_to(found, table_ref.shape).astype(jnp.int32)
    low_block, high_block, start, length = (
        place_ref[0],
        place_ref[1],
        place_ref[2],
        place_ref[3],
    )
    out_ref[:, :inner] = end_ref[16 - taps :, :]
    out_ref[:, inner:channels] = state_end_ref[16 - taps :, :]
    here = lax.broadcasted_iota(jnp.int32, (16, 1), 0)
    wanted = length - taps - start

    def kept_rows(low_ref, high_ref):
        low = low_ref[...].astype(F32)
        high = high_ref[...].astype(F32)
        found = []
        for i in range(taps):
            in_low = (low_block * 16 + here) == (wanted + i)
            in_high = ((high_block * 16 + here) == (wanted + i)) & (high_block > low_block)
            picked = jnp.where(in_low, low, 0.0) + jnp.where(in_high, high, 0.0)
            found.append(jnp.sum(picked, axis=0, keepdims=True))
        return jnp.concatenate(found, axis=0).astype(BF16)

    out_ref[:, channels : channels + inner] = kept_rows(kept_ref, kept_next_ref)
    out_ref[:, channels + inner : 2 * channels] = kept_rows(state_kept_ref, state_next_ref)
    out_ref[:, 2 * channels : 2 * channels + width] = jnp.concatenate(firsts, axis=0).astype(BF16)
    count = step_ref.shape[0]
    heads = raw_ref.shape[1]
    positions = start + lax.broadcasted_iota(jnp.int32, (count, heads), 0)
    raw = raw_ref[...].astype(F32) + bias_ref[...]
    step = jnp.maximum(raw, 0.0) + jnp.log1p(jnp.exp(-jnp.abs(raw)))
    step = jnp.where(positions < length, step, 0.0)
    step = jnp.concatenate([step, jnp.zeros((count, LANES - heads), F32)], axis=1)
    step_ref[...] = step
    total = jnp.sum(step * rate_ref[...], axis=0, keepdims=True)
    high = total.astype(BF16).astype(F32)
    middle = (total - high).astype(BF16).astype(F32)
    rest = total - high - middle
    parts = jnp.concatenate([high, middle, rest], axis=0)
    out_ref[:, 2 * channels + width :] = parts.astype(BF16)


def share(place, slots, every, rows, state_rows, step_raw, step_bias, rate):
    peers, _, width = every.shape
    taps, padded = KERNEL - 1, SLOT_PAD
    length, inner = rows.shape
    outer = state_rows.shape[1]
    heads = step_raw.shape[1]
    last = length // 16 - 1
    total = 2 * (inner + outer) + width + LANES
    lanes = pl.cdiv(peers * slots, LANES) * LANES
    return pl.pallas_call(
        functools.partial(share_kernel, slots),
        grid_spec=pltpu.PrefetchScalarGridSpec(
            num_scalar_prefetch=1,
            grid=(1,),
            in_specs=[
                pl.BlockSpec(every.shape, lambda t, c: (0, 0, 0)),
                pl.BlockSpec((16, inner), lambda t, c: (last, 0)),
                pl.BlockSpec((16, inner), lambda t, c: (c[0], 0)),
                pl.BlockSpec((16, inner), lambda t, c: (c[1], 0)),
                pl.BlockSpec((16, outer), lambda t, c: (last, 0)),
                pl.BlockSpec((16, outer), lambda t, c: (c[0], 0)),
                pl.BlockSpec((16, outer), lambda t, c: (c[1], 0)),
                pl.BlockSpec((length, heads), lambda t, c: (0, 0)),
                pl.BlockSpec((1, heads), lambda t, c: (0, 0)),
                pl.BlockSpec((1, LANES), lambda t, c: (0, 0)),
            ],
            out_specs=[
                pl.BlockSpec((taps, total), lambda t, c: (0, 0)),
                pl.BlockSpec((length, LANES), lambda t, c: (0, 0)),
                pl.BlockSpec((taps, padded, width), lambda t, c: (0, 0, 0)),
                pl.BlockSpec((8, lanes), lambda t, c: (0, 0)),
            ],
        ),
        out_shape=[
            jax.ShapeDtypeStruct((taps, total), BF16),
            jax.ShapeDtypeStruct((length, LANES), F32),
            jax.ShapeDtypeStruct((taps, padded, width), BF16),
            jax.ShapeDtypeStruct((8, lanes), jnp.int32),
        ],
        name="share",
    )(
        place,
        every,
        rows,
        rows,
        rows,
        state_rows,
        state_rows,
        state_rows,
        step_raw,
        step_bias,
        rate,
    )


def tail_kernel(
    chain_ref, shared_ref, moved_ref, tail_ref, inner_ref, outer_ref, decay_ref
):
    chain = chain_ref[0]
    count, taps = shared_ref.shape[:2]
    slots, inner_local = inner_ref.shape[1:]
    outer_local = outer_ref.shape[2]
    channels = tail_ref.shape[1]
    inner = count * inner_local
    at = 2 * channels
    window = jnp.concatenate(
        [shared_ref[s, :, at : at + inner_local] for s in range(count)]
        + [
            shared_ref[s, :, at + inner_local : at + inner_local + outer_local]
            for s in range(count)
        ],
        axis=1,
    ).astype(F32)
    earlier = shared_ref[jnp.maximum(chain - 1, 0), :, :channels].astype(F32)
    tail = jnp.where(chain == 0, window, earlier)
    tail_ref[...] = jnp.concatenate([jnp.zeros((8 - taps, channels), F32), tail], axis=0)
    kept = shared_ref[0, :, channels:at].astype(F32)
    for s in range(1, count):
        kept = kept + shared_ref[s, :, channels:at].astype(F32)
    own_inner = jnp.zeros((taps, inner_local), F32)
    own_outer = jnp.zeros((taps, outer_local), F32)
    for s in range(count):
        mine = chain == s
        inner_at, outer_at = s * inner_local, inner + s * outer_local
        own_inner = jnp.where(mine, kept[:, inner_at : inner_at + inner_local], own_inner)
        own_outer = jnp.where(mine, kept[:, outer_at : outer_at + outer_local], own_outer)
    width = inner_local + outer_local
    top = lax.broadcasted_iota(jnp.int32, (moved_ref.shape[1], 1), 0) == 0
    for tap in range(taps):
        moved = moved_ref[tap].astype(F32)
        both = jnp.where(top, own_inner[tap : tap + 1], moved[:, :inner_local])
        inner_ref[tap] = both.astype(BF16)[:slots]
        both = jnp.where(top, own_outer[tap : tap + 1], moved[:, inner_local:width])
        outer_ref[tap] = both.astype(BF16)[:slots]
    logs = []
    for s in range(count):
        parts = shared_ref[s, :, shared_ref.shape[2] - LANES :].astype(F32)
        logs.append(jnp.sum(parts, axis=0, keepdims=True))
    logs = jnp.concatenate(logs + [jnp.zeros((8 - count, LANES), F32)] * (count < 8), axis=0)
    columns = decay_ref.shape[1]
    head = lax.broadcasted_iota(jnp.int32, (LANES, columns), 0)
    lane = lax.broadcasted_iota(jnp.int32, (LANES, columns), 1)
    local_heads = columns // HEAD_DIM
    pick = (head == chain * local_heads + lane // HEAD_DIM).astype(F32)
    spread = dot(logs, pick, precision=lax.Precision.HIGHEST)
    decay_ref[...] = jnp.exp2(spread[:count])


def tails(chain, shared, moved, slots, channels, inner_local, outer_local, columns):
    count, taps = shared.shape[:2]
    whole = pl.BlockSpec(memory_space=pltpu.VMEM)
    return pl.pallas_call(
        tail_kernel,
        in_specs=[pl.BlockSpec(memory_space=pltpu.SMEM), whole, whole],
        out_shape=[
            jax.ShapeDtypeStruct((8, channels), F32),
            jax.ShapeDtypeStruct((taps, slots, inner_local), BF16),
            jax.ShapeDtypeStruct((taps, slots, outer_local), BF16),
            jax.ShapeDtypeStruct((count, columns), F32),
        ],
        name="tails",
    )(chain, shared, moved)


def exchange(value, axis):
    return lax.all_to_all(value, axis, split_axis=0, concat_axis=0, tiled=True)


def rotate(values, axis):
    count = lax.axis_size(axis)
    got = [values[0]] + [None] * (count - 1)
    hops = sorted(range(1, count), key=lambda hop: abs(2 * hop - count))
    for hop in hops:
        pairs = [(source, (source + hop) % count) for source in range(count)]
        got[hop] = lax.ppermute(values[hop], axis, pairs)
    return got


def device_body(
    pool_states,
    inner_window,
    state_window,
    move_plan,
    active_mask,
    inputs_inner,
    inputs_state,
    gate_rows,
    step_raw,
    lengths,
    conv_weight,
    conv_bias,
    step_bias,
    decay_log,
    skip_weight,
    norm_weight,
):
    peers = lax.axis_size("req")
    own_peer = lax.axis_index("req").astype(jnp.int32)
    chain_size = lax.axis_size("seq")
    chain_index = lax.axis_index("seq").astype(jnp.int32)
    slots, local_heads = pool_states.shape[:2]
    columns = local_heads * HEAD_DIM
    piece = columns // peers
    taps = KERNEL - 1
    inner_local = inner_window.shape[2]
    outer_local = state_window.shape[2]

    own = own_peer[None]
    pool_pieces = pool_states.reshape(slots, peers, piece, STATE_DIM)
    spread_a = rotate(pack(own, active_mask, pool_pieces), "req")
    packed = mark(
        move_plan.T,
        active_mask,
        inner_window.transpose(1, 0, 2),
        state_window.transpose(1, 0, 2),
        peers,
    )
    every = exchange(packed, "req")
    spread_b = exchange(pack_rest(active_mask, pool_pieces), "req")

    rows = inputs_inner[0]
    state_rows = inputs_state[0]
    local_length, inner_dim = rows.shape
    channels = inner_dim + state_rows.shape[1]
    start = chain_index * local_length
    length = lengths[0]
    last_tile = local_length // 16 - 1
    low_block = jnp.clip((length - taps - start) // 16, 0, last_tile)
    high_block = jnp.minimum(low_block + 1, last_tile)
    heads = decay_log.shape[0]
    rate = jnp.pad(-LOG2E * jnp.exp(decay_log), (0, LANES - heads))[None]
    payload, step, moved, table = share(
        jnp.stack([low_block, high_block, start, length]),
        slots,
        every,
        rows,
        state_rows,
        step_raw[0],
        step_bias[None],
        rate,
    )
    shared = lax.all_gather(payload, "seq", axis=0)
    chain = chain_index[None]
    tail, new_inner, new_outer, own_decay = tails(
        chain, shared, moved, slots, channels, inner_local, outer_local, columns
    )

    part, local_end, read_rows, decay = block_parts(
        chain,
        tail,
        rows,
        state_rows,
        step,
        rate,
        conv_weight,
        conv_bias[None],
        jnp.repeat(skip_weight, HEAD_DIM)[None],
        chain_size,
    )
    own_ends = rotate(local_end, "seq")

    rest_a, upper = reorder(own, table, spread_a)
    moved_a = exchange(rest_a, "req")
    first, rest_b = reorder_rest(own, table, spread_b, upper)
    first = rotate(first, "req")
    moved_b = rotate(rest_b, "req")

    place = jnp.stack([own_peer, chain_index])
    entering, final = combine(place, own_decay, own_ends, first)
    incoming = rotate(entering, "seq")
    finish_place = jnp.stack([start, length, chain_index])
    mixer_out = finish(
        finish_place,
        part,
        gate_rows[0],
        read_rows,
        decay,
        norm_weight[None],
        incoming,
    )
    states = unpack(final, moved_a)
    new_states = unpack_rest(own, final, moved_b, states).reshape(pool_states.shape)

    return (
        new_states,
        new_inner.transpose(1, 0, 2),
        new_outer.transpose(1, 0, 2),
        mixer_out[None],
    )


def solution(mesh):
    return jax.shard_map(
        device_body,
        mesh=mesh,
        in_specs=(
            P("req", "seq", None, None),
            P("req", None, "seq"),
            P("req", None, "seq"),
            P("req", None),
            P("req"),
            P("req", "seq", None),
            P("req", "seq", None),
            P("req", "seq", None),
            P("req", "seq", None),
            P("req"),
            P(),
            P(),
            P(),
            P(),
            P(),
            P(),
        ),
        out_specs=(
            P("req", "seq", None, None),
            P("req", None, "seq"),
            P("req", None, "seq"),
            P("req", "seq", None),
        ),
        check_vma=False,
    )
```

```python
import functools
import math

import jax
import jax.numpy as jnp
from jax import lax
from jax.experimental import pallas as pl
from jax.experimental.pallas import tpu as pltpu
from jax.sharding import PartitionSpec as P


HEAD_DIM = 64
STATE_DIM = 128
KERNEL = 4
BLOCK_LEN = 256
GROUP = 8
HALF = BLOCK_LEN // 2
GROUP_DIM = GROUP * HEAD_DIM
PAIR_DIM = 2 * HEAD_DIM
LANES = 128
TILE = 128
SLOT_TILE = 4
SLOT_PAD = 16
PEER_TILE = 2
PACK_TILE = 2
EPSILON = 1e-05
LOG2E = math.log2(math.e)
F32 = jnp.float32
BF16 = jnp.bfloat16


def dot(a, b, dims=((1,), (0,)), precision=None):
    return lax.dot_general(a, b, (dims, ((), ())), precision=precision, preferred_element_type=F32)


def silu(v):
    return v / (1.0 + jnp.exp(-v))


def conv_silu(tail, rows, weight, bias_row):
    extended = jnp.concatenate([tail, rows.astype(F32)], axis=0)
    count = rows.shape[0]
    start = tail.shape[0] - KERNEL + 1
    running = bias_row + weight[0:1] * extended[start : start + count]
    for k in range(1, KERNEL):
        running = running + weight[k : k + 1] * extended[start + k : start + k + count]
    return silu(running)


def pair_of(columns, i, low):
    return jnp.where(low, columns[:, 2 * i : 2 * i + 1], columns[:, 2 * i + 1 : 2 * i + 2])


def block_kernel(
    chain_ref,
    tail_ref,
    prev_ref,
    rows_ref,
    state_tail_ref,
    state_prev_ref,
    state_rows_ref,
    step_ref,
    rate_ref,
    weight_ref,
    bias_ref,
    state_weight_ref,
    state_bias_ref,
    skip_ref,
    part_ref,
    end_ref,
    read_ref,
    decay_ref,
    scores_scr,
    cum_scr,
    cum_t_scr,
    to_end_scr,
    decay_scr,
    write_t_scr,
    offset_scr,
    carry_scr,
):
    block = pl.program_id(0)
    group = pl.program_id(1)
    first = block == 0

    @pl.when(group == 0)
    def _():
        state_tail = jnp.where(first, state_tail_ref[...], state_prev_ref[8:16, :].astype(F32))
        mixed = conv_silu(state_tail, state_rows_ref[...], state_weight_ref[...], state_bias_ref[...])
        write = mixed[:, :STATE_DIM]
        read = mixed[:, STATE_DIM:].astype(BF16)
        read_ref[...] = read
        write_b = write.astype(BF16)
        scores_scr[...] = dot(read, write_b, ((1,), (1,)))
        write_t_scr[...] = write_b.astype(F32).T.astype(BF16)
        row = lax.broadcasted_iota(jnp.int32, (BLOCK_LEN, BLOCK_LEN), 0)
        col = lax.broadcasted_iota(jnp.int32, (BLOCK_LEN, BLOCK_LEN), 1)
        triangle = (row >= col).astype(F32)
        step = step_ref[...]
        cum = dot(triangle, step * rate_ref[...], precision=lax.Precision.HIGHEST)
        cum_scr[...] = cum
        cum_t_scr[...] = cum.T
        last = cum[BLOCK_LEN - 1 :, :]
        to_end_scr[...] = jnp.exp2(last - cum) * step
        decay_scr[...] = jnp.exp2(cum)
        offset = jnp.where(first, 0.0, offset_scr[0:1, :])
        decay_ref[...] = jnp.exp2(offset + cum)
        offset_scr[0:1, :] = offset + last

    shift = lax.rem(LANES - group * GROUP, LANES)
    cum = pltpu.roll(cum_scr[...], shift, 1)
    step = pltpu.roll(step_ref[...], shift, 1)
    to_end = pltpu.roll(to_end_scr[...], shift, 1)
    decay = pltpu.roll(decay_scr[...], shift, 1)
    cum_t = cum_t_scr[pl.ds(pl.multiple_of(group * GROUP, GROUP), GROUP), :]
    read = read_ref[...]
    write_t = write_t_scr[...]
    carry = jnp.where(first, 0.0, carry_scr[group])
    carry_b = carry.astype(BF16)
    low = lax.broadcasted_iota(jnp.int32, (1, PAIR_DIM), 1) < HEAD_DIM
    causal = lax.broadcasted_iota(jnp.int32, (HALF, HALF), 0) >= lax.broadcasted_iota(
        jnp.int32, (HALF, HALF), 1
    )
    scores_top = scores_scr[0:HALF, 0:HALF]
    scores_left = scores_scr[HALF:, 0:HALF]
    scores_right = scores_scr[HALF:, HALF:]

    def head_weights(i):
        later = cum[:, i : i + 1]
        earlier = cum_t[i : i + 1, :]
        gap_top = jnp.where(causal, later[:HALF] - earlier[:, :HALF], -1e30)
        gap_left = later[HALF:] - earlier[:, :HALF]
        gap_right = jnp.where(causal, later[HALF:] - earlier[:, HALF:], -1e30)
        top = (scores_top * jnp.exp2(gap_top)).astype(BF16)
        left = (scores_left * jnp.exp2(gap_left)).astype(BF16)
        right = (scores_right * jnp.exp2(gap_right)).astype(BF16)
        return top, jnp.concatenate([left, right], axis=1)

    for i in range(GROUP // 2):
        span = slice(i * PAIR_DIM, (i + 1) * PAIR_DIM)
        tail = jnp.where(first, tail_ref[:, span], prev_ref[8:16, span].astype(F32))
        mixed = conv_silu(tail, rows_ref[:, span], weight_ref[:, span], bias_ref[:, span])
        value = mixed.astype(BF16).astype(F32)
        stepped = (pair_of(step, i, low) * value).astype(BF16)
        scaled = (pair_of(to_end, i, low) * value).astype(BF16)
        stepped_low = jnp.where(low, stepped, jnp.zeros_like(stepped))
        stepped_high = jnp.where(low, jnp.zeros_like(stepped), stepped)
        top_0, bottom_0 = head_weights(2 * i)
        top_1, bottom_1 = head_weights(2 * i + 1)
        intra_top = dot(top_0, stepped_low[:HALF]) + dot(top_1, stepped_high[:HALF])
        intra_bottom = dot(bottom_0, stepped_low) + dot(bottom_1, stepped_high)
        inter = dot(read, carry_b[:, span]) * pair_of(decay, i, low)
        direct = inter + skip_ref[:, span] * value
        part_ref[0:HALF, span] = intra_top + direct[:HALF]
        part_ref[HALF:, span] = intra_bottom + direct[HALF:]
        kept = pair_of(decay[BLOCK_LEN - 1 :, :], i, low) * carry[:, span]
        ending = kept + dot(write_t, scaled)
        carry_scr[group, :, span] = ending
        end_ref[0, :, span] = ending.astype(BF16)


def block_parts(chain, tail, rows, state_rows, step, rate, weight, bias_row, skip_row, ends):
    length = rows.shape[0]
    channels = rows.shape[1]
    blocks = length // BLOCK_LEN
    groups = channels // GROUP_DIM
    end_groups = groups // ends
    state_dim = state_rows.shape[1]
    state_at = channels // state_dim
    per_block = BLOCK_LEN // 16

    def before(b):
        return jnp.maximum(b * per_block - 1, 0)

    def end_at(b, g, chain):
        return lax.rem(g // end_groups - chain[0] + ends, ends), 0, lax.rem(g, end_groups)

    return pl.pallas_call(
        block_kernel,
        grid_spec=pltpu.PrefetchScalarGridSpec(
        num_scalar_prefetch=1,
        grid=(blocks, groups),
        in_specs=[
            pl.BlockSpec((8, GROUP_DIM), lambda b, g, c: (0, g)),
            pl.BlockSpec((16, GROUP_DIM), lambda b, g, c: (before(b), g)),
            pl.BlockSpec((BLOCK_LEN, GROUP_DIM), lambda b, g, c: (b, g)),
            pl.BlockSpec((8, state_dim), lambda b, g, c: (0, state_at)),
            pl.BlockSpec((16, state_dim), lambda b, g, c: (before(b), 0)),
            pl.BlockSpec((BLOCK_LEN, state_dim), lambda b, g, c: (b, 0)),
            pl.BlockSpec((BLOCK_LEN, LANES), lambda b, g, c: (b, 0)),
            pl.BlockSpec((1, LANES), lambda b, g, c: (0, 0)),
            pl.BlockSpec((KERNEL, GROUP_DIM), lambda b, g, c: (0, g)),
            pl.BlockSpec((1, GROUP_DIM), lambda b, g, c: (0, g)),
            pl.BlockSpec((KERNEL, state_dim), lambda b, g, c: (0, state_at)),
            pl.BlockSpec((1, state_dim), lambda b, g, c: (0, state_at)),
            pl.BlockSpec((1, GROUP_DIM), lambda b, g, c: (0, g)),
        ],
        out_specs=[
            pl.BlockSpec((BLOCK_LEN, GROUP_DIM), lambda b, g, c: (b, g)),
            pl.BlockSpec((1, STATE_DIM, GROUP_DIM), end_at),
            pl.BlockSpec((BLOCK_LEN, STATE_DIM), lambda b, g, c: (b, 0)),
            pl.BlockSpec((BLOCK_LEN, LANES), lambda b, g, c: (b, 0)),
        ],
        scratch_shapes=[
            pltpu.VMEM((BLOCK_LEN, BLOCK_LEN), F32),
            pltpu.VMEM((BLOCK_LEN, LANES), F32),
            pltpu.VMEM((LANES, BLOCK_LEN), F32),
            pltpu.VMEM((BLOCK_LEN, LANES), F32),
            pltpu.VMEM((BLOCK_LEN, LANES), F32),
            pltpu.VMEM((STATE_DIM, BLOCK_LEN), BF16),
            pltpu.VMEM((8, LANES), F32),
            pltpu.VMEM((groups, STATE_DIM, GROUP_DIM), F32),
        ],
        ),
        out_shape=[
            jax.ShapeDtypeStruct((length, channels), F32),
            jax.ShapeDtypeStruct((ends, STATE_DIM, channels // ends), BF16),
            jax.ShapeDtypeStruct((length, STATE_DIM), BF16),
            jax.ShapeDtypeStruct((length, LANES), F32),
        ],
        compiler_params=pltpu.CompilerParams(dimension_semantics=("arbitrary", "arbitrary")),
        cost_estimate=pl.CostEstimate(
            flops=6_000_000_000, bytes_accessed=20_000_000, transcendentals=10_000_000
        ),
        name="block_parts",
    )(
        chain,
        tail,
        rows,
        rows,
        tail,
        state_rows,
        state_rows,
        step,
        rate,
        weight,
        bias_row,
        weight,
        bias_row,
        skip_row,
    )


def finish_kernel(
    place_ref, part_ref, gate_ref, read_ref, decay_ref, norm_ref, *refs
):
    state_refs, out_ref, gated_scr, state_scr = refs[:-3], refs[-3], refs[-2], refs[-1]
    tile = pl.program_id(0)
    chunks, _, width = state_scr.shape

    @pl.when(tile == 0)
    def _():
        for hop in range(chunks):
            state_scr[lax.rem(place_ref[2] - hop + chunks, chunks)] = state_refs[hop][...]

    positions = (
        place_ref[0] + tile * TILE + lax.broadcasted_iota(jnp.int32, (TILE, PAIR_DIM), 0)
    )
    valid = (positions < place_ref[1]).astype(F32)
    low = lax.broadcasted_iota(jnp.int32, (1, PAIR_DIM), 1) < HEAD_DIM
    read = read_ref[...]
    decay = decay_ref[...]
    total = jnp.zeros((TILE, PAIR_DIM), F32)
    for chunk in range(chunks):
        for i in range(width // PAIR_DIM):
            pair = chunk * (width // PAIR_DIM) + i
            span = slice(pair * PAIR_DIM, (pair + 1) * PAIR_DIM)
            inter = dot(read, state_scr[chunk, :, i * PAIR_DIM : (i + 1) * PAIR_DIM])
            y = part_ref[:, span] + inter * pair_of(decay, pair, low)
            y = (y * valid).astype(BF16).astype(F32)
            gated = y * silu(gate_ref[:, span].astype(F32))
            gated_scr[:, span] = gated
            total = total + gated * gated
    channels = chunks * width
    mean = jnp.sum(total, axis=1, keepdims=True) * (1.0 / channels)
    scale = lax.rsqrt(mean + EPSILON)
    for pair in range(channels // PAIR_DIM):
        span = slice(pair * PAIR_DIM, (pair + 1) * PAIR_DIM)
        out_ref[:, span] = (gated_scr[:, span] * scale * norm_ref[:, span]).astype(BF16)


def finish(place, part, gate, read, decay, norm_row, states):
    length, channels = part.shape
    return pl.pallas_call(
        finish_kernel,
        grid=(length // TILE,),
        in_specs=[
            pl.BlockSpec(memory_space=pltpu.SMEM),
            pl.BlockSpec((TILE, channels), lambda t: (t, 0)),
            pl.BlockSpec((TILE, channels), lambda t: (t, 0)),
            pl.BlockSpec((TILE, STATE_DIM), lambda t: (t, 0)),
            pl.BlockSpec((TILE, LANES), lambda t: (t, 0)),
            pl.BlockSpec((1, channels), lambda t: (0, 0)),
        ]
        + [pl.BlockSpec(state.shape, lambda t: (0, 0)) for state in states],
        out_specs=pl.BlockSpec((TILE, channels), lambda t: (t, 0)),
        out_shape=jax.ShapeDtypeStruct((length, channels), BF16),
        scratch_shapes=[
            pltpu.VMEM((TILE, channels), F32),
            pltpu.VMEM((len(states),) + states[0].shape, BF16),
        ],
        compiler_params=pltpu.CompilerParams(dimension_semantics=("arbitrary",)),
        cost_estimate=pl.CostEstimate(
            flops=3_000_000_000, bytes_accessed=16_000_000, transcendentals=4_000_000
        ),
        name="finish",
    )(place, part, gate, read, decay, norm_row, *states)


def mark_kernel(plan_ref, mask_ref, inner_ref, outer_ref, out_ref, scr):
    peers, padded, total = out_ref.shape
    taps, slots = inner_ref.shape[:2]
    width = inner_ref.shape[2] + outer_ref.shape[2]
    capacity = most_per_pair(slots, peers)
    scr[:, :width] = jnp.zeros((peers * padded, width), F32)
    scr[:, width:] = jnp.full((peers * padded, total - width), -1.0, F32)
    windows = []
    for tap in range(taps):
        both = [inner_ref[tap].astype(F32), outer_ref[tap].astype(F32)]
        windows.append(jnp.concatenate(both, axis=1))
    lane = lax.broadcasted_iota(jnp.int32, (1, LANES), 1)
    peer_marks = jnp.zeros((1, LANES), F32)
    slot_marks = jnp.zeros((1, LANES), F32)
    for slot in range(slots):
        peer, target = plan_ref[0, slot], plan_ref[1, slot]
        rank = jnp.int32(0)
        for earlier in range(slot):
            rank = rank + (plan_ref[0, earlier] == peer).astype(jnp.int32)
        keep = mask_ref[slot].astype(F32)
        for tap in range(taps):
            tag = jnp.full((1, total - width), (target + tap * SLOT_PAD).astype(F32))
            row = jnp.concatenate([windows[tap][slot : slot + 1] * keep, tag], axis=1)
            scr[pl.ds(peer * padded + tap * capacity + rank, 1), :] = row
        peer_marks = jnp.where(lane == slot, peer.astype(F32), peer_marks)
        slot_marks = jnp.where(lane == slot, target.astype(F32), slot_marks)
    for peer in range(peers):
        at = peer * padded + taps * capacity
        scr[at : at + 1, :LANES] = peer_marks
        scr[at + 1 : at + 2, :LANES] = slot_marks
        out_ref[peer] = scr[peer * padded : (peer + 1) * padded, :].astype(BF16)


def most_per_pair(slots, peers):
    return (2 * slots + peers - 1) // peers


def mark(plan, mask, inner, outer, peers):
    taps, slots = inner.shape[:2]
    width = inner.shape[2] + outer.shape[2]
    whole = pl.BlockSpec(memory_space=pltpu.VMEM)
    scalar = pl.BlockSpec(memory_space=pltpu.SMEM)
    total = width + LANES - width % LANES
    padded = pl.cdiv(taps * most_per_pair(slots, peers) + 2, 16) * 16
    return pl.pallas_call(
        mark_kernel,
        in_specs=[scalar, scalar, whole, whole],
        out_shape=jax.ShapeDtypeStruct((peers, padded, total), BF16),
        scratch_shapes=[pltpu.VMEM((peers * padded, total), F32)],
        name="mark",
    )(plan, mask, inner, outer)


def pack_lead_kernel(own_ref, mask_ref, state_ref, out_ref):
    first_slot = pl.program_id(0) * SLOT_TILE
    for j in range(SLOT_TILE):
        keep = mask_ref[jnp.minimum(first_slot + j, mask_ref.shape[0] - 1)].astype(F32)
        out_ref[j] = (state_ref[j, 0] * keep).astype(BF16)


def pack_lead(own, mask, states, hop):
    slots, peers, piece, width = states.shape

    def from_peer(t, own, mask):
        return t, lax.rem(own[0] + hop, peers), 0, 0

    return pl.pallas_call(
        pack_lead_kernel,
        grid_spec=pltpu.PrefetchScalarGridSpec(
            num_scalar_prefetch=2,
            grid=(pl.cdiv(slots, SLOT_TILE),),
            in_specs=[pl.BlockSpec((SLOT_TILE, 1, piece, width), from_peer)],
            out_specs=pl.BlockSpec((SLOT_TILE, piece, width), lambda t, own, mask: (t, 0, 0)),
        ),
        out_shape=jax.ShapeDtypeStruct((slots, piece, width), BF16),
        compiler_params=pltpu.CompilerParams(dimension_semantics=("arbitrary",)),
        name="pack_lead",
    )(own, mask, states)


def pack_kernel(hops, own_ref, mask_ref, state_ref, *out_refs):
    first_slot = pl.program_id(0) * PACK_TILE
    peers = state_ref.shape[1]
    for j in range(PACK_TILE):
        keep = mask_ref[jnp.minimum(first_slot + j, mask_ref.shape[0] - 1)].astype(F32)
        for hop, out_ref in zip(hops, out_refs):
            peer = lax.rem(own_ref[0] + hop, peers)
            out_ref[j] = (state_ref[j, peer] * keep).astype(BF16)


def pack(own, mask, states, hops):
    slots, peers, piece, width = states.shape
    return pl.pallas_call(
        functools.partial(pack_kernel, hops),
        grid=(pl.cdiv(slots, PACK_TILE),),
        in_specs=[
            pl.BlockSpec(memory_space=pltpu.SMEM),
            pl.BlockSpec(memory_space=pltpu.SMEM),
            pl.BlockSpec((PACK_TILE, peers, piece, width), lambda t: (t, 0, 0, 0)),
        ],
        out_specs=[pl.BlockSpec((PACK_TILE, piece, width), lambda t: (t, 0, 0))] * len(hops),
        out_shape=[jax.ShapeDtypeStruct((slots, piece, width), BF16)] * len(hops),
        compiler_params=pltpu.CompilerParams(dimension_semantics=("arbitrary",)),
        name="pack",
    )(own, mask, states)


def source_of(table_ref, target):
    code = table_ref[0, target]
    peer = lax.div(code, SLOT_PAD)
    return peer, code - peer * SLOT_PAD


def pick_first_kernel(own_ref, table_ref, *refs):
    in_refs, out_ref, sem = refs[:-2], refs[-2], refs[-1]
    peers = len(in_refs)
    slots = in_refs[0].shape[0]
    for target in range(peers):
        peer, index = source_of(table_ref, target * slots)
        source = lax.rem(own_ref[0] - peer + peers, peers)
        for hop in range(peers):

            @pl.when(source == hop)
            def _():
                pltpu.make_async_copy(
                    in_refs[hop].at[index], out_ref.at[target], sem.at[target]
                ).start()

    for target in range(peers):
        pltpu.make_async_copy(in_refs[0].at[0], out_ref.at[target], sem.at[target]).wait()


def pick_first(own, table, pieces):
    _, piece, width = pieces[0].shape
    peers = len(pieces)
    scalar = pl.BlockSpec(memory_space=pltpu.SMEM)
    return pl.pallas_call(
        pick_first_kernel,
        in_specs=[scalar, scalar] + [pl.BlockSpec(memory_space=pl.ANY)] * peers,
        out_specs=pl.BlockSpec(memory_space=pltpu.VMEM),
        out_shape=jax.ShapeDtypeStruct((peers, piece, width), BF16),
        scratch_shapes=[pltpu.SemaphoreType.DMA((peers,))],
        name="pick_first",
    )(own, table, *pieces)


def gather_pieces(own_ref, refs, scr):
    peers = len(refs)
    for hop in range(peers):
        scr[lax.rem(own_ref[0] - hop + peers, peers)] = refs[hop][...]


def reorder_kernel(own_ref, table_ref, *refs):
    scr = refs[-1]
    peers, slots = scr.shape[:2]
    gather_pieces(own_ref, refs[:peers], scr)
    for hop in range(peers):
        base = lax.rem(own_ref[0] + hop, peers) * slots
        out_ref = refs[peers + hop]

        def move(slot, unused):
            peer, index = source_of(table_ref, base + slot)
            out_ref[slot - 1] = scr[peer, index]
            return unused

        lax.fori_loop(1, slots, move, 0)


def reorder_rest_kernel(own_ref, table_ref, *refs):
    out_ref, scr = refs[-2:]
    peers, slots = scr.shape[:2]
    gather_pieces(own_ref, refs[:peers], scr)
    for target in range(peers):

        def move(slot, unused):
            peer, index = source_of(table_ref, target * slots + slot)
            out_ref[target, slot - 1] = scr[peer, index]
            return unused

        lax.fori_loop(1, slots, move, 0)


def reorder(own, table, pieces, part):
    slots, piece, width = pieces[0].shape
    half = piece // 2
    peers = len(pieces)
    scalar = pl.BlockSpec(memory_space=pltpu.SMEM)
    if part == 0:
        one = (slots - 1, half, width)
        out_specs = [pl.BlockSpec(one, lambda t: (0, 0, 0))] * peers
        out_shape = [jax.ShapeDtypeStruct(one, BF16)] * peers
    else:
        all_rest = (peers, slots - 1, half, width)
        out_specs = pl.BlockSpec(all_rest, lambda t: (0, 0, 0, 0))
        out_shape = jax.ShapeDtypeStruct(all_rest, BF16)
    return pl.pallas_call(
        reorder_kernel if part == 0 else reorder_rest_kernel,
        grid=(1,),
        in_specs=[scalar, scalar]
        + [pl.BlockSpec((slots, half, width), lambda t: (0, part, 0))] * peers,
        out_specs=out_specs,
        out_shape=out_shape,
        scratch_shapes=[pltpu.VMEM((peers, slots, half, width), BF16)],
        name="reorder" if part == 0 else "reorder_rest",
    )(own, table, *pieces)


def unpack_kernel(own_ref, final_ref, *refs):
    piece_refs, out_ref = refs[:-1], refs[-1]
    step = pl.program_id(0)
    half = out_ref.shape[2]
    out_ref[0, 0] = final_ref[:half, :]
    for hop in range(len(piece_refs)):

        @pl.when(step == hop)
        def _():
            out_ref[1:, 0] = piece_refs[hop][...].astype(F32)


def unpack(own, final, pieces):
    others, half, width = pieces[0].shape
    peers = len(pieces)
    slots, piece = others + 1, 2 * half

    def from_peer(hop, own):
        return lax.rem(own[0] - hop + peers, peers)

    return pl.pallas_call(
        unpack_kernel,
        grid_spec=pltpu.PrefetchScalarGridSpec(
            num_scalar_prefetch=1,
            grid=(peers,),
            in_specs=[pl.BlockSpec((piece, width), lambda h, own: (from_peer(h, own), 0))]
            + [pl.BlockSpec((others, half, width), lambda h, own: (0, 0, 0))] * peers,
            out_specs=pl.BlockSpec(
                (slots, 1, half, width), lambda h, own: (0, from_peer(h, own), 0, 0)
            ),
        ),
        out_shape=jax.ShapeDtypeStruct((slots, peers, piece, width), F32),
        compiler_params=pltpu.CompilerParams(dimension_semantics=("arbitrary",)),
        name="unpack",
    )(own, final, *pieces)


def unpack_rest_kernel(final_ref, pieces_ref, states_ref, out_ref):
    peers, half = pieces_ref.shape[0], pieces_ref.shape[2]
    for p in range(peers):
        out_ref[0, p] = final_ref[(2 * p + 1) * half : (2 * p + 2) * half, :]
        out_ref[1:, p] = pieces_ref[p].astype(F32)


def unpack_rest(final, pieces, states):
    slots, peers, piece, width = states.shape
    half = piece // 2
    return pl.pallas_call(
        unpack_rest_kernel,
        grid=(peers // PEER_TILE,),
        in_specs=[
            pl.BlockSpec((PEER_TILE * piece, width), lambda p: (p, 0)),
            pl.BlockSpec((PEER_TILE, slots - 1, half, width), lambda p: (p, 0, 0, 0)),
            pl.BlockSpec(memory_space=pl.ANY),
        ],
        out_specs=pl.BlockSpec((slots, PEER_TILE, half, width), lambda p: (0, p, 1, 0)),
        out_shape=jax.ShapeDtypeStruct(states.shape, F32),
        input_output_aliases={2: 0},
        compiler_params=pltpu.CompilerParams(dimension_semantics=("arbitrary",)),
        name="unpack_rest",
    )(final, pieces, states)


def combine_kernel(place_ref, decay_ref, *refs):
    count = decay_ref.shape[0]
    end_scr, enter_scr = refs[-2:]
    final_ref = refs[-3]
    entering_refs = refs[-3 - count : -3]
    end_refs, first_ref = refs[:count], refs[count]
    chain = place_ref[0]
    for hop in range(count):
        end_scr[lax.rem(chain - hop + count, count)] = end_refs[hop][...]
    state = first_ref[...].astype(F32).T
    for k in range(count):
        enter_scr[k] = state.astype(BF16)
        state = state * decay_ref[k : k + 1, :] + end_scr[k].astype(F32)
    for hop in range(count):
        entering_refs[hop][...] = enter_scr[lax.rem(chain + hop, count)]
    final_ref[...] = state.T


def combine(place, decay, ends, first):
    count = len(ends)
    whole = pl.BlockSpec(memory_space=pltpu.VMEM)
    rows, columns = ends[0].shape
    outs = pl.pallas_call(
        combine_kernel,
        grid=(1,),
        in_specs=[
            pl.BlockSpec(memory_space=pltpu.SMEM),
            pl.BlockSpec(decay.shape, lambda t: (0, 0)),
        ]
        + [pl.BlockSpec((rows, columns), lambda t: (0, 0))] * count
        + [pl.BlockSpec(first.shape, lambda t: (0, 0))],
        out_specs=[pl.BlockSpec((rows, columns), lambda t: (0, 0))] * count
        + [pl.BlockSpec((columns, rows), lambda t: (0, 0))],
        out_shape=[jax.ShapeDtypeStruct((rows, columns), BF16)] * count
        + [jax.ShapeDtypeStruct((columns, rows), F32)],
        scratch_shapes=[
            pltpu.VMEM((count, rows, columns), BF16),
            pltpu.VMEM((count, rows, columns), BF16),
        ],
        name="combine",
    )(place, decay, *ends, first)
    return outs[:count], outs[count]


def share_kernel(
    slot_count,
    place_ref,
    every_ref,
    end_ref,
    kept_ref,
    kept_next_ref,
    state_end_ref,
    state_kept_ref,
    state_next_ref,
    raw_ref,
    bias_ref,
    rate_ref,
    out_ref,
    step_ref,
    moved_ref,
    table_ref,
):
    taps = out_ref.shape[0]
    inner = end_ref.shape[1]
    outer = state_end_ref.shape[1]
    channels = inner + outer
    peers, packet, width = every_ref.shape
    padded = moved_ref.shape[1]
    slots = float(slot_count)
    rows = peers * packet
    everything = every_ref[...].astype(F32).reshape(rows, width)
    tags = everything[:, width - 1 :]
    lane = lax.broadcasted_iota(jnp.int32, (rows, LANES), 1).astype(F32)
    pick = (tags == lane).astype(BF16)
    moved = dot(pick, everything.astype(BF16), ((0,), (0,)))
    firsts = []
    for tap in range(taps):
        moved_ref[tap] = moved[tap * padded : (tap + 1) * padded].astype(BF16)
        firsts.append(moved[tap * padded : tap * padded + 1])
    at = taps * most_per_pair(slot_count, peers)
    peer_marks = [every_ref[p, at : at + 1, :LANES].astype(F32) for p in range(peers)]
    slot_marks = [every_ref[p, at + 1 : at + 2, :LANES].astype(F32) for p in range(peers)]
    target = jnp.concatenate(peer_marks, axis=0) * slots + jnp.concatenate(slot_marks, axis=0)
    columns = table_ref.shape[1]
    lane = lax.broadcasted_iota(jnp.int32, (peers, columns), 1).astype(F32)
    code = lax.broadcasted_iota(jnp.int32, (peers, columns), 0).astype(F32) * SLOT_PAD
    found = jnp.zeros((peers, columns), F32)
    for slot in range(slot_count):
        found = found + jnp.where(target[:, slot : slot + 1] == lane, code + slot, 0.0)
    found = jnp.sum(found, axis=0, keepdims=True)
    table_ref[...] = jnp.broadcast_to(found, table_ref.shape).astype(jnp.int32)
    low_block, high_block, start, length = (
        place_ref[0],
        place_ref[1],
        place_ref[2],
        place_ref[3],
    )
    out_ref[:, :inner] = end_ref[16 - taps :, :]
    out_ref[:, inner:channels] = state_end_ref[16 - taps :, :]
    here = lax.broadcasted_iota(jnp.int32, (16, 1), 0)
    wanted = length - taps - start

    def kept_rows(low_ref, high_ref):
        low = low_ref[...].astype(F32)
        high = high_ref[...].astype(F32)
        found = []
        for i in range(taps):
            in_low = (low_block * 16 + here) == (wanted + i)
            in_high = ((high_block * 16 + here) == (wanted + i)) & (high_block > low_block)
            picked = jnp.where(in_low, low, 0.0) + jnp.where(in_high, high, 0.0)
            found.append(jnp.sum(picked, axis=0, keepdims=True))
        return jnp.concatenate(found, axis=0).astype(BF16)

    out_ref[:, channels : channels + inner] = kept_rows(kept_ref, kept_next_ref)
    out_ref[:, channels + inner : 2 * channels] = kept_rows(state_kept_ref, state_next_ref)
    out_ref[:, 2 * channels : 2 * channels + width] = jnp.concatenate(firsts, axis=0).astype(BF16)
    count = step_ref.shape[0]
    heads = raw_ref.shape[1]
    positions = start + lax.broadcasted_iota(jnp.int32, (count, heads), 0)
    raw = raw_ref[...].astype(F32) + bias_ref[...]
    step = jnp.maximum(raw, 0.0) + jnp.log1p(jnp.exp(-jnp.abs(raw)))
    step = jnp.where(positions < length, step, 0.0)
    step = jnp.concatenate([step, jnp.zeros((count, LANES - heads), F32)], axis=1)
    step_ref[...] = step
    total = jnp.sum(step * rate_ref[...], axis=0, keepdims=True)
    high = total.astype(BF16).astype(F32)
    middle = (total - high).astype(BF16).astype(F32)
    rest = total - high - middle
    parts = jnp.concatenate([high, middle, rest], axis=0)
    out_ref[:, 2 * channels + width :] = parts.astype(BF16)


def share(place, slots, every, rows, state_rows, step_raw, step_bias, rate):
    peers, _, width = every.shape
    taps, padded = KERNEL - 1, SLOT_PAD
    length, inner = rows.shape
    outer = state_rows.shape[1]
    heads = step_raw.shape[1]
    last = length // 16 - 1
    total = 2 * (inner + outer) + width + LANES
    lanes = pl.cdiv(peers * slots, LANES) * LANES
    return pl.pallas_call(
        functools.partial(share_kernel, slots),
        grid_spec=pltpu.PrefetchScalarGridSpec(
            num_scalar_prefetch=1,
            grid=(1,),
            in_specs=[
                pl.BlockSpec(every.shape, lambda t, c: (0, 0, 0)),
                pl.BlockSpec((16, inner), lambda t, c: (last, 0)),
                pl.BlockSpec((16, inner), lambda t, c: (c[0], 0)),
                pl.BlockSpec((16, inner), lambda t, c: (c[1], 0)),
                pl.BlockSpec((16, outer), lambda t, c: (last, 0)),
                pl.BlockSpec((16, outer), lambda t, c: (c[0], 0)),
                pl.BlockSpec((16, outer), lambda t, c: (c[1], 0)),
                pl.BlockSpec((length, heads), lambda t, c: (0, 0)),
                pl.BlockSpec((1, heads), lambda t, c: (0, 0)),
                pl.BlockSpec((1, LANES), lambda t, c: (0, 0)),
            ],
            out_specs=[
                pl.BlockSpec((taps, total), lambda t, c: (0, 0)),
                pl.BlockSpec((length, LANES), lambda t, c: (0, 0)),
                pl.BlockSpec((taps, padded, width), lambda t, c: (0, 0, 0)),
                pl.BlockSpec((8, lanes), lambda t, c: (0, 0)),
            ],
        ),
        out_shape=[
            jax.ShapeDtypeStruct((taps, total), BF16),
            jax.ShapeDtypeStruct((length, LANES), F32),
            jax.ShapeDtypeStruct((taps, padded, width), BF16),
            jax.ShapeDtypeStruct((8, lanes), jnp.int32),
        ],
        name="share",
    )(
        place,
        every,
        rows,
        rows,
        rows,
        state_rows,
        state_rows,
        state_rows,
        step_raw,
        step_bias,
        rate,
    )


def tail_kernel(
    chain_ref, shared_ref, moved_ref, tail_ref, inner_ref, outer_ref, decay_ref
):
    chain = chain_ref[0]
    count, taps = shared_ref.shape[:2]
    slots, inner_local = inner_ref.shape[1:]
    outer_local = outer_ref.shape[2]
    channels = tail_ref.shape[1]
    inner = count * inner_local
    at = 2 * channels
    window = jnp.concatenate(
        [shared_ref[s, :, at : at + inner_local] for s in range(count)]
        + [
            shared_ref[s, :, at + inner_local : at + inner_local + outer_local]
            for s in range(count)
        ],
        axis=1,
    ).astype(F32)
    earlier = shared_ref[jnp.maximum(chain - 1, 0), :, :channels].astype(F32)
    tail = jnp.where(chain == 0, window, earlier)
    tail_ref[...] = jnp.concatenate([jnp.zeros((8 - taps, channels), F32), tail], axis=0)
    kept = shared_ref[0, :, channels:at].astype(F32)
    for s in range(1, count):
        kept = kept + shared_ref[s, :, channels:at].astype(F32)
    own_inner = jnp.zeros((taps, inner_local), F32)
    own_outer = jnp.zeros((taps, outer_local), F32)
    for s in range(count):
        mine = chain == s
        inner_at, outer_at = s * inner_local, inner + s * outer_local
        own_inner = jnp.where(mine, kept[:, inner_at : inner_at + inner_local], own_inner)
        own_outer = jnp.where(mine, kept[:, outer_at : outer_at + outer_local], own_outer)
    width = inner_local + outer_local
    top = lax.broadcasted_iota(jnp.int32, (moved_ref.shape[1], 1), 0) == 0
    for tap in range(taps):
        moved = moved_ref[tap].astype(F32)
        both = jnp.where(top, own_inner[tap : tap + 1], moved[:, :inner_local])
        inner_ref[tap] = both.astype(BF16)[:slots]
        both = jnp.where(top, own_outer[tap : tap + 1], moved[:, inner_local:width])
        outer_ref[tap] = both.astype(BF16)[:slots]
    logs = []
    for s in range(count):
        parts = shared_ref[s, :, shared_ref.shape[2] - LANES :].astype(F32)
        logs.append(jnp.sum(parts, axis=0, keepdims=True))
    logs = jnp.concatenate(logs + [jnp.zeros((8 - count, LANES), F32)] * (count < 8), axis=0)
    columns = decay_ref.shape[1]
    head = lax.broadcasted_iota(jnp.int32, (LANES, columns), 0)
    lane = lax.broadcasted_iota(jnp.int32, (LANES, columns), 1)
    local_heads = columns // HEAD_DIM
    pick = (head == chain * local_heads + lane // HEAD_DIM).astype(F32)
    spread = dot(logs, pick, precision=lax.Precision.HIGHEST)
    decay_ref[...] = jnp.exp2(spread[:count])


def tails(chain, shared, moved, slots, channels, inner_local, outer_local, columns):
    count, taps = shared.shape[:2]
    whole = pl.BlockSpec(memory_space=pltpu.VMEM)
    return pl.pallas_call(
        tail_kernel,
        in_specs=[pl.BlockSpec(memory_space=pltpu.SMEM), whole, whole],
        out_shape=[
            jax.ShapeDtypeStruct((8, channels), F32),
            jax.ShapeDtypeStruct((taps, slots, inner_local), BF16),
            jax.ShapeDtypeStruct((taps, slots, outer_local), BF16),
            jax.ShapeDtypeStruct((count, columns), F32),
        ],
        name="tails",
    )(chain, shared, moved)


def exchange(value, axis):
    return lax.all_to_all(value, axis, split_axis=0, concat_axis=0, tiled=True)


def hop_order(count):
    return sorted(range(1, count), key=lambda hop: abs(2 * hop - count))


def send(value, axis, hop):
    count = lax.axis_size(axis)
    pairs = [(source, (source + hop) % count) for source in range(count)]
    return lax.ppermute(value, axis, pairs)


def rotate(values, axis):
    got = list(values)
    for hop in hop_order(len(got)):
        got[hop] = send(values[hop], axis, hop)
    return got


def device_body(
    pool_states,
    inner_window,
    state_window,
    move_plan,
    active_mask,
    inputs_inner,
    inputs_state,
    gate_rows,
    step_raw,
    lengths,
    conv_weight,
    conv_bias,
    step_bias,
    decay_log,
    skip_weight,
    norm_weight,
):
    peers = lax.axis_size("req")
    own_peer = lax.axis_index("req").astype(jnp.int32)
    chain_size = lax.axis_size("seq")
    chain_index = lax.axis_index("seq").astype(jnp.int32)
    slots, local_heads = pool_states.shape[:2]
    columns = local_heads * HEAD_DIM
    piece = columns // peers
    taps = KERNEL - 1
    inner_local = inner_window.shape[2]
    outer_local = state_window.shape[2]

    own = own_peer[None]
    pool_pieces = pool_states.reshape(slots, peers, piece, STATE_DIM)
    lead, *others = hop_order(peers)
    spread = [None] * peers
    lead_pieces = pack_lead(own, active_mask, pool_pieces, lead)
    spread[lead] = send(lead_pieces, "req", lead)
    packed = mark(
        move_plan.T,
        active_mask,
        inner_window.transpose(1, 0, 2),
        state_window.transpose(1, 0, 2),
        peers,
    )
    every = exchange(packed, "req")
    others = [0] + others
    for hop, pieces in zip(others, pack(own, active_mask, pool_pieces, others)):
        spread[hop] = pieces if hop == 0 else send(pieces, "req", hop)

    rows = inputs_inner[0]
    state_rows = inputs_state[0]
    local_length, inner_dim = rows.shape
    channels = inner_dim + state_rows.shape[1]
    start = chain_index * local_length
    length = lengths[0]
    last_tile = local_length // 16 - 1
    low_block = jnp.clip((length - taps - start) // 16, 0, last_tile)
    high_block = jnp.minimum(low_block + 1, last_tile)
    heads = decay_log.shape[0]
    rate = jnp.pad(-LOG2E * jnp.exp(decay_log), (0, LANES - heads))[None]
    payload, step, moved, table = share(
        jnp.stack([low_block, high_block, start, length]),
        slots,
        every,
        rows,
        state_rows,
        step_raw[0],
        step_bias[None],
        rate,
    )
    shared = lax.all_gather(payload, "seq", axis=0)
    chain = chain_index[None]
    tail, new_inner, new_outer, own_decay = tails(
        chain, shared, moved, slots, channels, inner_local, outer_local, columns
    )

    part, local_end, read_rows, decay = block_parts(
        chain,
        tail,
        rows,
        state_rows,
        step,
        rate,
        conv_weight,
        conv_bias[None],
        jnp.repeat(skip_weight, HEAD_DIM)[None],
        chain_size,
    )
    own_ends = rotate(local_end, "seq")

    first = exchange(pick_first(own, table, spread), "req")
    moved_a = rotate(reorder(own, table, spread, 0), "req")
    moved_b = exchange(reorder(own, table, spread, 1), "req")
    entering, final = combine(
        chain, own_decay, own_ends, first.reshape(columns, STATE_DIM)
    )
    incoming = rotate(entering, "seq")
    mixer_out = finish(
        jnp.stack([start, length, chain_index]),
        part,
        gate_rows[0],
        read_rows,
        decay,
        norm_weight[None],
        incoming,
    )
    states = unpack(own, final, moved_a)
    new_states = unpack_rest(final, moved_b, states).reshape(pool_states.shape)

    return (
        new_states,
        new_inner.transpose(1, 0, 2),
        new_outer.transpose(1, 0, 2),
        mixer_out[None],
    )


def solution(mesh):
    return jax.shard_map(
        device_body,
        mesh=mesh,
        in_specs=(
            P("req", "seq", None, None),
            P("req", None, "seq"),
            P("req", None, "seq"),
            P("req", None),
            P("req"),
            P("req", "seq", None),
            P("req", "seq", None),
            P("req", "seq", None),
            P("req", "seq", None),
            P("req"),
            P(),
            P(),
            P(),
            P(),
            P(),
            P(),
        ),
        out_specs=(
            P("req", "seq", None, None),
            P("req", None, "seq"),
            P("req", None, "seq"),
            P("req", "seq", None),
        ),
        check_vma=False,
    )
```

```python
import functools
import math

import jax
import jax.numpy as jnp
from jax import lax
from jax.experimental import pallas as pl
from jax.experimental.pallas import tpu as pltpu
from jax.sharding import PartitionSpec as P


HEAD_DIM = 64
STATE_DIM = 128
KERNEL = 4
BLOCK_LEN = 256
GROUP = 8
HALF = BLOCK_LEN // 2
GROUP_DIM = GROUP * HEAD_DIM
PAIR_DIM = 2 * HEAD_DIM
LANES = 128
TILE = 128
SLOT_TILE = 4
SLOT_PAD = 16
PEER_TILE = 2
PACK_TILE = 2
EPSILON = 1e-05
LOG2E = math.log2(math.e)
F32 = jnp.float32
BF16 = jnp.bfloat16


def dot(a, b, dims=((1,), (0,)), precision=None):
    return lax.dot_general(a, b, (dims, ((), ())), precision=precision, preferred_element_type=F32)


def silu(v):
    return v / (1.0 + jnp.exp(-v))


def conv_silu(tail, rows, weight, bias_row):
    extended = jnp.concatenate([tail, rows.astype(F32)], axis=0)
    count = rows.shape[0]
    start = tail.shape[0] - KERNEL + 1
    running = bias_row + weight[0:1] * extended[start : start + count]
    for k in range(1, KERNEL):
        running = running + weight[k : k + 1] * extended[start + k : start + k + count]
    return silu(running)


def pair_of(columns, i, low):
    return jnp.where(low, columns[:, 2 * i : 2 * i + 1], columns[:, 2 * i + 1 : 2 * i + 2])


def block_kernel(
    chain_ref,
    tail_ref,
    prev_ref,
    rows_ref,
    state_tail_ref,
    state_prev_ref,
    state_rows_ref,
    step_ref,
    rate_ref,
    weight_ref,
    bias_ref,
    state_weight_ref,
    state_bias_ref,
    skip_ref,
    part_ref,
    end_ref,
    read_ref,
    decay_ref,
    scores_scr,
    cum_scr,
    cum_t_scr,
    to_end_scr,
    decay_scr,
    write_t_scr,
    offset_scr,
    carry_scr,
):
    block = pl.program_id(0)
    group = pl.program_id(1)
    first = block == 0

    @pl.when(group == 0)
    def _():
        state_tail = jnp.where(first, state_tail_ref[...], state_prev_ref[8:16, :].astype(F32))
        mixed = conv_silu(state_tail, state_rows_ref[...], state_weight_ref[...], state_bias_ref[...])
        write = mixed[:, :STATE_DIM]
        read = mixed[:, STATE_DIM:].astype(BF16)
        read_ref[...] = read
        write_b = write.astype(BF16)
        scores_scr[...] = dot(read, write_b, ((1,), (1,)))
        write_t_scr[...] = write_b.astype(F32).T.astype(BF16)
        row = lax.broadcasted_iota(jnp.int32, (BLOCK_LEN, BLOCK_LEN), 0)
        col = lax.broadcasted_iota(jnp.int32, (BLOCK_LEN, BLOCK_LEN), 1)
        triangle = (row >= col).astype(F32)
        step = step_ref[...]
        cum = dot(triangle, step * rate_ref[...], precision=lax.Precision.HIGHEST)
        cum_scr[...] = cum
        cum_t_scr[...] = cum.T
        last = cum[BLOCK_LEN - 1 :, :]
        to_end_scr[...] = jnp.exp2(last - cum) * step
        decay_scr[...] = jnp.exp2(cum)
        offset = jnp.where(first, 0.0, offset_scr[0:1, :])
        decay_ref[...] = jnp.exp2(offset + cum)
        offset_scr[0:1, :] = offset + last

    shift = lax.rem(LANES - group * GROUP, LANES)
    cum = pltpu.roll(cum_scr[...], shift, 1)
    step = pltpu.roll(step_ref[...], shift, 1)
    to_end = pltpu.roll(to_end_scr[...], shift, 1)
    decay = pltpu.roll(decay_scr[...], shift, 1)
    cum_t = cum_t_scr[pl.ds(pl.multiple_of(group * GROUP, GROUP), GROUP), :]
    read = read_ref[...]
    write_t = write_t_scr[...]
    carry = jnp.where(first, 0.0, carry_scr[group])
    carry_b = carry.astype(BF16)
    low = lax.broadcasted_iota(jnp.int32, (1, PAIR_DIM), 1) < HEAD_DIM
    causal = lax.broadcasted_iota(jnp.int32, (HALF, HALF), 0) >= lax.broadcasted_iota(
        jnp.int32, (HALF, HALF), 1
    )
    scores_top = scores_scr[0:HALF, 0:HALF]
    scores_left = scores_scr[HALF:, 0:HALF]
    scores_right = scores_scr[HALF:, HALF:]

    def head_weights(i):
        later = cum[:, i : i + 1]
        earlier = cum_t[i : i + 1, :]
        gap_top = jnp.where(causal, later[:HALF] - earlier[:, :HALF], -1e30)
        gap_left = later[HALF:] - earlier[:, :HALF]
        gap_right = jnp.where(causal, later[HALF:] - earlier[:, HALF:], -1e30)
        top = (scores_top * jnp.exp2(gap_top)).astype(BF16)
        left = (scores_left * jnp.exp2(gap_left)).astype(BF16)
        right = (scores_right * jnp.exp2(gap_right)).astype(BF16)
        return top, jnp.concatenate([left, right], axis=1)

    for i in range(GROUP // 2):
        span = slice(i * PAIR_DIM, (i + 1) * PAIR_DIM)
        tail = jnp.where(first, tail_ref[:, span], prev_ref[8:16, span].astype(F32))
        mixed = conv_silu(tail, rows_ref[:, span], weight_ref[:, span], bias_ref[:, span])
        value = mixed.astype(BF16).astype(F32)
        stepped = (pair_of(step, i, low) * value).astype(BF16)
        scaled = (pair_of(to_end, i, low) * value).astype(BF16)
        stepped_low = jnp.where(low, stepped, jnp.zeros_like(stepped))
        stepped_high = jnp.where(low, jnp.zeros_like(stepped), stepped)
        top_0, bottom_0 = head_weights(2 * i)
        top_1, bottom_1 = head_weights(2 * i + 1)
        intra_top = dot(top_0, stepped_low[:HALF]) + dot(top_1, stepped_high[:HALF])
        intra_bottom = dot(bottom_0, stepped_low) + dot(bottom_1, stepped_high)
        inter = dot(read, carry_b[:, span]) * pair_of(decay, i, low)
        direct = inter + skip_ref[:, span] * value
        part_ref[0:HALF, span] = intra_top + direct[:HALF]
        part_ref[HALF:, span] = intra_bottom + direct[HALF:]
        kept = pair_of(decay[BLOCK_LEN - 1 :, :], i, low) * carry[:, span]
        ending = kept + dot(write_t, scaled)
        carry_scr[group, :, span] = ending
        end_ref[0, :, span] = ending.astype(BF16)


def block_parts(chain, tail, rows, state_rows, step, rate, weight, bias_row, skip_row, ends):
    length = rows.shape[0]
    channels = rows.shape[1]
    blocks = length // BLOCK_LEN
    groups = channels // GROUP_DIM
    end_groups = groups // ends
    state_dim = state_rows.shape[1]
    state_at = channels // state_dim
    per_block = BLOCK_LEN // 16

    def before(b):
        return jnp.maximum(b * per_block - 1, 0)

    def end_at(b, g, chain):
        return lax.rem(g // end_groups - chain[0] + ends, ends), 0, lax.rem(g, end_groups)

    return pl.pallas_call(
        block_kernel,
        grid_spec=pltpu.PrefetchScalarGridSpec(
        num_scalar_prefetch=1,
        grid=(blocks, groups),
        in_specs=[
            pl.BlockSpec((8, GROUP_DIM), lambda b, g, c: (0, g)),
            pl.BlockSpec((16, GROUP_DIM), lambda b, g, c: (before(b), g)),
            pl.BlockSpec((BLOCK_LEN, GROUP_DIM), lambda b, g, c: (b, g)),
            pl.BlockSpec((8, state_dim), lambda b, g, c: (0, state_at)),
            pl.BlockSpec((16, state_dim), lambda b, g, c: (before(b), 0)),
            pl.BlockSpec((BLOCK_LEN, state_dim), lambda b, g, c: (b, 0)),
            pl.BlockSpec((BLOCK_LEN, LANES), lambda b, g, c: (b, 0)),
            pl.BlockSpec((1, LANES), lambda b, g, c: (0, 0)),
            pl.BlockSpec((KERNEL, GROUP_DIM), lambda b, g, c: (0, g)),
            pl.BlockSpec((1, GROUP_DIM), lambda b, g, c: (0, g)),
            pl.BlockSpec((KERNEL, state_dim), lambda b, g, c: (0, state_at)),
            pl.BlockSpec((1, state_dim), lambda b, g, c: (0, state_at)),
            pl.BlockSpec((1, GROUP_DIM), lambda b, g, c: (0, g)),
        ],
        out_specs=[
            pl.BlockSpec((BLOCK_LEN, GROUP_DIM), lambda b, g, c: (b, g)),
            pl.BlockSpec((1, STATE_DIM, GROUP_DIM), end_at),
            pl.BlockSpec((BLOCK_LEN, STATE_DIM), lambda b, g, c: (b, 0)),
            pl.BlockSpec((BLOCK_LEN, LANES), lambda b, g, c: (b, 0)),
        ],
        scratch_shapes=[
            pltpu.VMEM((BLOCK_LEN, BLOCK_LEN), F32),
            pltpu.VMEM((BLOCK_LEN, LANES), F32),
            pltpu.VMEM((LANES, BLOCK_LEN), F32),
            pltpu.VMEM((BLOCK_LEN, LANES), F32),
            pltpu.VMEM((BLOCK_LEN, LANES), F32),
            pltpu.VMEM((STATE_DIM, BLOCK_LEN), BF16),
            pltpu.VMEM((8, LANES), F32),
            pltpu.VMEM((groups, STATE_DIM, GROUP_DIM), F32),
        ],
        ),
        out_shape=[
            jax.ShapeDtypeStruct((length, channels), F32),
            jax.ShapeDtypeStruct((ends, STATE_DIM, channels // ends), BF16),
            jax.ShapeDtypeStruct((length, STATE_DIM), BF16),
            jax.ShapeDtypeStruct((length, LANES), F32),
        ],
        compiler_params=pltpu.CompilerParams(dimension_semantics=("arbitrary", "arbitrary")),
        cost_estimate=pl.CostEstimate(
            flops=6_000_000_000, bytes_accessed=20_000_000, transcendentals=10_000_000
        ),
        name="block_parts",
    )(
        chain,
        tail,
        rows,
        rows,
        tail,
        state_rows,
        state_rows,
        step,
        rate,
        weight,
        bias_row,
        weight,
        bias_row,
        skip_row,
    )


def finish_kernel(
    place_ref, part_ref, gate_ref, read_ref, decay_ref, norm_ref, *refs
):
    state_refs, out_ref, gated_scr, state_scr = refs[:-3], refs[-3], refs[-2], refs[-1]
    tile = pl.program_id(0)
    chunks, _, width = state_scr.shape

    @pl.when(tile == 0)
    def _():
        for hop in range(chunks):
            state_scr[lax.rem(place_ref[2] - hop + chunks, chunks)] = state_refs[hop][...]

    positions = (
        place_ref[0] + tile * TILE + lax.broadcasted_iota(jnp.int32, (TILE, PAIR_DIM), 0)
    )
    valid = (positions < place_ref[1]).astype(F32)
    low = lax.broadcasted_iota(jnp.int32, (1, PAIR_DIM), 1) < HEAD_DIM
    read = read_ref[...]
    decay = decay_ref[...]
    total = jnp.zeros((TILE, PAIR_DIM), F32)
    for chunk in range(chunks):
        for i in range(width // PAIR_DIM):
            pair = chunk * (width // PAIR_DIM) + i
            span = slice(pair * PAIR_DIM, (pair + 1) * PAIR_DIM)
            inter = dot(read, state_scr[chunk, :, i * PAIR_DIM : (i + 1) * PAIR_DIM])
            y = part_ref[:, span] + inter * pair_of(decay, pair, low)
            y = (y * valid).astype(BF16).astype(F32)
            gated = y * silu(gate_ref[:, span].astype(F32))
            gated_scr[:, span] = gated
            total = total + gated * gated
    channels = chunks * width
    mean = jnp.sum(total, axis=1, keepdims=True) * (1.0 / channels)
    scale = lax.rsqrt(mean + EPSILON)
    for pair in range(channels // PAIR_DIM):
        span = slice(pair * PAIR_DIM, (pair + 1) * PAIR_DIM)
        out_ref[:, span] = (gated_scr[:, span] * scale * norm_ref[:, span]).astype(BF16)


def finish(place, part, gate, read, decay, norm_row, states):
    length, channels = part.shape
    return pl.pallas_call(
        finish_kernel,
        grid=(length // TILE,),
        in_specs=[
            pl.BlockSpec(memory_space=pltpu.SMEM),
            pl.BlockSpec((TILE, channels), lambda t: (t, 0)),
            pl.BlockSpec((TILE, channels), lambda t: (t, 0)),
            pl.BlockSpec((TILE, STATE_DIM), lambda t: (t, 0)),
            pl.BlockSpec((TILE, LANES), lambda t: (t, 0)),
            pl.BlockSpec((1, channels), lambda t: (0, 0)),
        ]
        + [pl.BlockSpec(state.shape, lambda t: (0, 0)) for state in states],
        out_specs=pl.BlockSpec((TILE, channels), lambda t: (t, 0)),
        out_shape=jax.ShapeDtypeStruct((length, channels), BF16),
        scratch_shapes=[
            pltpu.VMEM((TILE, channels), F32),
            pltpu.VMEM((len(states),) + states[0].shape, BF16),
        ],
        compiler_params=pltpu.CompilerParams(dimension_semantics=("arbitrary",)),
        cost_estimate=pl.CostEstimate(
            flops=3_000_000_000, bytes_accessed=16_000_000, transcendentals=4_000_000
        ),
        name="finish",
    )(place, part, gate, read, decay, norm_row, *states)


def most_per_pair(slots, peers):
    return (2 * slots + peers - 1) // peers


def padded_windows(inner_ref, outer_ref, total):
    taps, slots = inner_ref.shape[:2]
    width = inner_ref.shape[2] + outer_ref.shape[2]
    windows = []
    for tap in range(taps):
        both = [inner_ref[tap].astype(F32), outer_ref[tap].astype(F32)]
        both.append(jnp.zeros((slots, total - width), F32))
        windows.append(jnp.concatenate(both, axis=1))
    return windows


def mark_kernel(plan_ref, mask_ref, inner_ref, outer_ref, out_ref):
    peers, packet, _ = out_ref.shape
    taps, slots = inner_ref.shape[:2]
    chunks = (packet - 2) // taps
    fill = jnp.zeros((SLOT_PAD - slots, chunks * LANES), F32)
    row = lax.broadcasted_iota(jnp.int32, (peers, LANES), 0)
    lane = lax.broadcasted_iota(jnp.int32, (peers, LANES), 1)
    pick = jnp.zeros((peers, LANES), F32)
    peer_marks = jnp.zeros((1, LANES), F32)
    slot_marks = jnp.zeros((1, LANES), F32)
    for slot in range(slots):
        peer, target = plan_ref[0, slot], plan_ref[1, slot]
        here = (row == peer) & (lane == slot) & (target == 0)
        pick = jnp.where(here, mask_ref[slot].astype(F32), pick)
        peer_marks = jnp.where(lane[:1] == slot, peer.astype(F32), peer_marks)
        slot_marks = jnp.where(lane[:1] == slot, target.astype(F32), slot_marks)
    pick = pick[:, :SLOT_PAD].astype(BF16)
    picked = []
    for window in padded_windows(inner_ref, outer_ref, chunks * LANES):
        window = jnp.concatenate([window, fill], axis=0).astype(BF16)
        picked.append(dot(pick, window))
    spare = packet - chunks * taps - 2
    for peer in range(peers):
        lines = []
        for chunk in range(chunks):
            span = slice(chunk * LANES, (chunk + 1) * LANES)
            lines += [picked[tap][peer : peer + 1, span] for tap in range(taps)]
        lines += [peer_marks, slot_marks]
        if spare > 0:
            lines.append(jnp.zeros((spare, LANES), F32))
        out_ref[peer] = jnp.concatenate(lines, axis=0).astype(BF16)


def mark(plan, mask, inner, outer, peers):
    taps, _ = inner.shape[:2]
    width = inner.shape[2] + outer.shape[2]
    whole = pl.BlockSpec(memory_space=pltpu.VMEM)
    scalar = pl.BlockSpec(memory_space=pltpu.SMEM)
    packet = pl.cdiv(taps * pl.cdiv(width, LANES) + 2, 16) * 16
    return pl.pallas_call(
        mark_kernel,
        in_specs=[scalar, scalar, whole, whole],
        out_shape=jax.ShapeDtypeStruct((peers, packet, LANES), BF16),
        name="mark",
    )(plan, mask, inner, outer)


def window_kernel(plan_ref, mask_ref, inner_ref, outer_ref, out_ref, scr):
    peers = out_ref.shape[0]
    taps, slots = inner_ref.shape[:2]
    total = scr.shape[1]
    chunks = total // LANES
    padded = out_ref.shape[1] // chunks
    capacity = most_per_pair(slots, peers)
    at = total - LANES
    scr[...] = jnp.zeros((peers * padded, total), F32)
    windows = padded_windows(inner_ref, outer_ref, total)
    last = lax.broadcasted_iota(jnp.int32, (1, total), 1) == total - 1
    for line in range(peers * padded // 8):
        lane = lax.broadcasted_iota(jnp.int32, (8, LANES), 1)
        scr[line * 8 : line * 8 + 8, at:] = jnp.where(lane == LANES - 1, -1.0, 0.0)
    for slot in range(slots):
        peer, target = plan_ref[0, slot], plan_ref[1, slot]
        rank = jnp.int32(0)
        for earlier in range(slot):
            rank = rank + (plan_ref[0, earlier] == peer).astype(jnp.int32)
        keep = mask_ref[slot].astype(F32)
        for tap in range(taps):
            tag = (target + tap * SLOT_PAD).astype(F32)
            line = jnp.where(last, tag, windows[tap][slot : slot + 1] * keep)
            scr[pl.ds(peer * padded + tap * capacity + rank, 1), :] = line
    for peer in range(peers):
        for chunk in range(chunks):
            block = scr[peer * padded : (peer + 1) * padded, chunk * LANES : (chunk + 1) * LANES]
            out_ref[peer, chunk * padded : (chunk + 1) * padded, :] = block.astype(BF16)


def window_packets(plan, mask, inner, outer, peers):
    taps, slots = inner.shape[:2]
    width = inner.shape[2] + outer.shape[2]
    whole = pl.BlockSpec(memory_space=pltpu.VMEM)
    scalar = pl.BlockSpec(memory_space=pltpu.SMEM)
    total = width + LANES - width % LANES
    padded = pl.cdiv(taps * most_per_pair(slots, peers), 16) * 16
    return pl.pallas_call(
        window_kernel,
        in_specs=[scalar, scalar, whole, whole],
        out_shape=jax.ShapeDtypeStruct((peers, padded * (total // LANES), LANES), BF16),
        scratch_shapes=[pltpu.VMEM((peers * padded, total), F32)],
        name="window_packets",
    )(plan, mask, inner, outer)


def settle_kernel(got_ref, inner_own_ref, outer_own_ref, inner_ref, outer_ref):
    peers, lines, _ = got_ref.shape
    taps, slots, inner_local = inner_ref.shape
    width = inner_local + outer_ref.shape[2]
    chunks = width // LANES + 1
    padded = pl.cdiv(taps * most_per_pair(slots, peers), 16) * 16
    start = lines - chunks * padded
    rows = peers * padded
    parts = []
    for chunk in range(chunks):
        at = start + chunk * padded
        part = got_ref[:, at : at + padded, :].astype(F32)
        parts.append(part.reshape(rows, LANES))
    tags = parts[-1][:, LANES - 1 :]
    lane = lax.broadcasted_iota(jnp.int32, (rows, LANES), 1).astype(F32)
    pick = (tags == lane).astype(BF16)
    moved = dot(pick, jnp.concatenate(parts, axis=1).astype(BF16), ((0,), (0,)))
    top = lax.broadcasted_iota(jnp.int32, (SLOT_PAD, 1), 0) == 0
    for tap in range(taps):
        block = moved[tap * SLOT_PAD : (tap + 1) * SLOT_PAD]
        own = inner_own_ref[tap : tap + 1, :].astype(F32)
        inner_ref[tap] = jnp.where(top, own, block[:, :inner_local]).astype(BF16)[:slots]
        own = outer_own_ref[tap : tap + 1, :].astype(F32)
        outer_ref[tap] = jnp.where(top, own, block[:, inner_local:width]).astype(BF16)[:slots]


def settle(got, inner_own, outer_own, slots):
    taps, inner_local = inner_own.shape
    whole = pl.BlockSpec(memory_space=pltpu.VMEM)
    return pl.pallas_call(
        settle_kernel,
        in_specs=[whole, whole, whole],
        out_shape=[
            jax.ShapeDtypeStruct((taps, slots, inner_local), BF16),
            jax.ShapeDtypeStruct((taps, slots, outer_own.shape[1]), BF16),
        ],
        name="settle",
    )(got, inner_own, outer_own)


def pack_lead_kernel(own_ref, mask_ref, state_ref, out_ref):
    first_slot = pl.program_id(0) * SLOT_TILE
    for j in range(SLOT_TILE):
        keep = mask_ref[jnp.minimum(first_slot + j, mask_ref.shape[0] - 1)].astype(F32)
        out_ref[j] = (state_ref[j, 0] * keep).astype(BF16)


def pack_lead(own, mask, states, hop):
    slots, peers, piece, width = states.shape

    def from_peer(t, own, mask):
        return t, lax.rem(own[0] + hop, peers), 0, 0

    return pl.pallas_call(
        pack_lead_kernel,
        grid_spec=pltpu.PrefetchScalarGridSpec(
            num_scalar_prefetch=2,
            grid=(pl.cdiv(slots, SLOT_TILE),),
            in_specs=[pl.BlockSpec((SLOT_TILE, 1, piece, width), from_peer)],
            out_specs=pl.BlockSpec((SLOT_TILE, piece, width), lambda t, own, mask: (t, 0, 0)),
        ),
        out_shape=jax.ShapeDtypeStruct((slots, piece, width), BF16),
        compiler_params=pltpu.CompilerParams(dimension_semantics=("arbitrary",)),
        name="pack_lead",
    )(own, mask, states)


def pack_kernel(hops, own_ref, mask_ref, state_ref, *out_refs):
    first_slot = pl.program_id(0) * PACK_TILE
    peers = state_ref.shape[1]
    for j in range(PACK_TILE):
        keep = mask_ref[jnp.minimum(first_slot + j, mask_ref.shape[0] - 1)].astype(F32)
        for hop, out_ref in zip(hops, out_refs):
            peer = lax.rem(own_ref[0] + hop, peers)
            out_ref[j] = (state_ref[j, peer] * keep).astype(BF16)


def pack(own, mask, states, hops):
    slots, peers, piece, width = states.shape
    return pl.pallas_call(
        functools.partial(pack_kernel, hops),
        grid=(pl.cdiv(slots, PACK_TILE),),
        in_specs=[
            pl.BlockSpec(memory_space=pltpu.SMEM),
            pl.BlockSpec(memory_space=pltpu.SMEM),
            pl.BlockSpec((PACK_TILE, peers, piece, width), lambda t: (t, 0, 0, 0)),
        ],
        out_specs=[pl.BlockSpec((PACK_TILE, piece, width), lambda t: (t, 0, 0))] * len(hops),
        out_shape=[jax.ShapeDtypeStruct((slots, piece, width), BF16)] * len(hops),
        compiler_params=pltpu.CompilerParams(dimension_semantics=("arbitrary",)),
        name="pack",
    )(own, mask, states)


def source_of(table_ref, target):
    code = table_ref[0, target]
    peer = lax.div(code, SLOT_PAD)
    return peer, code - peer * SLOT_PAD


def pick_first_kernel(own_ref, table_ref, packet_ref, *refs):
    in_refs, out_ref, sem = refs[:-2], refs[-2], refs[-1]
    peers = len(in_refs)
    slots, piece, _ = in_refs[0].shape
    own_piece = pl.ds(0, piece)
    for target in range(peers):
        peer, index = source_of(table_ref, target * slots)
        source = lax.rem(own_ref[0] - peer + peers, peers)
        for hop in range(peers):

            @pl.when(source == hop)
            def _():
                pltpu.make_async_copy(
                    in_refs[hop].at[index], out_ref.at[target, own_piece], sem.at[target]
                ).start()

    for target in range(peers):
        out_ref[target, piece:, :] = packet_ref[target]
    for target in range(peers):
        pltpu.make_async_copy(
            in_refs[0].at[0], out_ref.at[target, own_piece], sem.at[target]
        ).wait()


def pick_first(own, table, packets, pieces):
    _, piece, width = pieces[0].shape
    peers = len(pieces)
    scalar = pl.BlockSpec(memory_space=pltpu.SMEM)
    return pl.pallas_call(
        pick_first_kernel,
        in_specs=[scalar, scalar, pl.BlockSpec(memory_space=pltpu.VMEM)]
        + [pl.BlockSpec(memory_space=pl.ANY)] * peers,
        out_specs=pl.BlockSpec(memory_space=pltpu.VMEM),
        out_shape=jax.ShapeDtypeStruct((peers, piece + packets.shape[1], width), BF16),
        scratch_shapes=[pltpu.SemaphoreType.DMA((peers,))],
        name="pick_first",
    )(own, table, packets, *pieces)


def gather_pieces(own_ref, refs, scr):
    peers = len(refs)
    for hop in range(peers):
        scr[lax.rem(own_ref[0] - hop + peers, peers)] = refs[hop][...]


def reorder_kernel(own_ref, table_ref, *refs):
    scr = refs[-1]
    peers, slots = scr.shape[:2]
    gather_pieces(own_ref, refs[:peers], scr)
    for hop in range(peers):
        base = lax.rem(own_ref[0] + hop, peers) * slots
        out_ref = refs[peers + hop]

        def move(slot, unused):
            peer, index = source_of(table_ref, base + slot)
            out_ref[slot - 1] = scr[peer, index]
            return unused

        lax.fori_loop(1, slots, move, 0)


def reorder_rest_kernel(own_ref, table_ref, *refs):
    out_ref, scr = refs[-2:]
    peers, slots = scr.shape[:2]
    gather_pieces(own_ref, refs[:peers], scr)
    for target in range(peers):

        def move(slot, unused):
            peer, index = source_of(table_ref, target * slots + slot)
            out_ref[target, slot - 1] = scr[peer, index]
            return unused

        lax.fori_loop(1, slots, move, 0)


def reorder(own, table, pieces, part):
    slots, piece, width = pieces[0].shape
    half = piece // 2
    peers = len(pieces)
    scalar = pl.BlockSpec(memory_space=pltpu.SMEM)
    if part == 0:
        one = (slots - 1, half, width)
        out_specs = [pl.BlockSpec(one, lambda t: (0, 0, 0))] * peers
        out_shape = [jax.ShapeDtypeStruct(one, BF16)] * peers
    else:
        all_rest = (peers, slots - 1, half, width)
        out_specs = pl.BlockSpec(all_rest, lambda t: (0, 0, 0, 0))
        out_shape = jax.ShapeDtypeStruct(all_rest, BF16)
    return pl.pallas_call(
        reorder_kernel if part == 0 else reorder_rest_kernel,
        grid=(1,),
        in_specs=[scalar, scalar]
        + [pl.BlockSpec((slots, half, width), lambda t: (0, part, 0))] * peers,
        out_specs=out_specs,
        out_shape=out_shape,
        scratch_shapes=[pltpu.VMEM((peers, slots, half, width), BF16)],
        name="reorder" if part == 0 else "reorder_rest",
    )(own, table, *pieces)


def unpack_kernel(own_ref, final_ref, *refs):
    piece_refs, out_ref = refs[:-1], refs[-1]
    step = pl.program_id(0)
    half = out_ref.shape[2]
    out_ref[0, 0] = final_ref[:half, :]
    for hop in range(len(piece_refs)):

        @pl.when(step == hop)
        def _():
            out_ref[1:, 0] = piece_refs[hop][...].astype(F32)


def unpack(own, final, pieces):
    others, half, width = pieces[0].shape
    peers = len(pieces)
    slots, piece = others + 1, 2 * half

    def from_peer(hop, own):
        return lax.rem(own[0] - hop + peers, peers)

    return pl.pallas_call(
        unpack_kernel,
        grid_spec=pltpu.PrefetchScalarGridSpec(
            num_scalar_prefetch=1,
            grid=(peers,),
            in_specs=[pl.BlockSpec((piece, width), lambda h, own: (from_peer(h, own), 0))]
            + [pl.BlockSpec((others, half, width), lambda h, own: (0, 0, 0))] * peers,
            out_specs=pl.BlockSpec(
                (slots, 1, half, width), lambda h, own: (0, from_peer(h, own), 0, 0)
            ),
        ),
        out_shape=jax.ShapeDtypeStruct((slots, peers, piece, width), F32),
        compiler_params=pltpu.CompilerParams(dimension_semantics=("arbitrary",)),
        name="unpack",
    )(own, final, *pieces)


def unpack_rest_kernel(final_ref, pieces_ref, states_ref, out_ref):
    peers, half = pieces_ref.shape[0], pieces_ref.shape[2]
    for p in range(peers):
        out_ref[0, p] = final_ref[(2 * p + 1) * half : (2 * p + 2) * half, :]
        out_ref[1:, p] = pieces_ref[p].astype(F32)


def unpack_rest(final, pieces, states):
    slots, peers, piece, width = states.shape
    half = piece // 2
    return pl.pallas_call(
        unpack_rest_kernel,
        grid=(peers // PEER_TILE,),
        in_specs=[
            pl.BlockSpec((PEER_TILE * piece, width), lambda p: (p, 0)),
            pl.BlockSpec((PEER_TILE, slots - 1, half, width), lambda p: (p, 0, 0, 0)),
            pl.BlockSpec(memory_space=pl.ANY),
        ],
        out_specs=pl.BlockSpec((slots, PEER_TILE, half, width), lambda p: (0, p, 1, 0)),
        out_shape=jax.ShapeDtypeStruct(states.shape, F32),
        input_output_aliases={2: 0},
        compiler_params=pltpu.CompilerParams(dimension_semantics=("arbitrary",)),
        name="unpack_rest",
    )(final, pieces, states)


def combine_kernel(place_ref, decay_ref, *refs):
    count = decay_ref.shape[0]
    end_scr, enter_scr = refs[-2:]
    final_ref = refs[-3]
    entering_refs = refs[-3 - count : -3]
    end_refs, first_ref = refs[:count], refs[count]
    chain = place_ref[0]
    for hop in range(count):
        end_scr[lax.rem(chain - hop + count, count)] = end_refs[hop][...]
    peers, piece, width = first_ref.shape
    state = first_ref[...].astype(F32).reshape(peers * piece, width).T
    for k in range(count):
        enter_scr[k] = state.astype(BF16)
        state = state * decay_ref[k : k + 1, :] + end_scr[k].astype(F32)
    for hop in range(count):
        entering_refs[hop][...] = enter_scr[lax.rem(chain + hop, count)]
    final_ref[...] = state.T


def combine(place, decay, ends, first):
    count = len(ends)
    whole = pl.BlockSpec(memory_space=pltpu.VMEM)
    rows, columns = ends[0].shape
    peers = first.shape[0]
    outs = pl.pallas_call(
        combine_kernel,
        grid=(1,),
        in_specs=[
            pl.BlockSpec(memory_space=pltpu.SMEM),
            pl.BlockSpec(decay.shape, lambda t: (0, 0)),
        ]
        + [pl.BlockSpec((rows, columns), lambda t: (0, 0))] * count
        + [pl.BlockSpec((peers, columns // peers, rows), lambda t: (0, 0, 0))],
        out_specs=[pl.BlockSpec((rows, columns), lambda t: (0, 0))] * count
        + [pl.BlockSpec((columns, rows), lambda t: (0, 0))],
        out_shape=[jax.ShapeDtypeStruct((rows, columns), BF16)] * count
        + [jax.ShapeDtypeStruct((columns, rows), F32)],
        scratch_shapes=[
            pltpu.VMEM((count, rows, columns), BF16),
            pltpu.VMEM((count, rows, columns), BF16),
        ],
        name="combine",
    )(place, decay, *ends, first)
    return outs[:count], outs[count]


def share_kernel(
    slot_count,
    place_ref,
    every_ref,
    end_ref,
    kept_ref,
    kept_next_ref,
    state_end_ref,
    state_kept_ref,
    state_next_ref,
    raw_ref,
    bias_ref,
    rate_ref,
    out_ref,
    step_ref,
    table_ref,
):
    taps = out_ref.shape[0]
    inner = end_ref.shape[1]
    outer = state_end_ref.shape[1]
    channels = inner + outer
    peers, packet, _ = every_ref.shape
    slots = float(slot_count)
    chunks = (packet - 2) // taps
    width = chunks * LANES
    everything = [every_ref[p].astype(F32) for p in range(peers)]
    firsts = everything[0]
    for part in everything[1:]:
        firsts = firsts + part
    at = chunks * taps
    target = jnp.concatenate([part[at : at + 1] for part in everything], axis=0) * slots
    target = target + jnp.concatenate([part[at + 1 : at + 2] for part in everything], axis=0)
    columns = table_ref.shape[1]
    lane = lax.broadcasted_iota(jnp.int32, (peers, columns), 1).astype(F32)
    code = lax.broadcasted_iota(jnp.int32, (peers, columns), 0).astype(F32) * SLOT_PAD
    found = jnp.zeros((peers, columns), F32)
    for slot in range(slot_count):
        found = found + jnp.where(target[:, slot : slot + 1] == lane, code + slot, 0.0)
    found = jnp.sum(found, axis=0, keepdims=True)
    table_ref[...] = jnp.broadcast_to(found, table_ref.shape).astype(jnp.int32)
    low_block, high_block, start, length = (
        place_ref[0],
        place_ref[1],
        place_ref[2],
        place_ref[3],
    )
    out_ref[:, :inner] = end_ref[16 - taps :, :]
    out_ref[:, inner:channels] = state_end_ref[16 - taps :, :]
    here = lax.broadcasted_iota(jnp.int32, (16, 1), 0)
    wanted = length - taps - start

    def kept_rows(low_ref, high_ref):
        low = low_ref[...].astype(F32)
        high = high_ref[...].astype(F32)
        found = []
        for i in range(taps):
            in_low = (low_block * 16 + here) == (wanted + i)
            in_high = ((high_block * 16 + here) == (wanted + i)) & (high_block > low_block)
            picked = jnp.where(in_low, low, 0.0) + jnp.where(in_high, high, 0.0)
            found.append(jnp.sum(picked, axis=0, keepdims=True))
        return jnp.concatenate(found, axis=0).astype(BF16)

    out_ref[:, channels : channels + inner] = kept_rows(kept_ref, kept_next_ref)
    out_ref[:, channels + inner : 2 * channels] = kept_rows(state_kept_ref, state_next_ref)
    for chunk in range(chunks):
        at = 2 * channels + chunk * LANES
        lines = firsts[chunk * taps : (chunk + 1) * taps]
        out_ref[:, at : at + LANES] = lines.astype(BF16)
    count = step_ref.shape[0]
    heads = raw_ref.shape[1]
    positions = start + lax.broadcasted_iota(jnp.int32, (count, heads), 0)
    raw = raw_ref[...].astype(F32) + bias_ref[...]
    step = jnp.maximum(raw, 0.0) + jnp.log1p(jnp.exp(-jnp.abs(raw)))
    step = jnp.where(positions < length, step, 0.0)
    step = jnp.concatenate([step, jnp.zeros((count, LANES - heads), F32)], axis=1)
    step_ref[...] = step
    total = jnp.sum(step * rate_ref[...], axis=0, keepdims=True)
    high = total.astype(BF16).astype(F32)
    middle = (total - high).astype(BF16).astype(F32)
    rest = total - high - middle
    parts = jnp.concatenate([high, middle, rest], axis=0)
    out_ref[:, 2 * channels + width :] = parts.astype(BF16)


def share(place, slots, every, rows, state_rows, step_raw, step_bias, rate):
    peers, packet, _ = every.shape
    taps = KERNEL - 1
    width = (packet - 2) // taps * LANES
    length, inner = rows.shape
    outer = state_rows.shape[1]
    heads = step_raw.shape[1]
    last = length // 16 - 1
    total = 2 * (inner + outer) + width + LANES
    lanes = pl.cdiv(peers * slots, LANES) * LANES
    return pl.pallas_call(
        functools.partial(share_kernel, slots),
        grid_spec=pltpu.PrefetchScalarGridSpec(
            num_scalar_prefetch=1,
            grid=(1,),
            in_specs=[
                pl.BlockSpec(every.shape, lambda t, c: (0, 0, 0)),
                pl.BlockSpec((16, inner), lambda t, c: (last, 0)),
                pl.BlockSpec((16, inner), lambda t, c: (c[0], 0)),
                pl.BlockSpec((16, inner), lambda t, c: (c[1], 0)),
                pl.BlockSpec((16, outer), lambda t, c: (last, 0)),
                pl.BlockSpec((16, outer), lambda t, c: (c[0], 0)),
                pl.BlockSpec((16, outer), lambda t, c: (c[1], 0)),
                pl.BlockSpec((length, heads), lambda t, c: (0, 0)),
                pl.BlockSpec((1, heads), lambda t, c: (0, 0)),
                pl.BlockSpec((1, LANES), lambda t, c: (0, 0)),
            ],
            out_specs=[
                pl.BlockSpec((taps, total), lambda t, c: (0, 0)),
                pl.BlockSpec((length, LANES), lambda t, c: (0, 0)),
                pl.BlockSpec((8, lanes), lambda t, c: (0, 0)),
            ],
        ),
        out_shape=[
            jax.ShapeDtypeStruct((taps, total), BF16),
            jax.ShapeDtypeStruct((length, LANES), F32),
            jax.ShapeDtypeStruct((8, lanes), jnp.int32),
        ],
        name="share",
    )(
        place,
        every,
        rows,
        rows,
        rows,
        state_rows,
        state_rows,
        state_rows,
        step_raw,
        step_bias,
        rate,
    )


def tail_kernel(
    chain_ref, shared_ref, tail_ref, inner_ref, outer_ref, decay_ref
):
    chain = chain_ref[0]
    count, taps = shared_ref.shape[:2]
    inner_local, outer_local = inner_ref.shape[1], outer_ref.shape[1]
    channels = tail_ref.shape[1]
    inner = count * inner_local
    at = 2 * channels
    window = jnp.concatenate(
        [shared_ref[s, :, at : at + inner_local] for s in range(count)]
        + [
            shared_ref[s, :, at + inner_local : at + inner_local + outer_local]
            for s in range(count)
        ],
        axis=1,
    ).astype(F32)
    earlier = shared_ref[jnp.maximum(chain - 1, 0), :, :channels].astype(F32)
    tail = jnp.where(chain == 0, window, earlier)
    tail_ref[...] = jnp.concatenate([jnp.zeros((8 - taps, channels), F32), tail], axis=0)
    kept = shared_ref[0, :, channels:at].astype(F32)
    for s in range(1, count):
        kept = kept + shared_ref[s, :, channels:at].astype(F32)
    own_inner = jnp.zeros((taps, inner_local), F32)
    own_outer = jnp.zeros((taps, outer_local), F32)
    for s in range(count):
        mine = chain == s
        inner_at, outer_at = s * inner_local, inner + s * outer_local
        own_inner = jnp.where(mine, kept[:, inner_at : inner_at + inner_local], own_inner)
        own_outer = jnp.where(mine, kept[:, outer_at : outer_at + outer_local], own_outer)
    inner_ref[...] = own_inner.astype(BF16)
    outer_ref[...] = own_outer.astype(BF16)
    logs = []
    for s in range(count):
        parts = shared_ref[s, :, shared_ref.shape[2] - LANES :].astype(F32)
        logs.append(jnp.sum(parts, axis=0, keepdims=True))
    logs = jnp.concatenate(logs + [jnp.zeros((8 - count, LANES), F32)] * (count < 8), axis=0)
    columns = decay_ref.shape[1]
    head = lax.broadcasted_iota(jnp.int32, (LANES, columns), 0)
    lane = lax.broadcasted_iota(jnp.int32, (LANES, columns), 1)
    local_heads = columns // HEAD_DIM
    pick = (head == chain * local_heads + lane // HEAD_DIM).astype(F32)
    spread = dot(logs, pick, precision=lax.Precision.HIGHEST)
    decay_ref[...] = jnp.exp2(spread[:count])


def tails(chain, shared, channels, inner_local, outer_local, columns):
    count, taps = shared.shape[:2]
    whole = pl.BlockSpec(memory_space=pltpu.VMEM)
    return pl.pallas_call(
        tail_kernel,
        in_specs=[pl.BlockSpec(memory_space=pltpu.SMEM), whole],
        out_shape=[
            jax.ShapeDtypeStruct((8, channels), F32),
            jax.ShapeDtypeStruct((taps, inner_local), BF16),
            jax.ShapeDtypeStruct((taps, outer_local), BF16),
            jax.ShapeDtypeStruct((count, columns), F32),
        ],
        name="tails",
    )(chain, shared)


def exchange(value, axis):
    return lax.all_to_all(value, axis, split_axis=0, concat_axis=0, tiled=True)


def hop_order(count):
    return sorted(range(1, count), key=lambda hop: abs(2 * hop - count))


def send(value, axis, hop):
    count = lax.axis_size(axis)
    pairs = [(source, (source + hop) % count) for source in range(count)]
    return lax.ppermute(value, axis, pairs)


def rotate(values, axis):
    got = list(values)
    for hop in hop_order(len(got)):
        got[hop] = send(values[hop], axis, hop)
    return got


def device_body(
    pool_states,
    inner_window,
    state_window,
    move_plan,
    active_mask,
    inputs_inner,
    inputs_state,
    gate_rows,
    step_raw,
    lengths,
    conv_weight,
    conv_bias,
    step_bias,
    decay_log,
    skip_weight,
    norm_weight,
):
    peers = lax.axis_size("req")
    own_peer = lax.axis_index("req").astype(jnp.int32)
    chain_size = lax.axis_size("seq")
    chain_index = lax.axis_index("seq").astype(jnp.int32)
    slots, local_heads = pool_states.shape[:2]
    columns = local_heads * HEAD_DIM
    piece = columns // peers
    taps = KERNEL - 1
    inner_local = inner_window.shape[2]
    outer_local = state_window.shape[2]

    own = own_peer[None]
    pool_pieces = pool_states.reshape(slots, peers, piece, STATE_DIM)
    lead, *others = hop_order(peers)
    spread = [None] * peers
    lead_pieces = pack_lead(own, active_mask, pool_pieces, lead)
    spread[lead] = send(lead_pieces, "req", lead)
    plan = move_plan.T
    inner_taps = inner_window.transpose(1, 0, 2)
    outer_taps = state_window.transpose(1, 0, 2)
    packed = mark(plan, active_mask, inner_taps, outer_taps, peers)
    every = exchange(packed, "req")
    others = [0] + others
    for hop, pieces in zip(others, pack(own, active_mask, pool_pieces, others)):
        spread[hop] = pieces if hop == 0 else send(pieces, "req", hop)

    rows = inputs_inner[0]
    state_rows = inputs_state[0]
    local_length, inner_dim = rows.shape
    channels = inner_dim + state_rows.shape[1]
    start = chain_index * local_length
    length = lengths[0]
    last_tile = local_length // 16 - 1
    low_block = jnp.clip((length - taps - start) // 16, 0, last_tile)
    high_block = jnp.minimum(low_block + 1, last_tile)
    heads = decay_log.shape[0]
    rate = jnp.pad(-LOG2E * jnp.exp(decay_log), (0, LANES - heads))[None]
    payload, step, table = share(
        jnp.stack([low_block, high_block, start, length]),
        slots,
        every,
        rows,
        state_rows,
        step_raw[0],
        step_bias[None],
        rate,
    )
    shared = lax.all_gather(payload, "seq", axis=0)
    chain = chain_index[None]
    tail, kept_inner, kept_outer, own_decay = tails(
        chain, shared, channels, inner_local, outer_local, columns
    )
    packets = window_packets(plan, active_mask, inner_taps, outer_taps, peers)

    part, local_end, read_rows, decay = block_parts(
        chain,
        tail,
        rows,
        state_rows,
        step,
        rate,
        conv_weight,
        conv_bias[None],
        jnp.repeat(skip_weight, HEAD_DIM)[None],
        chain_size,
    )
    own_ends = rotate(local_end, "seq")

    first = exchange(pick_first(own, table, packets, spread), "req")
    moved_a = rotate(reorder(own, table, spread, 0), "req")
    moved_b = exchange(reorder(own, table, spread, 1), "req")
    entering, final = combine(chain, own_decay, own_ends, first)
    new_inner, new_outer = settle(first, kept_inner, kept_outer, slots)
    incoming = rotate(entering, "seq")
    mixer_out = finish(
        jnp.stack([start, length, chain_index]),
        part,
        gate_rows[0],
        read_rows,
        decay,
        norm_weight[None],
        incoming,
    )
    states = unpack(own, final, moved_a)
    new_states = unpack_rest(final, moved_b, states).reshape(pool_states.shape)

    return (
        new_states,
        new_inner.transpose(1, 0, 2),
        new_outer.transpose(1, 0, 2),
        mixer_out[None],
    )


def solution(mesh):
    return jax.shard_map(
        device_body,
        mesh=mesh,
        in_specs=(
            P("req", "seq", None, None),
            P("req", None, "seq"),
            P("req", None, "seq"),
            P("req", None),
            P("req"),
            P("req", "seq", None),
            P("req", "seq", None),
            P("req", "seq", None),
            P("req", "seq", None),
            P("req"),
            P(),
            P(),
            P(),
            P(),
            P(),
            P(),
        ),
        out_specs=(
            P("req", "seq", None, None),
            P("req", None, "seq"),
            P("req", None, "seq"),
            P("req", "seq", None),
        ),
        check_vma=False,
    )
```

```python
import functools
import math

import jax
import jax.numpy as jnp
from jax import lax
from jax.experimental import pallas as pl
from jax.experimental.pallas import tpu as pltpu
from jax.sharding import PartitionSpec as P


HEAD_DIM = 64
STATE_DIM = 128
KERNEL = 4
BLOCK_LEN = 256
GROUP = 8
HALF = BLOCK_LEN // 2
GROUP_DIM = GROUP * HEAD_DIM
PAIR_DIM = 2 * HEAD_DIM
LANES = 128
TILE = 128
SLOT_PAD = 16
PEER_TILE = 2
PACK_TILE = 2
EPSILON = 1e-05
LOG2E = math.log2(math.e)
F32 = jnp.float32
BF16 = jnp.bfloat16


def dot(a, b, dims=((1,), (0,)), precision=None):
    return lax.dot_general(a, b, (dims, ((), ())), precision=precision, preferred_element_type=F32)


def silu(v):
    half = 0.5 * v
    return half + half * jnp.tanh(half)


def conv_silu(tail, rows, weight, bias_row):
    extended = jnp.concatenate([tail, rows.astype(F32)], axis=0)
    count = rows.shape[0]
    start = tail.shape[0] - KERNEL + 1
    running = bias_row + weight[0:1] * extended[start : start + count]
    for k in range(1, KERNEL):
        running = running + weight[k : k + 1] * extended[start + k : start + k + count]
    return silu(running)


def pair_of(columns, i, low):
    return jnp.where(low, columns[:, 2 * i : 2 * i + 1], columns[:, 2 * i + 1 : 2 * i + 2])


def block_kernel(
    chain_ref,
    tail_ref,
    prev_ref,
    rows_ref,
    state_tail_ref,
    state_prev_ref,
    state_rows_ref,
    step_ref,
    rate_ref,
    weight_ref,
    bias_ref,
    state_weight_ref,
    state_bias_ref,
    skip_ref,
    part_ref,
    end_ref,
    read_ref,
    decay_ref,
    scores_scr,
    cum_scr,
    cum_t_scr,
    to_end_scr,
    decay_scr,
    write_t_scr,
    offset_scr,
    carry_scr,
):
    block = pl.program_id(0)
    group = pl.program_id(1)
    first = block == 0

    @pl.when(group == 0)
    def _():
        state_tail = jnp.where(first, state_tail_ref[...], state_prev_ref[8:16, :].astype(F32))
        mixed = conv_silu(state_tail, state_rows_ref[...], state_weight_ref[...], state_bias_ref[...])
        write = mixed[:, :STATE_DIM]
        read = mixed[:, STATE_DIM:].astype(BF16)
        read_ref[...] = read
        write_b = write.astype(BF16)
        scores_scr[...] = dot(read, write_b, ((1,), (1,)))
        write_t_scr[...] = write_b.astype(F32).T.astype(BF16)
        row = lax.broadcasted_iota(jnp.int32, (BLOCK_LEN, BLOCK_LEN), 0)
        col = lax.broadcasted_iota(jnp.int32, (BLOCK_LEN, BLOCK_LEN), 1)
        triangle = (row >= col).astype(F32)
        step = step_ref[...]
        cum = dot(triangle, step * rate_ref[...], precision=lax.Precision.HIGHEST)
        cum_scr[...] = cum
        cum_t_scr[...] = cum.T
        last = cum[BLOCK_LEN - 1 :, :]
        to_end_scr[...] = jnp.exp2(last - cum) * step
        decay_scr[...] = jnp.exp2(cum)
        offset = jnp.where(first, 0.0, offset_scr[0:1, :])
        decay_ref[...] = jnp.exp2(offset + cum)
        offset_scr[0:1, :] = offset + last

    shift = lax.rem(LANES - group * GROUP, LANES)
    cum = pltpu.roll(cum_scr[...], shift, 1)
    step = pltpu.roll(step_ref[...], shift, 1)
    to_end = pltpu.roll(to_end_scr[...], shift, 1)
    decay = pltpu.roll(decay_scr[...], shift, 1)
    cum_t = cum_t_scr[pl.ds(pl.multiple_of(group * GROUP, GROUP), GROUP), :]
    read = read_ref[...]
    write_t = write_t_scr[...]
    carry = jnp.where(first, 0.0, carry_scr[group])
    carry_b = carry.astype(BF16)
    low = lax.broadcasted_iota(jnp.int32, (1, PAIR_DIM), 1) < HEAD_DIM
    causal = lax.broadcasted_iota(jnp.int32, (HALF, HALF), 0) >= lax.broadcasted_iota(
        jnp.int32, (HALF, HALF), 1
    )
    scores_top = scores_scr[0:HALF, 0:HALF]
    scores_left = scores_scr[HALF:, 0:HALF]
    scores_right = scores_scr[HALF:, HALF:]

    def head_weights(i):
        later = cum[:, i : i + 1]
        earlier = cum_t[i : i + 1, :]
        gap_top = jnp.where(causal, later[:HALF] - earlier[:, :HALF], -1e30)
        gap_left = later[HALF:] - earlier[:, :HALF]
        gap_right = jnp.where(causal, later[HALF:] - earlier[:, HALF:], -1e30)
        top = (scores_top * jnp.exp2(gap_top)).astype(BF16)
        left = (scores_left * jnp.exp2(gap_left)).astype(BF16)
        right = (scores_right * jnp.exp2(gap_right)).astype(BF16)
        return top, jnp.concatenate([left, right], axis=1)

    for i in range(GROUP // 2):
        span = slice(i * PAIR_DIM, (i + 1) * PAIR_DIM)
        tail = jnp.where(first, tail_ref[:, span], prev_ref[8:16, span].astype(F32))
        mixed = conv_silu(tail, rows_ref[:, span], weight_ref[:, span], bias_ref[:, span])
        value = mixed.astype(BF16).astype(F32)
        stepped = (pair_of(step, i, low) * value).astype(BF16)
        scaled = (pair_of(to_end, i, low) * value).astype(BF16)
        stepped_low = jnp.where(low, stepped, jnp.zeros_like(stepped))
        stepped_high = jnp.where(low, jnp.zeros_like(stepped), stepped)
        top_0, bottom_0 = head_weights(2 * i)
        top_1, bottom_1 = head_weights(2 * i + 1)
        intra_top = dot(top_0, stepped_low[:HALF]) + dot(top_1, stepped_high[:HALF])
        intra_bottom = dot(bottom_0, stepped_low) + dot(bottom_1, stepped_high)
        inter = dot(read, carry_b[:, span]) * pair_of(decay, i, low)
        direct = inter + skip_ref[:, span] * value
        part_ref[0:HALF, span] = intra_top + direct[:HALF]
        part_ref[HALF:, span] = intra_bottom + direct[HALF:]
        kept = pair_of(decay[BLOCK_LEN - 1 :, :], i, low) * carry[:, span]
        ending = kept + dot(write_t, scaled)
        carry_scr[group, :, span] = ending
        end_ref[0, :, span] = ending.astype(BF16)


def block_parts(chain, tail, rows, state_rows, step, rate, weight, bias_row, skip_row, ends):
    length = rows.shape[0]
    channels = rows.shape[1]
    blocks = length // BLOCK_LEN
    groups = channels // GROUP_DIM
    end_groups = groups // ends
    state_dim = state_rows.shape[1]
    state_at = channels // state_dim
    per_block = BLOCK_LEN // 16

    def before(b):
        return jnp.maximum(b * per_block - 1, 0)

    def end_at(b, g, chain):
        return lax.rem(g // end_groups - chain[0] + ends, ends), 0, lax.rem(g, end_groups)

    return pl.pallas_call(
        block_kernel,
        grid_spec=pltpu.PrefetchScalarGridSpec(
        num_scalar_prefetch=1,
        grid=(blocks, groups),
        in_specs=[
            pl.BlockSpec((8, GROUP_DIM), lambda b, g, c: (0, g)),
            pl.BlockSpec((16, GROUP_DIM), lambda b, g, c: (before(b), g)),
            pl.BlockSpec((BLOCK_LEN, GROUP_DIM), lambda b, g, c: (b, g)),
            pl.BlockSpec((8, state_dim), lambda b, g, c: (0, state_at)),
            pl.BlockSpec((16, state_dim), lambda b, g, c: (before(b), 0)),
            pl.BlockSpec((BLOCK_LEN, state_dim), lambda b, g, c: (b, 0)),
            pl.BlockSpec((BLOCK_LEN, LANES), lambda b, g, c: (b, 0)),
            pl.BlockSpec((1, LANES), lambda b, g, c: (0, 0)),
            pl.BlockSpec((KERNEL, GROUP_DIM), lambda b, g, c: (0, g)),
            pl.BlockSpec((1, GROUP_DIM), lambda b, g, c: (0, g)),
            pl.BlockSpec((KERNEL, state_dim), lambda b, g, c: (0, state_at)),
            pl.BlockSpec((1, state_dim), lambda b, g, c: (0, state_at)),
            pl.BlockSpec((1, GROUP_DIM), lambda b, g, c: (0, g)),
        ],
        out_specs=[
            pl.BlockSpec((BLOCK_LEN, GROUP_DIM), lambda b, g, c: (b, g)),
            pl.BlockSpec((1, STATE_DIM, GROUP_DIM), end_at),
            pl.BlockSpec((BLOCK_LEN, STATE_DIM), lambda b, g, c: (b, 0)),
            pl.BlockSpec((BLOCK_LEN, LANES), lambda b, g, c: (b, 0)),
        ],
        scratch_shapes=[
            pltpu.VMEM((BLOCK_LEN, BLOCK_LEN), F32),
            pltpu.VMEM((BLOCK_LEN, LANES), F32),
            pltpu.VMEM((LANES, BLOCK_LEN), F32),
            pltpu.VMEM((BLOCK_LEN, LANES), F32),
            pltpu.VMEM((BLOCK_LEN, LANES), F32),
            pltpu.VMEM((STATE_DIM, BLOCK_LEN), BF16),
            pltpu.VMEM((8, LANES), F32),
            pltpu.VMEM((groups, STATE_DIM, GROUP_DIM), F32),
        ],
        ),
        out_shape=[
            jax.ShapeDtypeStruct((length, channels), F32),
            jax.ShapeDtypeStruct((ends, STATE_DIM, channels // ends), BF16),
            jax.ShapeDtypeStruct((length, STATE_DIM), BF16),
            jax.ShapeDtypeStruct((length, LANES), F32),
        ],
        compiler_params=pltpu.CompilerParams(dimension_semantics=("arbitrary", "arbitrary")),
        cost_estimate=pl.CostEstimate(
            flops=6_000_000_000, bytes_accessed=20_000_000, transcendentals=10_000_000
        ),
        name="block_parts",
    )(
        chain,
        tail,
        rows,
        rows,
        tail,
        state_rows,
        state_rows,
        step,
        rate,
        weight,
        bias_row,
        weight,
        bias_row,
        skip_row,
    )


def finish_kernel(
    place_ref, part_ref, gate_ref, read_ref, decay_ref, norm_ref, *refs
):
    state_refs, out_ref, gated_scr, state_scr = refs[:-3], refs[-3], refs[-2], refs[-1]
    tile = pl.program_id(0)
    chunks, _, width = state_scr.shape

    @pl.when(tile == 0)
    def _():
        for hop in range(chunks):
            state_scr[lax.rem(place_ref[2] - hop + chunks, chunks)] = state_refs[hop][...]

    positions = (
        place_ref[0] + tile * TILE + lax.broadcasted_iota(jnp.int32, (TILE, PAIR_DIM), 0)
    )
    valid = (positions < place_ref[1]).astype(F32)
    low = lax.broadcasted_iota(jnp.int32, (1, PAIR_DIM), 1) < HEAD_DIM
    read = read_ref[...]
    decay = decay_ref[...]
    total = jnp.zeros((TILE, PAIR_DIM), F32)
    for chunk in range(chunks):
        for i in range(width // PAIR_DIM):
            pair = chunk * (width // PAIR_DIM) + i
            span = slice(pair * PAIR_DIM, (pair + 1) * PAIR_DIM)
            inter = dot(read, state_scr[chunk, :, i * PAIR_DIM : (i + 1) * PAIR_DIM])
            y = part_ref[:, span] + inter * pair_of(decay, pair, low)
            y = (y * valid).astype(BF16).astype(F32)
            gated = y * silu(gate_ref[:, span].astype(F32))
            gated_scr[:, span] = gated
            total = total + gated * gated
    channels = chunks * width
    mean = jnp.sum(total, axis=1, keepdims=True) * (1.0 / channels)
    scale = lax.rsqrt(mean + EPSILON)
    for pair in range(channels // PAIR_DIM):
        span = slice(pair * PAIR_DIM, (pair + 1) * PAIR_DIM)
        out_ref[:, span] = (gated_scr[:, span] * scale * norm_ref[:, span]).astype(BF16)


def finish(place, part, gate, read, decay, norm_row, states):
    length, channels = part.shape
    return pl.pallas_call(
        finish_kernel,
        grid=(length // TILE,),
        in_specs=[
            pl.BlockSpec(memory_space=pltpu.SMEM),
            pl.BlockSpec((TILE, channels), lambda t: (t, 0)),
            pl.BlockSpec((TILE, channels), lambda t: (t, 0)),
            pl.BlockSpec((TILE, STATE_DIM), lambda t: (t, 0)),
            pl.BlockSpec((TILE, LANES), lambda t: (t, 0)),
            pl.BlockSpec((1, channels), lambda t: (0, 0)),
        ]
        + [pl.BlockSpec(state.shape, lambda t: (0, 0)) for state in states],
        out_specs=pl.BlockSpec((TILE, channels), lambda t: (t, 0)),
        out_shape=jax.ShapeDtypeStruct((length, channels), BF16),
        scratch_shapes=[
            pltpu.VMEM((TILE, channels), F32),
            pltpu.VMEM((len(states),) + states[0].shape, BF16),
        ],
        compiler_params=pltpu.CompilerParams(dimension_semantics=("arbitrary",)),
        cost_estimate=pl.CostEstimate(
            flops=3_000_000_000, bytes_accessed=16_000_000, transcendentals=4_000_000
        ),
        name="finish",
    )(place, part, gate, read, decay, norm_row, *states)


def most_per_pair(slots, peers):
    return (2 * slots + peers - 1) // peers


def padded_windows(inner_ref, outer_ref, total):
    taps, slots = inner_ref.shape[:2]
    width = inner_ref.shape[2] + outer_ref.shape[2]
    windows = []
    for tap in range(taps):
        both = [inner_ref[tap].astype(F32), outer_ref[tap].astype(F32)]
        both.append(jnp.zeros((slots, total - width), F32))
        windows.append(jnp.concatenate(both, axis=1))
    return windows


def mark_kernel(plan_ref, mask_ref, inner_ref, outer_ref, out_ref):
    peers, packet, _ = out_ref.shape
    taps, slots = inner_ref.shape[:2]
    chunks = (packet - 2) // taps
    fill = jnp.zeros((SLOT_PAD - slots, chunks * LANES), F32)
    row = lax.broadcasted_iota(jnp.int32, (peers, LANES), 0)
    lane = lax.broadcasted_iota(jnp.int32, (peers, LANES), 1)
    pick = jnp.zeros((peers, LANES), F32)
    peer_marks = jnp.zeros((1, LANES), F32)
    slot_marks = jnp.zeros((1, LANES), F32)
    for slot in range(slots):
        peer, target = plan_ref[0, slot], plan_ref[1, slot]
        here = (row == peer) & (lane == slot) & (target == 0)
        pick = jnp.where(here, mask_ref[slot].astype(F32), pick)
        peer_marks = jnp.where(lane[:1] == slot, peer.astype(F32), peer_marks)
        slot_marks = jnp.where(lane[:1] == slot, target.astype(F32), slot_marks)
    pick = pick[:, :SLOT_PAD].astype(BF16)
    picked = []
    for window in padded_windows(inner_ref, outer_ref, chunks * LANES):
        window = jnp.concatenate([window, fill], axis=0).astype(BF16)
        picked.append(dot(pick, window))
    spare = packet - chunks * taps - 2
    for peer in range(peers):
        lines = []
        for chunk in range(chunks):
            span = slice(chunk * LANES, (chunk + 1) * LANES)
            lines += [picked[tap][peer : peer + 1, span] for tap in range(taps)]
        lines += [peer_marks, slot_marks]
        if spare > 0:
            lines.append(jnp.zeros((spare, LANES), F32))
        out_ref[peer] = jnp.concatenate(lines, axis=0).astype(BF16)


def mark(plan, mask, inner, outer, peers):
    taps, _ = inner.shape[:2]
    width = inner.shape[2] + outer.shape[2]
    whole = pl.BlockSpec(memory_space=pltpu.VMEM)
    scalar = pl.BlockSpec(memory_space=pltpu.SMEM)
    packet = pl.cdiv(taps * pl.cdiv(width, LANES) + 2, 16) * 16
    return pl.pallas_call(
        mark_kernel,
        in_specs=[scalar, scalar, whole, whole],
        out_shape=jax.ShapeDtypeStruct((peers, packet, LANES), BF16),
        name="mark",
    )(plan, mask, inner, outer)


def window_kernel(plan_ref, mask_ref, inner_ref, outer_ref, out_ref, scr):
    peers = out_ref.shape[0]
    taps, slots = inner_ref.shape[:2]
    total = scr.shape[1]
    chunks = total // LANES
    padded = out_ref.shape[1] // chunks
    capacity = most_per_pair(slots, peers)
    at = total - LANES
    scr[...] = jnp.zeros((peers * padded, total), F32)
    windows = padded_windows(inner_ref, outer_ref, total)
    last = lax.broadcasted_iota(jnp.int32, (1, total), 1) == total - 1
    for line in range(peers * padded // 8):
        lane = lax.broadcasted_iota(jnp.int32, (8, LANES), 1)
        scr[line * 8 : line * 8 + 8, at:] = jnp.where(lane == LANES - 1, -1.0, 0.0)
    for slot in range(slots):
        peer, target = plan_ref[0, slot], plan_ref[1, slot]
        rank = jnp.int32(0)
        for earlier in range(slot):
            rank = rank + (plan_ref[0, earlier] == peer).astype(jnp.int32)
        keep = mask_ref[slot].astype(F32)
        for tap in range(taps):
            tag = (target + tap * SLOT_PAD).astype(F32)
            line = jnp.where(last, tag, windows[tap][slot : slot + 1] * keep)
            scr[pl.ds(peer * padded + tap * capacity + rank, 1), :] = line
    for peer in range(peers):
        for chunk in range(chunks):
            block = scr[peer * padded : (peer + 1) * padded, chunk * LANES : (chunk + 1) * LANES]
            out_ref[peer, chunk * padded : (chunk + 1) * padded, :] = block.astype(BF16)


def window_packets(plan, mask, inner, outer, peers):
    taps, slots = inner.shape[:2]
    width = inner.shape[2] + outer.shape[2]
    whole = pl.BlockSpec(memory_space=pltpu.VMEM)
    scalar = pl.BlockSpec(memory_space=pltpu.SMEM)
    total = width + LANES - width % LANES
    padded = pl.cdiv(taps * most_per_pair(slots, peers), 16) * 16
    return pl.pallas_call(
        window_kernel,
        in_specs=[scalar, scalar, whole, whole],
        out_shape=jax.ShapeDtypeStruct((peers, padded * (total // LANES), LANES), BF16),
        scratch_shapes=[pltpu.VMEM((peers * padded, total), F32)],
        name="window_packets",
    )(plan, mask, inner, outer)


def settle_kernel(got_ref, inner_own_ref, outer_own_ref, inner_ref, outer_ref):
    peers, lines, _ = got_ref.shape
    taps, slots, inner_local = inner_ref.shape
    width = inner_local + outer_ref.shape[2]
    chunks = width // LANES + 1
    padded = pl.cdiv(taps * most_per_pair(slots, peers), 16) * 16
    start = lines - chunks * padded
    rows = peers * padded
    parts = []
    for chunk in range(chunks):
        at = start + chunk * padded
        part = got_ref[:, at : at + padded, :].astype(F32)
        parts.append(part.reshape(rows, LANES))
    tags = parts[-1][:, LANES - 1 :]
    lane = lax.broadcasted_iota(jnp.int32, (rows, LANES), 1).astype(F32)
    pick = (tags == lane).astype(BF16)
    moved = dot(pick, jnp.concatenate(parts, axis=1).astype(BF16), ((0,), (0,)))
    top = lax.broadcasted_iota(jnp.int32, (SLOT_PAD, 1), 0) == 0
    for tap in range(taps):
        block = moved[tap * SLOT_PAD : (tap + 1) * SLOT_PAD]
        own = inner_own_ref[tap : tap + 1, :].astype(F32)
        inner_ref[tap] = jnp.where(top, own, block[:, :inner_local]).astype(BF16)[:slots]
        own = outer_own_ref[tap : tap + 1, :].astype(F32)
        outer_ref[tap] = jnp.where(top, own, block[:, inner_local:width]).astype(BF16)[:slots]


def settle(got, inner_own, outer_own, slots):
    taps, inner_local = inner_own.shape
    whole = pl.BlockSpec(memory_space=pltpu.VMEM)
    return pl.pallas_call(
        settle_kernel,
        in_specs=[whole, whole, whole],
        out_shape=[
            jax.ShapeDtypeStruct((taps, slots, inner_local), BF16),
            jax.ShapeDtypeStruct((taps, slots, outer_own.shape[1]), BF16),
        ],
        name="settle",
    )(got, inner_own, outer_own)


def pack_lead_kernel(own_ref, mask_ref, state_ref, out_ref):
    for slot in range(out_ref.shape[0]):
        keep = mask_ref[slot].astype(F32)
        out_ref[slot] = (state_ref[slot, 0] * keep).astype(BF16)


def pack_lead(own, mask, states, hop):
    slots, peers, piece, width = states.shape

    def from_peer(t, own, mask):
        return 0, lax.rem(own[0] + hop, peers), 0, 0

    return pl.pallas_call(
        pack_lead_kernel,
        grid_spec=pltpu.PrefetchScalarGridSpec(
            num_scalar_prefetch=2,
            grid=(1,),
            in_specs=[pl.BlockSpec((slots, 1, piece, width), from_peer)],
            out_specs=pl.BlockSpec((slots, piece, width), lambda t, own, mask: (0, 0, 0)),
        ),
        out_shape=jax.ShapeDtypeStruct((slots, piece, width), BF16),
        compiler_params=pltpu.CompilerParams(dimension_semantics=("arbitrary",)),
        name="pack_lead",
    )(own, mask, states)


def pack_kernel(hops, own_ref, mask_ref, state_ref, *out_refs):
    first_slot = pl.program_id(0) * PACK_TILE
    peers = state_ref.shape[1]
    for j in range(PACK_TILE):
        keep = mask_ref[jnp.minimum(first_slot + j, mask_ref.shape[0] - 1)].astype(F32)
        for hop, out_ref in zip(hops, out_refs):
            peer = lax.rem(own_ref[0] + hop, peers)
            out_ref[j] = (state_ref[j, peer] * keep).astype(BF16)


def pack(own, mask, states, hops):
    slots, peers, piece, width = states.shape
    return pl.pallas_call(
        functools.partial(pack_kernel, hops),
        grid=(pl.cdiv(slots, PACK_TILE),),
        in_specs=[
            pl.BlockSpec(memory_space=pltpu.SMEM),
            pl.BlockSpec(memory_space=pltpu.SMEM),
            pl.BlockSpec((PACK_TILE, peers, piece, width), lambda t: (t, 0, 0, 0)),
        ],
        out_specs=[pl.BlockSpec((PACK_TILE, piece, width), lambda t: (t, 0, 0))] * len(hops),
        out_shape=[jax.ShapeDtypeStruct((slots, piece, width), BF16)] * len(hops),
        compiler_params=pltpu.CompilerParams(dimension_semantics=("arbitrary",)),
        name="pack",
    )(own, mask, states)


def source_of(table_ref, target):
    code = table_ref[0, target]
    peer = lax.div(code, SLOT_PAD)
    return peer, code - peer * SLOT_PAD


def pick_first_kernel(own_ref, table_ref, packet_ref, *refs):
    in_refs, out_ref, sem = refs[:-2], refs[-2], refs[-1]
    peers = len(in_refs)
    slots, piece, _ = in_refs[0].shape
    own_piece = pl.ds(0, piece)
    for target in range(peers):
        peer, index = source_of(table_ref, target * slots)
        source = lax.rem(own_ref[0] - peer + peers, peers)
        for hop in range(peers):

            @pl.when(source == hop)
            def _():
                pltpu.make_async_copy(
                    in_refs[hop].at[index], out_ref.at[target, own_piece], sem.at[target]
                ).start()

    for target in range(peers):
        out_ref[target, piece:, :] = packet_ref[target]
    for target in range(peers):
        pltpu.make_async_copy(
            in_refs[0].at[0], out_ref.at[target, own_piece], sem.at[target]
        ).wait()


def pick_first(own, table, packets, pieces):
    _, piece, width = pieces[0].shape
    peers = len(pieces)
    scalar = pl.BlockSpec(memory_space=pltpu.SMEM)
    return pl.pallas_call(
        pick_first_kernel,
        in_specs=[scalar, scalar, pl.BlockSpec(memory_space=pltpu.VMEM)]
        + [pl.BlockSpec(memory_space=pl.ANY)] * peers,
        out_specs=pl.BlockSpec(memory_space=pltpu.VMEM),
        out_shape=jax.ShapeDtypeStruct((peers, piece + packets.shape[1], width), BF16),
        scratch_shapes=[pltpu.SemaphoreType.DMA((peers,))],
        name="pick_first",
    )(own, table, packets, *pieces)


def gather_pieces(own_ref, refs, scr):
    peers = len(refs)
    for hop in range(peers):
        scr[lax.rem(own_ref[0] - hop + peers, peers)] = refs[hop][...]


def reorder_kernel(own_ref, table_ref, *refs):
    scr = refs[-1]
    peers, slots = scr.shape[:2]
    gather_pieces(own_ref, refs[:peers], scr)
    for hop in range(peers):
        base = lax.rem(own_ref[0] + hop, peers) * slots
        out_ref = refs[peers + hop]

        def move(slot, unused):
            peer, index = source_of(table_ref, base + slot)
            out_ref[slot - 1] = scr[peer, index]
            return unused

        lax.fori_loop(1, slots, move, 0)


def reorder_rest_kernel(own_ref, table_ref, *refs):
    out_ref, scr = refs[-2:]
    peers, slots = scr.shape[:2]
    gather_pieces(own_ref, refs[:peers], scr)
    for target in range(peers):

        def move(slot, unused):
            peer, index = source_of(table_ref, target * slots + slot)
            out_ref[target, slot - 1] = scr[peer, index]
            return unused

        lax.fori_loop(1, slots, move, 0)


def reorder(own, table, pieces, part):
    slots, piece, width = pieces[0].shape
    half = piece // 2
    peers = len(pieces)
    scalar = pl.BlockSpec(memory_space=pltpu.SMEM)
    if part == 0:
        one = (slots - 1, half, width)
        out_specs = [pl.BlockSpec(one, lambda t: (0, 0, 0))] * peers
        out_shape = [jax.ShapeDtypeStruct(one, BF16)] * peers
    else:
        all_rest = (peers, slots - 1, half, width)
        out_specs = pl.BlockSpec(all_rest, lambda t: (0, 0, 0, 0))
        out_shape = jax.ShapeDtypeStruct(all_rest, BF16)
    return pl.pallas_call(
        reorder_kernel if part == 0 else reorder_rest_kernel,
        grid=(1,),
        in_specs=[scalar, scalar]
        + [pl.BlockSpec((slots, half, width), lambda t: (0, part, 0))] * peers,
        out_specs=out_specs,
        out_shape=out_shape,
        scratch_shapes=[pltpu.VMEM((peers, slots, half, width), BF16)],
        name="reorder" if part == 0 else "reorder_rest",
    )(own, table, *pieces)


def unpack_kernel(own_ref, final_ref, *refs):
    piece_refs, out_ref = refs[:-1], refs[-1]
    step = pl.program_id(0)
    half = out_ref.shape[2]
    out_ref[0, 0] = final_ref[:half, :]
    for hop in range(len(piece_refs)):

        @pl.when(step == hop)
        def _():
            out_ref[1:, 0] = piece_refs[hop][...].astype(F32)


def unpack(own, final, pieces):
    others, half, width = pieces[0].shape
    peers = len(pieces)
    slots, piece = others + 1, 2 * half

    def from_peer(hop, own):
        return lax.rem(own[0] - hop + peers, peers)

    return pl.pallas_call(
        unpack_kernel,
        grid_spec=pltpu.PrefetchScalarGridSpec(
            num_scalar_prefetch=1,
            grid=(peers,),
            in_specs=[pl.BlockSpec((piece, width), lambda h, own: (from_peer(h, own), 0))]
            + [pl.BlockSpec((others, half, width), lambda h, own: (0, 0, 0))] * peers,
            out_specs=pl.BlockSpec(
                (slots, 1, half, width), lambda h, own: (0, from_peer(h, own), 0, 0)
            ),
        ),
        out_shape=jax.ShapeDtypeStruct((slots, peers, piece, width), F32),
        compiler_params=pltpu.CompilerParams(dimension_semantics=("arbitrary",)),
        name="unpack",
    )(own, final, *pieces)


def unpack_rest_kernel(final_ref, pieces_ref, states_ref, out_ref):
    peers, half = pieces_ref.shape[0], pieces_ref.shape[2]
    for p in range(peers):
        out_ref[0, p] = final_ref[(2 * p + 1) * half : (2 * p + 2) * half, :]
        out_ref[1:, p] = pieces_ref[p].astype(F32)


def unpack_rest(final, pieces, states):
    slots, peers, piece, width = states.shape
    half = piece // 2
    return pl.pallas_call(
        unpack_rest_kernel,
        grid=(peers // PEER_TILE,),
        in_specs=[
            pl.BlockSpec((PEER_TILE * piece, width), lambda p: (p, 0)),
            pl.BlockSpec((PEER_TILE, slots - 1, half, width), lambda p: (p, 0, 0, 0)),
            pl.BlockSpec(memory_space=pl.ANY),
        ],
        out_specs=pl.BlockSpec((slots, PEER_TILE, half, width), lambda p: (0, p, 1, 0)),
        out_shape=jax.ShapeDtypeStruct(states.shape, F32),
        input_output_aliases={2: 0},
        compiler_params=pltpu.CompilerParams(dimension_semantics=("arbitrary",)),
        name="unpack_rest",
    )(final, pieces, states)


def combine_kernel(place_ref, decay_ref, *refs):
    count = decay_ref.shape[0]
    end_scr, enter_scr = refs[-2:]
    final_ref = refs[-3]
    entering_refs = refs[-3 - count : -3]
    end_refs, first_ref = refs[:count], refs[count]
    chain = place_ref[0]
    for hop in range(count):
        end_scr[lax.rem(chain - hop + count, count)] = end_refs[hop][...]
    peers, piece, width = first_ref.shape
    state = first_ref[...].astype(F32).reshape(peers * piece, width).T
    for k in range(count):
        enter_scr[k] = state.astype(BF16)
        state = state * decay_ref[k : k + 1, :] + end_scr[k].astype(F32)
    for hop in range(count):
        entering_refs[hop][...] = enter_scr[lax.rem(chain + hop, count)]
    final_ref[...] = state.T


def combine(place, decay, ends, first):
    count = len(ends)
    whole = pl.BlockSpec(memory_space=pltpu.VMEM)
    rows, columns = ends[0].shape
    peers = first.shape[0]
    outs = pl.pallas_call(
        combine_kernel,
        grid=(1,),
        in_specs=[
            pl.BlockSpec(memory_space=pltpu.SMEM),
            pl.BlockSpec(decay.shape, lambda t: (0, 0)),
        ]
        + [pl.BlockSpec((rows, columns), lambda t: (0, 0))] * count
        + [pl.BlockSpec((peers, columns // peers, rows), lambda t: (0, 0, 0))],
        out_specs=[pl.BlockSpec((rows, columns), lambda t: (0, 0))] * count
        + [pl.BlockSpec((columns, rows), lambda t: (0, 0))],
        out_shape=[jax.ShapeDtypeStruct((rows, columns), BF16)] * count
        + [jax.ShapeDtypeStruct((columns, rows), F32)],
        scratch_shapes=[
            pltpu.VMEM((count, rows, columns), BF16),
            pltpu.VMEM((count, rows, columns), BF16),
        ],
        name="combine",
    )(place, decay, *ends, first)
    return outs[:count], outs[count]


def share_kernel(
    slot_count,
    place_ref,
    every_ref,
    end_ref,
    kept_ref,
    kept_next_ref,
    state_end_ref,
    state_kept_ref,
    state_next_ref,
    raw_ref,
    bias_ref,
    rate_ref,
    out_ref,
    step_ref,
    table_ref,
):
    taps = out_ref.shape[0]
    inner = end_ref.shape[1]
    outer = state_end_ref.shape[1]
    channels = inner + outer
    peers, packet, _ = every_ref.shape
    slots = float(slot_count)
    chunks = (packet - 2) // taps
    width = chunks * LANES
    everything = [every_ref[p].astype(F32) for p in range(peers)]
    firsts = everything[0]
    for part in everything[1:]:
        firsts = firsts + part
    at = chunks * taps
    target = jnp.concatenate([part[at : at + 1] for part in everything], axis=0) * slots
    target = target + jnp.concatenate([part[at + 1 : at + 2] for part in everything], axis=0)
    columns = table_ref.shape[1]
    lane = lax.broadcasted_iota(jnp.int32, (peers, columns), 1).astype(F32)
    code = lax.broadcasted_iota(jnp.int32, (peers, columns), 0).astype(F32) * SLOT_PAD
    found = jnp.zeros((peers, columns), F32)
    for slot in range(slot_count):
        found = found + jnp.where(target[:, slot : slot + 1] == lane, code + slot, 0.0)
    found = jnp.sum(found, axis=0, keepdims=True)
    table_ref[...] = jnp.broadcast_to(found, table_ref.shape).astype(jnp.int32)
    low_block, high_block, start, length = (
        place_ref[0],
        place_ref[1],
        place_ref[2],
        place_ref[3],
    )
    out_ref[:, :inner] = end_ref[16 - taps :, :]
    out_ref[:, inner:channels] = state_end_ref[16 - taps :, :]
    here = lax.broadcasted_iota(jnp.int32, (16, 1), 0)
    wanted = length - taps - start

    def kept_rows(low_ref, high_ref):
        low = low_ref[...].astype(F32)
        high = high_ref[...].astype(F32)
        found = []
        for i in range(taps):
            in_low = (low_block * 16 + here) == (wanted + i)
            in_high = ((high_block * 16 + here) == (wanted + i)) & (high_block > low_block)
            picked = jnp.where(in_low, low, 0.0) + jnp.where(in_high, high, 0.0)
            found.append(jnp.sum(picked, axis=0, keepdims=True))
        return jnp.concatenate(found, axis=0).astype(BF16)

    out_ref[:, channels : channels + inner] = kept_rows(kept_ref, kept_next_ref)
    out_ref[:, channels + inner : 2 * channels] = kept_rows(state_kept_ref, state_next_ref)
    for chunk in range(chunks):
        at = 2 * channels + chunk * LANES
        lines = firsts[chunk * taps : (chunk + 1) * taps]
        out_ref[:, at : at + LANES] = lines.astype(BF16)
    count = step_ref.shape[0]
    heads = raw_ref.shape[1]
    positions = start + lax.broadcasted_iota(jnp.int32, (count, heads), 0)
    raw = raw_ref[...].astype(F32) + bias_ref[...]
    step = jnp.maximum(raw, 0.0) + jnp.log1p(jnp.exp(-jnp.abs(raw)))
    step = jnp.where(positions < length, step, 0.0)
    step = jnp.concatenate([step, jnp.zeros((count, LANES - heads), F32)], axis=1)
    step_ref[...] = step
    total = jnp.sum(step * rate_ref[...], axis=0, keepdims=True)
    high = total.astype(BF16).astype(F32)
    middle = (total - high).astype(BF16).astype(F32)
    rest = total - high - middle
    parts = jnp.concatenate([high, middle, rest], axis=0)
    out_ref[:, 2 * channels + width :] = parts.astype(BF16)


def share(place, slots, every, rows, state_rows, step_raw, step_bias, rate):
    peers, packet, _ = every.shape
    taps = KERNEL - 1
    width = (packet - 2) // taps * LANES
    length, inner = rows.shape
    outer = state_rows.shape[1]
    heads = step_raw.shape[1]
    last = length // 16 - 1
    total = 2 * (inner + outer) + width + LANES
    lanes = pl.cdiv(peers * slots, LANES) * LANES
    return pl.pallas_call(
        functools.partial(share_kernel, slots),
        grid_spec=pltpu.PrefetchScalarGridSpec(
            num_scalar_prefetch=1,
            grid=(1,),
            in_specs=[
                pl.BlockSpec(every.shape, lambda t, c: (0, 0, 0)),
                pl.BlockSpec((16, inner), lambda t, c: (last, 0)),
                pl.BlockSpec((16, inner), lambda t, c: (c[0], 0)),
                pl.BlockSpec((16, inner), lambda t, c: (c[1], 0)),
                pl.BlockSpec((16, outer), lambda t, c: (last, 0)),
                pl.BlockSpec((16, outer), lambda t, c: (c[0], 0)),
                pl.BlockSpec((16, outer), lambda t, c: (c[1], 0)),
                pl.BlockSpec((length, heads), lambda t, c: (0, 0)),
                pl.BlockSpec((1, heads), lambda t, c: (0, 0)),
                pl.BlockSpec((1, LANES), lambda t, c: (0, 0)),
            ],
            out_specs=[
                pl.BlockSpec((taps, total), lambda t, c: (0, 0)),
                pl.BlockSpec((length, LANES), lambda t, c: (0, 0)),
                pl.BlockSpec((8, lanes), lambda t, c: (0, 0)),
            ],
        ),
        out_shape=[
            jax.ShapeDtypeStruct((taps, total), BF16),
            jax.ShapeDtypeStruct((length, LANES), F32),
            jax.ShapeDtypeStruct((8, lanes), jnp.int32),
        ],
        name="share",
    )(
        place,
        every,
        rows,
        rows,
        rows,
        state_rows,
        state_rows,
        state_rows,
        step_raw,
        step_bias,
        rate,
    )


def tail_kernel(
    chain_ref, shared_ref, tail_ref, inner_ref, outer_ref, decay_ref
):
    chain = chain_ref[0]
    count, taps = shared_ref.shape[:2]
    inner_local, outer_local = inner_ref.shape[1], outer_ref.shape[1]
    channels = tail_ref.shape[1]
    inner = count * inner_local
    at = 2 * channels
    window = jnp.concatenate(
        [shared_ref[s, :, at : at + inner_local] for s in range(count)]
        + [
            shared_ref[s, :, at + inner_local : at + inner_local + outer_local]
            for s in range(count)
        ],
        axis=1,
    ).astype(F32)
    earlier = shared_ref[jnp.maximum(chain - 1, 0), :, :channels].astype(F32)
    tail = jnp.where(chain == 0, window, earlier)
    tail_ref[...] = jnp.concatenate([jnp.zeros((8 - taps, channels), F32), tail], axis=0)
    kept = shared_ref[0, :, channels:at].astype(F32)
    for s in range(1, count):
        kept = kept + shared_ref[s, :, channels:at].astype(F32)
    own_inner = jnp.zeros((taps, inner_local), F32)
    own_outer = jnp.zeros((taps, outer_local), F32)
    for s in range(count):
        mine = chain == s
        inner_at, outer_at = s * inner_local, inner + s * outer_local
        own_inner = jnp.where(mine, kept[:, inner_at : inner_at + inner_local], own_inner)
        own_outer = jnp.where(mine, kept[:, outer_at : outer_at + outer_local], own_outer)
    inner_ref[...] = own_inner.astype(BF16)
    outer_ref[...] = own_outer.astype(BF16)
    logs = []
    for s in range(count):
        parts = shared_ref[s, :, shared_ref.shape[2] - LANES :].astype(F32)
        logs.append(jnp.sum(parts, axis=0, keepdims=True))
    logs = jnp.concatenate(logs + [jnp.zeros((8 - count, LANES), F32)] * (count < 8), axis=0)
    columns = decay_ref.shape[1]
    head = lax.broadcasted_iota(jnp.int32, (LANES, columns), 0)
    lane = lax.broadcasted_iota(jnp.int32, (LANES, columns), 1)
    local_heads = columns // HEAD_DIM
    pick = (head == chain * local_heads + lane // HEAD_DIM).astype(F32)
    spread = dot(logs, pick, precision=lax.Precision.HIGHEST)
    decay_ref[...] = jnp.exp2(spread[:count])


def tails(chain, shared, channels, inner_local, outer_local, columns):
    count, taps = shared.shape[:2]
    whole = pl.BlockSpec(memory_space=pltpu.VMEM)
    return pl.pallas_call(
        tail_kernel,
        in_specs=[pl.BlockSpec(memory_space=pltpu.SMEM), whole],
        out_shape=[
            jax.ShapeDtypeStruct((8, channels), F32),
            jax.ShapeDtypeStruct((taps, inner_local), BF16),
            jax.ShapeDtypeStruct((taps, outer_local), BF16),
            jax.ShapeDtypeStruct((count, columns), F32),
        ],
        name="tails",
    )(chain, shared)


def exchange(value, axis):
    return lax.all_to_all(value, axis, split_axis=0, concat_axis=0, tiled=True)


def hop_order(count):
    return sorted(range(1, count), key=lambda hop: abs(2 * hop - count))


def send(value, axis, hop):
    count = lax.axis_size(axis)
    pairs = [(source, (source + hop) % count) for source in range(count)]
    return lax.ppermute(value, axis, pairs)


def rotate(values, axis):
    got = [values[hop] for hop in range(lax.axis_size(axis))]
    for hop in hop_order(len(got)):
        got[hop] = send(got[hop], axis, hop)
    return got


def device_body(
    pool_states,
    inner_window,
    state_window,
    move_plan,
    active_mask,
    inputs_inner,
    inputs_state,
    gate_rows,
    step_raw,
    lengths,
    conv_weight,
    conv_bias,
    step_bias,
    decay_log,
    skip_weight,
    norm_weight,
):
    peers = lax.axis_size("req")
    own_peer = lax.axis_index("req").astype(jnp.int32)
    chain_size = lax.axis_size("seq")
    chain_index = lax.axis_index("seq").astype(jnp.int32)
    slots, local_heads = pool_states.shape[:2]
    columns = local_heads * HEAD_DIM
    piece = columns // peers
    taps = KERNEL - 1
    inner_local = inner_window.shape[2]
    outer_local = state_window.shape[2]

    own = own_peer[None]
    pool_pieces = pool_states.reshape(slots, peers, piece, STATE_DIM)
    lead, *others = hop_order(peers)
    spread = [None] * peers
    lead_pieces = pack_lead(own, active_mask, pool_pieces, lead)
    spread[lead] = send(lead_pieces, "req", lead)
    plan = move_plan.T
    inner_taps = inner_window.transpose(1, 0, 2)
    outer_taps = state_window.transpose(1, 0, 2)
    packed = mark(plan, active_mask, inner_taps, outer_taps, peers)
    packets = window_packets(plan, active_mask, inner_taps, outer_taps, peers)
    every = exchange(packed, "req")
    others = [0] + others
    for hop, pieces in zip(others, pack(own, active_mask, pool_pieces, others)):
        spread[hop] = pieces if hop == 0 else send(pieces, "req", hop)

    rows = inputs_inner[0]
    state_rows = inputs_state[0]
    local_length, inner_dim = rows.shape
    channels = inner_dim + state_rows.shape[1]
    start = chain_index * local_length
    length = lengths[0]
    last_tile = local_length // 16 - 1
    low_block = jnp.clip((length - taps - start) // 16, 0, last_tile)
    high_block = jnp.minimum(low_block + 1, last_tile)
    heads = decay_log.shape[0]
    rate = jnp.pad(-LOG2E * jnp.exp(decay_log), (0, LANES - heads))[None]
    payload, step, table = share(
        jnp.stack([low_block, high_block, start, length]),
        slots,
        every,
        rows,
        state_rows,
        step_raw[0],
        step_bias[None],
        rate,
    )
    shared = lax.all_gather(payload, "seq", axis=0)
    chain = chain_index[None]
    tail, kept_inner, kept_outer, own_decay = tails(
        chain, shared, channels, inner_local, outer_local, columns
    )

    part, local_end, read_rows, decay = block_parts(
        chain,
        tail,
        rows,
        state_rows,
        step,
        rate,
        conv_weight,
        conv_bias[None],
        jnp.repeat(skip_weight, HEAD_DIM)[None],
        chain_size,
    )
    own_ends = rotate(local_end, "seq")

    first = exchange(pick_first(own, table, packets, spread), "req")
    moved_a = rotate(reorder(own, table, spread, 0), "req")
    moved_b = exchange(reorder(own, table, spread, 1), "req")
    entering, final = combine(chain, own_decay, own_ends, first)
    new_inner, new_outer = settle(first, kept_inner, kept_outer, slots)
    incoming = rotate(entering, "seq")
    mixer_out = finish(
        jnp.stack([start, length, chain_index]),
        part,
        gate_rows[0],
        read_rows,
        decay,
        norm_weight[None],
        incoming,
    )
    states = unpack(own, final, moved_a)
    new_states = unpack_rest(final, moved_b, states).reshape(pool_states.shape)

    return (
        new_states,
        new_inner.transpose(1, 0, 2),
        new_outer.transpose(1, 0, 2),
        mixer_out[None],
    )


def solution(mesh):
    return jax.shard_map(
        device_body,
        mesh=mesh,
        in_specs=(
            P("req", "seq", None, None),
            P("req", None, "seq"),
            P("req", None, "seq"),
            P("req", None),
            P("req"),
            P("req", "seq", None),
            P("req", "seq", None),
            P("req", "seq", None),
            P("req", "seq", None),
            P("req"),
            P(),
            P(),
            P(),
            P(),
            P(),
            P(),
        ),
        out_specs=(
            P("req", "seq", None, None),
            P("req", None, "seq"),
            P("req", None, "seq"),
            P("req", "seq", None),
        ),
        check_vma=False,
    )
```

```python
import functools
import math

import jax
import jax.numpy as jnp
from jax import lax
from jax.experimental import pallas as pl
from jax.experimental.pallas import tpu as pltpu
from jax.sharding import PartitionSpec as P


HEAD_DIM = 64
STATE_DIM = 128
KERNEL = 4
BLOCK_LEN = 256
GROUP = 8
HALF = BLOCK_LEN // 2
GROUP_DIM = GROUP * HEAD_DIM
PAIR_DIM = 2 * HEAD_DIM
LANES = 128
TILE = 128
SLOT_PAD = 16
PEER_TILE = 2
PACK_TILE = 2
EPSILON = 1e-05
LOG2E = math.log2(math.e)
F32 = jnp.float32
BF16 = jnp.bfloat16


def dot(a, b, dims=((1,), (0,)), precision=None):
    return lax.dot_general(a, b, (dims, ((), ())), precision=precision, preferred_element_type=F32)


def silu(v):
    half = 0.5 * v
    return half + half * jnp.tanh(half)


def conv_silu(tail, rows, weight, bias_row):
    extended = jnp.concatenate([tail, rows.astype(F32)], axis=0)
    count = rows.shape[0]
    start = tail.shape[0] - KERNEL + 1
    running = bias_row + weight[0:1] * extended[start : start + count]
    for k in range(1, KERNEL):
        running = running + weight[k : k + 1] * extended[start + k : start + k + count]
    return silu(running)


def pair_of(columns, i, low):
    return jnp.where(low, columns[:, 2 * i : 2 * i + 1], columns[:, 2 * i + 1 : 2 * i + 2])


def block_kernel(
    chain_ref,
    tail_ref,
    prev_ref,
    rows_ref,
    state_tail_ref,
    state_prev_ref,
    state_rows_ref,
    step_ref,
    rate_ref,
    weight_ref,
    bias_ref,
    state_weight_ref,
    state_bias_ref,
    skip_ref,
    part_ref,
    end_ref,
    read_ref,
    decay_ref,
    scores_scr,
    cum_scr,
    cum_t_scr,
    to_end_scr,
    decay_scr,
    write_t_scr,
    offset_scr,
    carry_scr,
):
    block = pl.program_id(0)
    group = pl.program_id(1)
    first = block == 0

    @pl.when(group == 0)
    def _():
        state_tail = jnp.where(first, state_tail_ref[...], state_prev_ref[8:16, :].astype(F32))
        mixed = conv_silu(state_tail, state_rows_ref[...], state_weight_ref[...], state_bias_ref[...])
        write = mixed[:, :STATE_DIM]
        read = mixed[:, STATE_DIM:].astype(BF16)
        read_ref[...] = read
        write_b = write.astype(BF16)
        scores_scr[...] = dot(read, write_b, ((1,), (1,)))
        write_t_scr[...] = write_b.astype(F32).T.astype(BF16)
        row = lax.broadcasted_iota(jnp.int32, (BLOCK_LEN, BLOCK_LEN), 0)
        col = lax.broadcasted_iota(jnp.int32, (BLOCK_LEN, BLOCK_LEN), 1)
        triangle = (row >= col).astype(F32)
        step = step_ref[...]
        cum = dot(triangle, step * rate_ref[...], precision=lax.Precision.HIGHEST)
        cum_scr[...] = cum
        cum_t_scr[...] = cum.T
        last = cum[BLOCK_LEN - 1 :, :]
        to_end_scr[...] = jnp.exp2(last - cum) * step
        decay_scr[...] = jnp.exp2(cum)
        offset = jnp.where(first, 0.0, offset_scr[0:1, :])
        decay_ref[...] = jnp.exp2(offset + cum)
        offset_scr[0:1, :] = offset + last

    shift = lax.rem(LANES - group * GROUP, LANES)
    cum = pltpu.roll(cum_scr[...], shift, 1)
    step = pltpu.roll(step_ref[...], shift, 1)
    to_end = pltpu.roll(to_end_scr[...], shift, 1)
    decay = pltpu.roll(decay_scr[...], shift, 1)
    cum_t = cum_t_scr[pl.ds(pl.multiple_of(group * GROUP, GROUP), GROUP), :]
    read = read_ref[...]
    write_t = write_t_scr[...]
    carry = jnp.where(first, 0.0, carry_scr[group])
    carry_b = carry.astype(BF16)
    low = lax.broadcasted_iota(jnp.int32, (1, PAIR_DIM), 1) < HEAD_DIM
    causal = lax.broadcasted_iota(jnp.int32, (HALF, HALF), 0) >= lax.broadcasted_iota(
        jnp.int32, (HALF, HALF), 1
    )
    scores_top = scores_scr[0:HALF, 0:HALF]
    scores_left = scores_scr[HALF:, 0:HALF]
    scores_right = scores_scr[HALF:, HALF:]

    def head_weights(i):
        later = cum[:, i : i + 1]
        earlier = cum_t[i : i + 1, :]
        gap_top = jnp.where(causal, later[:HALF] - earlier[:, :HALF], -1e30)
        gap_left = later[HALF:] - earlier[:, :HALF]
        gap_right = jnp.where(causal, later[HALF:] - earlier[:, HALF:], -1e30)
        top = (scores_top * jnp.exp2(gap_top)).astype(BF16)
        left = (scores_left * jnp.exp2(gap_left)).astype(BF16)
        right = (scores_right * jnp.exp2(gap_right)).astype(BF16)
        return top, jnp.concatenate([left, right], axis=1)

    for i in range(GROUP // 2):
        span = slice(i * PAIR_DIM, (i + 1) * PAIR_DIM)
        tail = jnp.where(first, tail_ref[:, span], prev_ref[8:16, span].astype(F32))
        mixed = conv_silu(tail, rows_ref[:, span], weight_ref[:, span], bias_ref[:, span])
        value = mixed.astype(BF16).astype(F32)
        stepped = (pair_of(step, i, low) * value).astype(BF16)
        scaled = (pair_of(to_end, i, low) * value).astype(BF16)
        stepped_low = jnp.where(low, stepped, jnp.zeros_like(stepped))
        stepped_high = jnp.where(low, jnp.zeros_like(stepped), stepped)
        top_0, bottom_0 = head_weights(2 * i)
        top_1, bottom_1 = head_weights(2 * i + 1)
        intra_top = dot(top_0, stepped_low[:HALF]) + dot(top_1, stepped_high[:HALF])
        intra_bottom = dot(bottom_0, stepped_low) + dot(bottom_1, stepped_high)
        inter = dot(read, carry_b[:, span]) * pair_of(decay, i, low)
        direct = inter + skip_ref[:, span] * value
        part_ref[0:HALF, span] = intra_top + direct[:HALF]
        part_ref[HALF:, span] = intra_bottom + direct[HALF:]
        kept = pair_of(decay[BLOCK_LEN - 1 :, :], i, low) * carry[:, span]
        ending = kept + dot(write_t, scaled)
        carry_scr[group, :, span] = ending
        end_ref[0, :, span] = ending.astype(BF16)


def block_parts(chain, tail, rows, state_rows, step, rate, weight, bias_row, skip_row, ends):
    length = rows.shape[0]
    channels = rows.shape[1]
    blocks = length // BLOCK_LEN
    groups = channels // GROUP_DIM
    end_groups = groups // ends
    state_dim = state_rows.shape[1]
    state_at = channels // state_dim
    per_block = BLOCK_LEN // 16

    def before(b):
        return jnp.maximum(b * per_block - 1, 0)

    def end_at(b, g, chain):
        return lax.rem(g // end_groups - chain[0] + ends, ends), 0, lax.rem(g, end_groups)

    return pl.pallas_call(
        block_kernel,
        grid_spec=pltpu.PrefetchScalarGridSpec(
        num_scalar_prefetch=1,
        grid=(blocks, groups),
        in_specs=[
            pl.BlockSpec((8, GROUP_DIM), lambda b, g, c: (0, g)),
            pl.BlockSpec((16, GROUP_DIM), lambda b, g, c: (before(b), g)),
            pl.BlockSpec((BLOCK_LEN, GROUP_DIM), lambda b, g, c: (b, g)),
            pl.BlockSpec((8, state_dim), lambda b, g, c: (0, state_at)),
            pl.BlockSpec((16, state_dim), lambda b, g, c: (before(b), 0)),
            pl.BlockSpec((BLOCK_LEN, state_dim), lambda b, g, c: (b, 0)),
            pl.BlockSpec((BLOCK_LEN, LANES), lambda b, g, c: (b, 0)),
            pl.BlockSpec((1, LANES), lambda b, g, c: (0, 0)),
            pl.BlockSpec((KERNEL, GROUP_DIM), lambda b, g, c: (0, g)),
            pl.BlockSpec((1, GROUP_DIM), lambda b, g, c: (0, g)),
            pl.BlockSpec((KERNEL, state_dim), lambda b, g, c: (0, state_at)),
            pl.BlockSpec((1, state_dim), lambda b, g, c: (0, state_at)),
            pl.BlockSpec((1, GROUP_DIM), lambda b, g, c: (0, g)),
        ],
        out_specs=[
            pl.BlockSpec((BLOCK_LEN, GROUP_DIM), lambda b, g, c: (b, g)),
            pl.BlockSpec((1, STATE_DIM, GROUP_DIM), end_at),
            pl.BlockSpec((BLOCK_LEN, STATE_DIM), lambda b, g, c: (b, 0)),
            pl.BlockSpec((BLOCK_LEN, LANES), lambda b, g, c: (b, 0)),
        ],
        scratch_shapes=[
            pltpu.VMEM((BLOCK_LEN, BLOCK_LEN), F32),
            pltpu.VMEM((BLOCK_LEN, LANES), F32),
            pltpu.VMEM((LANES, BLOCK_LEN), F32),
            pltpu.VMEM((BLOCK_LEN, LANES), F32),
            pltpu.VMEM((BLOCK_LEN, LANES), F32),
            pltpu.VMEM((STATE_DIM, BLOCK_LEN), BF16),
            pltpu.VMEM((8, LANES), F32),
            pltpu.VMEM((groups, STATE_DIM, GROUP_DIM), F32),
        ],
        ),
        out_shape=[
            jax.ShapeDtypeStruct((length, channels), F32),
            jax.ShapeDtypeStruct((ends, STATE_DIM, channels // ends), BF16),
            jax.ShapeDtypeStruct((length, STATE_DIM), BF16),
            jax.ShapeDtypeStruct((length, LANES), F32),
        ],
        compiler_params=pltpu.CompilerParams(dimension_semantics=("arbitrary", "arbitrary")),
        cost_estimate=pl.CostEstimate(
            flops=6_000_000_000, bytes_accessed=20_000_000, transcendentals=10_000_000
        ),
        name="block_parts",
    )(
        chain,
        tail,
        rows,
        rows,
        tail,
        state_rows,
        state_rows,
        step,
        rate,
        weight,
        bias_row,
        weight,
        bias_row,
        skip_row,
    )


def finish_kernel(
    place_ref, part_ref, gate_ref, read_ref, decay_ref, norm_ref, *refs
):
    state_refs, out_ref, gated_scr, state_scr = refs[:-3], refs[-3], refs[-2], refs[-1]
    tile = pl.program_id(0)
    chunks, _, width = state_scr.shape

    @pl.when(tile == 0)
    def _():
        for hop in range(chunks):
            state_scr[lax.rem(place_ref[2] - hop + chunks, chunks)] = state_refs[hop][...]

    positions = (
        place_ref[0] + tile * TILE + lax.broadcasted_iota(jnp.int32, (TILE, PAIR_DIM), 0)
    )
    valid = (positions < place_ref[1]).astype(F32)
    low = lax.broadcasted_iota(jnp.int32, (1, PAIR_DIM), 1) < HEAD_DIM
    read = read_ref[...]
    decay = decay_ref[...]
    total = jnp.zeros((TILE, PAIR_DIM), F32)
    for chunk in range(chunks):
        for i in range(width // PAIR_DIM):
            pair = chunk * (width // PAIR_DIM) + i
            span = slice(pair * PAIR_DIM, (pair + 1) * PAIR_DIM)
            inter = dot(read, state_scr[chunk, :, i * PAIR_DIM : (i + 1) * PAIR_DIM])
            y = part_ref[:, span] + inter * pair_of(decay, pair, low)
            y = (y * valid).astype(BF16).astype(F32)
            gated = y * silu(gate_ref[:, span].astype(F32))
            gated_scr[:, span] = gated
            total = total + gated * gated
    channels = chunks * width
    mean = jnp.sum(total, axis=1, keepdims=True) * (1.0 / channels)
    scale = lax.rsqrt(mean + EPSILON)
    for pair in range(channels // PAIR_DIM):
        span = slice(pair * PAIR_DIM, (pair + 1) * PAIR_DIM)
        out_ref[:, span] = (gated_scr[:, span] * scale * norm_ref[:, span]).astype(BF16)


def finish(place, part, gate, read, decay, norm_row, states):
    length, channels = part.shape
    return pl.pallas_call(
        finish_kernel,
        grid=(length // TILE,),
        in_specs=[
            pl.BlockSpec(memory_space=pltpu.SMEM),
            pl.BlockSpec((TILE, channels), lambda t: (t, 0)),
            pl.BlockSpec((TILE, channels), lambda t: (t, 0)),
            pl.BlockSpec((TILE, STATE_DIM), lambda t: (t, 0)),
            pl.BlockSpec((TILE, LANES), lambda t: (t, 0)),
            pl.BlockSpec((1, channels), lambda t: (0, 0)),
        ]
        + [pl.BlockSpec(state.shape, lambda t: (0, 0)) for state in states],
        out_specs=pl.BlockSpec((TILE, channels), lambda t: (t, 0)),
        out_shape=jax.ShapeDtypeStruct((length, channels), BF16),
        scratch_shapes=[
            pltpu.VMEM((TILE, channels), F32),
            pltpu.VMEM((len(states),) + states[0].shape, BF16),
        ],
        compiler_params=pltpu.CompilerParams(dimension_semantics=("arbitrary",)),
        cost_estimate=pl.CostEstimate(
            flops=3_000_000_000, bytes_accessed=16_000_000, transcendentals=4_000_000
        ),
        name="finish",
    )(place, part, gate, read, decay, norm_row, *states)


def most_per_pair(slots, peers):
    return (2 * slots + peers - 1) // peers


def padded_windows(inner_ref, outer_ref, total):
    taps, slots = inner_ref.shape[:2]
    width = inner_ref.shape[2] + outer_ref.shape[2]
    windows = []
    for tap in range(taps):
        both = [inner_ref[tap].astype(F32), outer_ref[tap].astype(F32)]
        both.append(jnp.zeros((slots, total - width), F32))
        windows.append(jnp.concatenate(both, axis=1))
    return windows


def mark_kernel(plan_ref, mask_ref, inner_ref, outer_ref, out_ref):
    peers, packet, _ = out_ref.shape
    taps, slots = inner_ref.shape[:2]
    chunks = (packet - 2) // taps
    fill = jnp.zeros((SLOT_PAD - slots, chunks * LANES), F32)
    row = lax.broadcasted_iota(jnp.int32, (peers, LANES), 0)
    lane = lax.broadcasted_iota(jnp.int32, (peers, LANES), 1)
    pick = jnp.zeros((peers, LANES), F32)
    peer_marks = jnp.zeros((1, LANES), F32)
    slot_marks = jnp.zeros((1, LANES), F32)
    for slot in range(slots):
        peer, target = plan_ref[0, slot], plan_ref[1, slot]
        here = (row == peer) & (lane == slot) & (target == 0)
        pick = jnp.where(here, mask_ref[slot].astype(F32), pick)
        peer_marks = jnp.where(lane[:1] == slot, peer.astype(F32), peer_marks)
        slot_marks = jnp.where(lane[:1] == slot, target.astype(F32), slot_marks)
    pick = pick[:, :SLOT_PAD].astype(BF16)
    picked = []
    for window in padded_windows(inner_ref, outer_ref, chunks * LANES):
        window = jnp.concatenate([window, fill], axis=0).astype(BF16)
        picked.append(dot(pick, window))
    spare = packet - chunks * taps - 2
    for peer in range(peers):
        lines = []
        for chunk in range(chunks):
            span = slice(chunk * LANES, (chunk + 1) * LANES)
            lines += [picked[tap][peer : peer + 1, span] for tap in range(taps)]
        lines += [peer_marks, slot_marks]
        if spare > 0:
            lines.append(jnp.zeros((spare, LANES), F32))
        out_ref[peer] = jnp.concatenate(lines, axis=0).astype(BF16)


def mark(plan, mask, inner, outer, peers):
    taps, _ = inner.shape[:2]
    width = inner.shape[2] + outer.shape[2]
    whole = pl.BlockSpec(memory_space=pltpu.VMEM)
    scalar = pl.BlockSpec(memory_space=pltpu.SMEM)
    packet = pl.cdiv(taps * pl.cdiv(width, LANES) + 2, 16) * 16
    return pl.pallas_call(
        mark_kernel,
        in_specs=[scalar, scalar, whole, whole],
        out_shape=jax.ShapeDtypeStruct((peers, packet, LANES), BF16),
        name="mark",
    )(plan, mask, inner, outer)


def window_kernel(plan_ref, mask_ref, inner_ref, outer_ref, out_ref, scr):
    peers = out_ref.shape[0]
    taps, slots = inner_ref.shape[:2]
    total = scr.shape[1]
    chunks = total // LANES
    padded = out_ref.shape[1] // chunks
    capacity = most_per_pair(slots, peers)
    at = total - LANES
    scr[...] = jnp.zeros((peers * padded, total), F32)
    windows = padded_windows(inner_ref, outer_ref, total)
    last = lax.broadcasted_iota(jnp.int32, (1, total), 1) == total - 1
    for line in range(peers * padded // 8):
        lane = lax.broadcasted_iota(jnp.int32, (8, LANES), 1)
        scr[line * 8 : line * 8 + 8, at:] = jnp.where(lane == LANES - 1, -1.0, 0.0)
    for slot in range(slots):
        peer, target = plan_ref[0, slot], plan_ref[1, slot]
        rank = jnp.int32(0)
        for earlier in range(slot):
            rank = rank + (plan_ref[0, earlier] == peer).astype(jnp.int32)
        keep = mask_ref[slot].astype(F32)
        for tap in range(taps):
            tag = (target + tap * SLOT_PAD).astype(F32)
            line = jnp.where(last, tag, windows[tap][slot : slot + 1] * keep)
            scr[pl.ds(peer * padded + tap * capacity + rank, 1), :] = line
    for peer in range(peers):
        for chunk in range(chunks):
            block = scr[peer * padded : (peer + 1) * padded, chunk * LANES : (chunk + 1) * LANES]
            out_ref[peer, chunk * padded : (chunk + 1) * padded, :] = block.astype(BF16)


def window_packets(plan, mask, inner, outer, peers):
    taps, slots = inner.shape[:2]
    width = inner.shape[2] + outer.shape[2]
    whole = pl.BlockSpec(memory_space=pltpu.VMEM)
    scalar = pl.BlockSpec(memory_space=pltpu.SMEM)
    total = width + LANES - width % LANES
    padded = pl.cdiv(taps * most_per_pair(slots, peers), 16) * 16
    return pl.pallas_call(
        window_kernel,
        in_specs=[scalar, scalar, whole, whole],
        out_shape=jax.ShapeDtypeStruct((peers, padded * (total // LANES), LANES), BF16),
        scratch_shapes=[pltpu.VMEM((peers * padded, total), F32)],
        name="window_packets",
    )(plan, mask, inner, outer)


def settle_kernel(inner_own_ref, outer_own_ref, *refs):
    got_refs, inner_ref, outer_ref = refs[:-2], refs[-2], refs[-1]
    peers, lines = len(got_refs), got_refs[0].shape[0]
    taps, slots, inner_local = inner_ref.shape
    width = inner_local + outer_ref.shape[2]
    chunks = width // LANES + 1
    padded = pl.cdiv(taps * most_per_pair(slots, peers), 16) * 16
    start = lines - chunks * padded
    rows = peers * padded
    parts = []
    for chunk in range(chunks):
        at = start + chunk * padded
        part = [got_ref[at : at + padded, :] for got_ref in got_refs]
        parts.append(jnp.concatenate(part, axis=0).astype(F32))
    tags = parts[-1][:, LANES - 1 :]
    lane = lax.broadcasted_iota(jnp.int32, (rows, LANES), 1).astype(F32)
    pick = (tags == lane).astype(BF16)
    moved = dot(pick, jnp.concatenate(parts, axis=1).astype(BF16), ((0,), (0,)))
    top = lax.broadcasted_iota(jnp.int32, (SLOT_PAD, 1), 0) == 0
    for tap in range(taps):
        block = moved[tap * SLOT_PAD : (tap + 1) * SLOT_PAD]
        own = inner_own_ref[tap : tap + 1, :].astype(F32)
        inner_ref[tap] = jnp.where(top, own, block[:, :inner_local]).astype(BF16)[:slots]
        own = outer_own_ref[tap : tap + 1, :].astype(F32)
        outer_ref[tap] = jnp.where(top, own, block[:, inner_local:width]).astype(BF16)[:slots]


def settle(got, inner_own, outer_own, slots):
    taps, inner_local = inner_own.shape
    whole = pl.BlockSpec(memory_space=pltpu.VMEM)
    return pl.pallas_call(
        settle_kernel,
        in_specs=[whole] * (2 + len(got)),
        out_shape=[
            jax.ShapeDtypeStruct((taps, slots, inner_local), BF16),
            jax.ShapeDtypeStruct((taps, slots, outer_own.shape[1]), BF16),
        ],
        name="settle",
    )(inner_own, outer_own, *got)


def pack_lead_kernel(own_ref, mask_ref, state_ref, out_ref):
    for slot in range(out_ref.shape[0]):
        keep = mask_ref[slot].astype(F32)
        out_ref[slot] = (state_ref[slot, 0] * keep).astype(BF16)


def pack_lead(own, mask, states, hop):
    slots, peers, piece, width = states.shape

    def from_peer(t, own, mask):
        return 0, lax.rem(own[0] + hop, peers), 0, 0

    return pl.pallas_call(
        pack_lead_kernel,
        grid_spec=pltpu.PrefetchScalarGridSpec(
            num_scalar_prefetch=2,
            grid=(1,),
            in_specs=[pl.BlockSpec((slots, 1, piece, width), from_peer)],
            out_specs=pl.BlockSpec((slots, piece, width), lambda t, own, mask: (0, 0, 0)),
        ),
        out_shape=jax.ShapeDtypeStruct((slots, piece, width), BF16),
        compiler_params=pltpu.CompilerParams(dimension_semantics=("arbitrary",)),
        name="pack_lead",
    )(own, mask, states)


def pack_kernel(hops, own_ref, mask_ref, state_ref, *out_refs):
    first_slot = pl.program_id(0) * PACK_TILE
    peers = state_ref.shape[1]
    for j in range(PACK_TILE):
        keep = mask_ref[jnp.minimum(first_slot + j, mask_ref.shape[0] - 1)].astype(F32)
        for hop, out_ref in zip(hops, out_refs):
            peer = lax.rem(own_ref[0] + hop, peers)
            out_ref[j] = (state_ref[j, peer] * keep).astype(BF16)


def pack(own, mask, states, hops):
    slots, peers, piece, width = states.shape
    return pl.pallas_call(
        functools.partial(pack_kernel, hops),
        grid=(pl.cdiv(slots, PACK_TILE),),
        in_specs=[
            pl.BlockSpec(memory_space=pltpu.SMEM),
            pl.BlockSpec(memory_space=pltpu.SMEM),
            pl.BlockSpec((PACK_TILE, peers, piece, width), lambda t: (t, 0, 0, 0)),
        ],
        out_specs=[pl.BlockSpec((PACK_TILE, piece, width), lambda t: (t, 0, 0))] * len(hops),
        out_shape=[jax.ShapeDtypeStruct((slots, piece, width), BF16)] * len(hops),
        compiler_params=pltpu.CompilerParams(dimension_semantics=("arbitrary",)),
        name="pack",
    )(own, mask, states)


def source_of(table_ref, target):
    code = table_ref[0, target]
    peer = lax.div(code, SLOT_PAD)
    return peer, code - peer * SLOT_PAD


def pick_first_kernel(own_ref, table_ref, packet_ref, *refs):
    peers = (len(refs) - 1) // 2
    in_refs, out_refs, sem = refs[:peers], refs[peers:-1], refs[-1]
    slots, piece, _ = in_refs[0].shape
    own_piece = pl.ds(0, piece)
    for to in range(peers):
        target = lax.rem(own_ref[0] + to, peers)
        peer, index = source_of(table_ref, target * slots)
        source = lax.rem(own_ref[0] - peer + peers, peers)
        for hop in range(peers):

            @pl.when(source == hop)
            def _():
                pltpu.make_async_copy(
                    in_refs[hop].at[index], out_refs[to].at[own_piece], sem.at[to]
                ).start()

    for to in range(peers):
        out_refs[to][piece:, :] = packet_ref[lax.rem(own_ref[0] + to, peers)]
    for to in range(peers):
        pltpu.make_async_copy(
            in_refs[0].at[0], out_refs[to].at[own_piece], sem.at[to]
        ).wait()


def pick_first(own, table, packets, pieces):
    _, piece, width = pieces[0].shape
    peers = len(pieces)
    scalar = pl.BlockSpec(memory_space=pltpu.SMEM)
    return pl.pallas_call(
        pick_first_kernel,
        in_specs=[scalar, scalar, pl.BlockSpec(memory_space=pltpu.VMEM)]
        + [pl.BlockSpec(memory_space=pl.ANY)] * peers,
        out_specs=[pl.BlockSpec(memory_space=pltpu.VMEM)] * peers,
        out_shape=[jax.ShapeDtypeStruct((piece + packets.shape[1], width), BF16)] * peers,
        scratch_shapes=[pltpu.SemaphoreType.DMA((peers,))],
        name="pick_first",
    )(own, table, packets, *pieces)


def gather_pieces(own_ref, refs, scr):
    peers = len(refs)
    for hop in range(peers):
        scr[lax.rem(own_ref[0] - hop + peers, peers)] = refs[hop][...]


def reorder_kernel(own_ref, table_ref, *refs):
    scr = refs[-1]
    peers, slots = scr.shape[:2]
    gather_pieces(own_ref, refs[:peers], scr)
    for hop in range(peers):
        base = lax.rem(own_ref[0] + hop, peers) * slots
        out_ref = refs[peers + hop]

        def move(slot, unused):
            peer, index = source_of(table_ref, base + slot)
            out_ref[slot - 1] = scr[peer, index]
            return unused

        lax.fori_loop(1, slots, move, 0)


def reorder_rest_kernel(own_ref, table_ref, *refs):
    out_ref, scr = refs[-2:]
    peers, slots = scr.shape[:2]
    gather_pieces(own_ref, refs[:peers], scr)
    for target in range(peers):

        def move(slot, unused):
            peer, index = source_of(table_ref, target * slots + slot)
            out_ref[target, slot - 1] = scr[peer, index]
            return unused

        lax.fori_loop(1, slots, move, 0)


def reorder(own, table, pieces, part):
    slots, piece, width = pieces[0].shape
    half = piece // 2
    peers = len(pieces)
    scalar = pl.BlockSpec(memory_space=pltpu.SMEM)
    if part == 0:
        one = (slots - 1, half, width)
        out_specs = [pl.BlockSpec(one, lambda t: (0, 0, 0))] * peers
        out_shape = [jax.ShapeDtypeStruct(one, BF16)] * peers
    else:
        all_rest = (peers, slots - 1, half, width)
        out_specs = pl.BlockSpec(all_rest, lambda t: (0, 0, 0, 0))
        out_shape = jax.ShapeDtypeStruct(all_rest, BF16)
    return pl.pallas_call(
        reorder_kernel if part == 0 else reorder_rest_kernel,
        grid=(1,),
        in_specs=[scalar, scalar]
        + [pl.BlockSpec((slots, half, width), lambda t: (0, part, 0))] * peers,
        out_specs=out_specs,
        out_shape=out_shape,
        scratch_shapes=[pltpu.VMEM((peers, slots, half, width), BF16)],
        name="reorder" if part == 0 else "reorder_rest",
    )(own, table, *pieces)


def unpack_kernel(own_ref, final_ref, *refs):
    piece_refs, out_ref = refs[:-1], refs[-1]
    step = pl.program_id(0)
    half = out_ref.shape[2]
    out_ref[0, 0] = final_ref[:half, :]
    for hop in range(len(piece_refs)):

        @pl.when(step == hop)
        def _():
            out_ref[1:, 0] = piece_refs[hop][...].astype(F32)


def unpack(own, final, pieces):
    others, half, width = pieces[0].shape
    peers = len(pieces)
    slots, piece = others + 1, 2 * half

    def from_peer(hop, own):
        return lax.rem(own[0] - hop + peers, peers)

    return pl.pallas_call(
        unpack_kernel,
        grid_spec=pltpu.PrefetchScalarGridSpec(
            num_scalar_prefetch=1,
            grid=(peers,),
            in_specs=[pl.BlockSpec((piece, width), lambda h, own: (from_peer(h, own), 0))]
            + [pl.BlockSpec((others, half, width), lambda h, own: (0, 0, 0))] * peers,
            out_specs=pl.BlockSpec(
                (slots, 1, half, width), lambda h, own: (0, from_peer(h, own), 0, 0)
            ),
        ),
        out_shape=jax.ShapeDtypeStruct((slots, peers, piece, width), F32),
        compiler_params=pltpu.CompilerParams(dimension_semantics=("arbitrary",)),
        name="unpack",
    )(own, final, *pieces)


def unpack_rest_kernel(final_ref, pieces_ref, states_ref, out_ref):
    peers, half = pieces_ref.shape[0], pieces_ref.shape[2]
    for p in range(peers):
        out_ref[0, p] = final_ref[(2 * p + 1) * half : (2 * p + 2) * half, :]
        out_ref[1:, p] = pieces_ref[p].astype(F32)


def unpack_rest(final, pieces, states):
    slots, peers, piece, width = states.shape
    half = piece // 2
    return pl.pallas_call(
        unpack_rest_kernel,
        grid=(peers // PEER_TILE,),
        in_specs=[
            pl.BlockSpec((PEER_TILE * piece, width), lambda p: (p, 0)),
            pl.BlockSpec((PEER_TILE, slots - 1, half, width), lambda p: (p, 0, 0, 0)),
            pl.BlockSpec(memory_space=pl.ANY),
        ],
        out_specs=pl.BlockSpec((slots, PEER_TILE, half, width), lambda p: (0, p, 1, 0)),
        out_shape=jax.ShapeDtypeStruct(states.shape, F32),
        input_output_aliases={2: 0},
        compiler_params=pltpu.CompilerParams(dimension_semantics=("arbitrary",)),
        name="unpack_rest",
    )(final, pieces, states)


def combine_kernel(place_ref, decay_ref, *refs):
    count = decay_ref.shape[0]
    end_scr, enter_scr, first_scr = refs[-3:]
    refs = refs[:-1]
    final_ref = refs[-3]
    entering_refs = refs[-3 - count : -3]
    inputs = refs[: -3 - count]
    end_refs, first_refs = inputs[:count], inputs[count:]
    chain = place_ref[0]
    peers = len(first_refs)
    piece = first_refs[0].shape[0]
    for hop in range(peers):
        peer = lax.rem(place_ref[1] - hop + peers, peers)
        at = pl.multiple_of(peer * piece, 16)
        first_scr[pl.ds(at, piece), :] = first_refs[hop][...]
    for hop in range(count):
        end_scr[lax.rem(chain - hop + count, count)] = end_refs[hop][...]
    state = first_scr[...].astype(F32).T
    for k in range(count):
        enter_scr[k] = state.astype(BF16)
        state = state * decay_ref[k : k + 1, :] + end_scr[k].astype(F32)
    for hop in range(count):
        entering_refs[hop][...] = enter_scr[lax.rem(chain + hop, count)]
    final_ref[...] = state.T


def combine(place, decay, ends, first):
    count = len(ends)
    whole = pl.BlockSpec(memory_space=pltpu.VMEM)
    rows, columns = ends[0].shape
    peers = len(first)
    outs = pl.pallas_call(
        combine_kernel,
        grid=(1,),
        in_specs=[
            pl.BlockSpec(memory_space=pltpu.SMEM),
            pl.BlockSpec(decay.shape, lambda t: (0, 0)),
        ]
        + [pl.BlockSpec((rows, columns), lambda t: (0, 0))] * count
        + [pl.BlockSpec((columns // peers, rows), lambda t: (0, 0))] * peers,
        out_specs=[pl.BlockSpec((rows, columns), lambda t: (0, 0))] * count
        + [pl.BlockSpec((columns, rows), lambda t: (0, 0))],
        out_shape=[jax.ShapeDtypeStruct((rows, columns), BF16)] * count
        + [jax.ShapeDtypeStruct((columns, rows), F32)],
        scratch_shapes=[
            pltpu.VMEM((count, rows, columns), BF16),
            pltpu.VMEM((count, rows, columns), BF16),
            pltpu.VMEM((columns, rows), BF16),
        ],
        name="combine",
    )(place, decay, *ends, *first)
    return outs[:count], outs[count]


def share_kernel(
    slot_count,
    place_ref,
    every_ref,
    end_ref,
    kept_ref,
    kept_next_ref,
    state_end_ref,
    state_kept_ref,
    state_next_ref,
    raw_ref,
    bias_ref,
    rate_ref,
    out_ref,
    step_ref,
    table_ref,
):
    taps = out_ref.shape[0]
    inner = end_ref.shape[1]
    outer = state_end_ref.shape[1]
    channels = inner + outer
    peers, packet, _ = every_ref.shape
    slots = float(slot_count)
    chunks = (packet - 2) // taps
    width = chunks * LANES
    everything = [every_ref[p].astype(F32) for p in range(peers)]
    firsts = everything[0]
    for part in everything[1:]:
        firsts = firsts + part
    at = chunks * taps
    target = jnp.concatenate([part[at : at + 1] for part in everything], axis=0) * slots
    target = target + jnp.concatenate([part[at + 1 : at + 2] for part in everything], axis=0)
    columns = table_ref.shape[1]
    lane = lax.broadcasted_iota(jnp.int32, (peers, columns), 1).astype(F32)
    code = lax.broadcasted_iota(jnp.int32, (peers, columns), 0).astype(F32) * SLOT_PAD
    found = jnp.zeros((peers, columns), F32)
    for slot in range(slot_count):
        found = found + jnp.where(target[:, slot : slot + 1] == lane, code + slot, 0.0)
    found = jnp.sum(found, axis=0, keepdims=True)
    table_ref[...] = jnp.broadcast_to(found, table_ref.shape).astype(jnp.int32)
    low_block, high_block, start, length = (
        place_ref[0],
        place_ref[1],
        place_ref[2],
        place_ref[3],
    )
    out_ref[:, :inner] = end_ref[16 - taps :, :]
    out_ref[:, inner:channels] = state_end_ref[16 - taps :, :]
    here = lax.broadcasted_iota(jnp.int32, (16, 1), 0)
    wanted = length - taps - start

    def kept_rows(low_ref, high_ref):
        low = low_ref[...].astype(F32)
        high = high_ref[...].astype(F32)
        found = []
        for i in range(taps):
            in_low = (low_block * 16 + here) == (wanted + i)
            in_high = ((high_block * 16 + here) == (wanted + i)) & (high_block > low_block)
            picked = jnp.where(in_low, low, 0.0) + jnp.where(in_high, high, 0.0)
            found.append(jnp.sum(picked, axis=0, keepdims=True))
        return jnp.concatenate(found, axis=0).astype(BF16)

    out_ref[:, channels : channels + inner] = kept_rows(kept_ref, kept_next_ref)
    out_ref[:, channels + inner : 2 * channels] = kept_rows(state_kept_ref, state_next_ref)
    for chunk in range(chunks):
        at = 2 * channels + chunk * LANES
        lines = firsts[chunk * taps : (chunk + 1) * taps]
        out_ref[:, at : at + LANES] = lines.astype(BF16)
    count = step_ref.shape[0]
    heads = raw_ref.shape[1]
    positions = start + lax.broadcasted_iota(jnp.int32, (count, heads), 0)
    raw = raw_ref[...].astype(F32) + bias_ref[...]
    step = jnp.maximum(raw, 0.0) + jnp.log1p(jnp.exp(-jnp.abs(raw)))
    step = jnp.where(positions < length, step, 0.0)
    step = jnp.concatenate([step, jnp.zeros((count, LANES - heads), F32)], axis=1)
    step_ref[...] = step
    total = jnp.sum(step * rate_ref[...], axis=0, keepdims=True)
    high = total.astype(BF16).astype(F32)
    middle = (total - high).astype(BF16).astype(F32)
    rest = total - high - middle
    parts = jnp.concatenate([high, middle, rest], axis=0)
    out_ref[:, 2 * channels + width :] = parts.astype(BF16)


def share(place, slots, every, rows, state_rows, step_raw, step_bias, rate):
    peers, packet, _ = every.shape
    taps = KERNEL - 1
    width = (packet - 2) // taps * LANES
    length, inner = rows.shape
    outer = state_rows.shape[1]
    heads = step_raw.shape[1]
    last = length // 16 - 1
    total = 2 * (inner + outer) + width + LANES
    lanes = pl.cdiv(peers * slots, LANES) * LANES
    return pl.pallas_call(
        functools.partial(share_kernel, slots),
        grid_spec=pltpu.PrefetchScalarGridSpec(
            num_scalar_prefetch=1,
            grid=(1,),
            in_specs=[
                pl.BlockSpec(every.shape, lambda t, c: (0, 0, 0)),
                pl.BlockSpec((16, inner), lambda t, c: (last, 0)),
                pl.BlockSpec((16, inner), lambda t, c: (c[0], 0)),
                pl.BlockSpec((16, inner), lambda t, c: (c[1], 0)),
                pl.BlockSpec((16, outer), lambda t, c: (last, 0)),
                pl.BlockSpec((16, outer), lambda t, c: (c[0], 0)),
                pl.BlockSpec((16, outer), lambda t, c: (c[1], 0)),
                pl.BlockSpec((length, heads), lambda t, c: (0, 0)),
                pl.BlockSpec((1, heads), lambda t, c: (0, 0)),
                pl.BlockSpec((1, LANES), lambda t, c: (0, 0)),
            ],
            out_specs=[
                pl.BlockSpec((taps, total), lambda t, c: (0, 0)),
                pl.BlockSpec((length, LANES), lambda t, c: (0, 0)),
                pl.BlockSpec((8, lanes), lambda t, c: (0, 0)),
            ],
        ),
        out_shape=[
            jax.ShapeDtypeStruct((taps, total), BF16),
            jax.ShapeDtypeStruct((length, LANES), F32),
            jax.ShapeDtypeStruct((8, lanes), jnp.int32),
        ],
        name="share",
    )(
        place,
        every,
        rows,
        rows,
        rows,
        state_rows,
        state_rows,
        state_rows,
        step_raw,
        step_bias,
        rate,
    )


def tail_kernel(
    chain_ref, shared_ref, tail_ref, inner_ref, outer_ref, decay_ref
):
    chain = chain_ref[0]
    count, taps = shared_ref.shape[:2]
    inner_local, outer_local = inner_ref.shape[1], outer_ref.shape[1]
    channels = tail_ref.shape[1]
    inner = count * inner_local
    at = 2 * channels
    window = jnp.concatenate(
        [shared_ref[s, :, at : at + inner_local] for s in range(count)]
        + [
            shared_ref[s, :, at + inner_local : at + inner_local + outer_local]
            for s in range(count)
        ],
        axis=1,
    ).astype(F32)
    earlier = shared_ref[jnp.maximum(chain - 1, 0), :, :channels].astype(F32)
    tail = jnp.where(chain == 0, window, earlier)
    tail_ref[...] = jnp.concatenate([jnp.zeros((8 - taps, channels), F32), tail], axis=0)
    kept = shared_ref[0, :, channels:at].astype(F32)
    for s in range(1, count):
        kept = kept + shared_ref[s, :, channels:at].astype(F32)
    own_inner = jnp.zeros((taps, inner_local), F32)
    own_outer = jnp.zeros((taps, outer_local), F32)
    for s in range(count):
        mine = chain == s
        inner_at, outer_at = s * inner_local, inner + s * outer_local
        own_inner = jnp.where(mine, kept[:, inner_at : inner_at + inner_local], own_inner)
        own_outer = jnp.where(mine, kept[:, outer_at : outer_at + outer_local], own_outer)
    inner_ref[...] = own_inner.astype(BF16)
    outer_ref[...] = own_outer.astype(BF16)
    logs = []
    for s in range(count):
        parts = shared_ref[s, :, shared_ref.shape[2] - LANES :].astype(F32)
        logs.append(jnp.sum(parts, axis=0, keepdims=True))
    logs = jnp.concatenate(logs + [jnp.zeros((8 - count, LANES), F32)] * (count < 8), axis=0)
    columns = decay_ref.shape[1]
    head = lax.broadcasted_iota(jnp.int32, (LANES, columns), 0)
    lane = lax.broadcasted_iota(jnp.int32, (LANES, columns), 1)
    local_heads = columns // HEAD_DIM
    pick = (head == chain * local_heads + lane // HEAD_DIM).astype(F32)
    spread = dot(logs, pick, precision=lax.Precision.HIGHEST)
    decay_ref[...] = jnp.exp2(spread[:count])


def tails(chain, shared, channels, inner_local, outer_local, columns):
    count, taps = shared.shape[:2]
    whole = pl.BlockSpec(memory_space=pltpu.VMEM)
    return pl.pallas_call(
        tail_kernel,
        in_specs=[pl.BlockSpec(memory_space=pltpu.SMEM), whole],
        out_shape=[
            jax.ShapeDtypeStruct((8, channels), F32),
            jax.ShapeDtypeStruct((taps, inner_local), BF16),
            jax.ShapeDtypeStruct((taps, outer_local), BF16),
            jax.ShapeDtypeStruct((count, columns), F32),
        ],
        name="tails",
    )(chain, shared)


def exchange(value, axis):
    return lax.all_to_all(value, axis, split_axis=0, concat_axis=0, tiled=True)


def hop_order(count):
    return sorted(range(1, count), key=lambda hop: abs(2 * hop - count))


def send(value, axis, hop):
    count = lax.axis_size(axis)
    pairs = [(source, (source + hop) % count) for source in range(count)]
    return lax.ppermute(value, axis, pairs)


def rotate(values, axis):
    got = [values[hop] for hop in range(lax.axis_size(axis))]
    for hop in hop_order(len(got)):
        got[hop] = send(got[hop], axis, hop)
    return got


def device_body(
    pool_states,
    inner_window,
    state_window,
    move_plan,
    active_mask,
    inputs_inner,
    inputs_state,
    gate_rows,
    step_raw,
    lengths,
    conv_weight,
    conv_bias,
    step_bias,
    decay_log,
    skip_weight,
    norm_weight,
):
    peers = lax.axis_size("req")
    own_peer = lax.axis_index("req").astype(jnp.int32)
    chain_size = lax.axis_size("seq")
    chain_index = lax.axis_index("seq").astype(jnp.int32)
    slots, local_heads = pool_states.shape[:2]
    columns = local_heads * HEAD_DIM
    piece = columns // peers
    taps = KERNEL - 1
    inner_local = inner_window.shape[2]
    outer_local = state_window.shape[2]

    own = own_peer[None]
    pool_pieces = pool_states.reshape(slots, peers, piece, STATE_DIM)
    lead, *others = hop_order(peers)
    spread = [None] * peers
    lead_pieces = pack_lead(own, active_mask, pool_pieces, lead)
    spread[lead] = send(lead_pieces, "req", lead)
    plan = move_plan.T
    inner_taps = inner_window.transpose(1, 0, 2)
    outer_taps = state_window.transpose(1, 0, 2)
    packed = mark(plan, active_mask, inner_taps, outer_taps, peers)
    packets = window_packets(plan, active_mask, inner_taps, outer_taps, peers)
    every = exchange(packed, "req")
    others = [0] + others
    for hop, pieces in zip(others, pack(own, active_mask, pool_pieces, others)):
        spread[hop] = pieces if hop == 0 else send(pieces, "req", hop)

    rows = inputs_inner[0]
    state_rows = inputs_state[0]
    local_length, inner_dim = rows.shape
    channels = inner_dim + state_rows.shape[1]
    start = chain_index * local_length
    length = lengths[0]
    last_tile = local_length // 16 - 1
    low_block = jnp.clip((length - taps - start) // 16, 0, last_tile)
    high_block = jnp.minimum(low_block + 1, last_tile)
    heads = decay_log.shape[0]
    rate = jnp.pad(-LOG2E * jnp.exp(decay_log), (0, LANES - heads))[None]
    payload, step, table = share(
        jnp.stack([low_block, high_block, start, length]),
        slots,
        every,
        rows,
        state_rows,
        step_raw[0],
        step_bias[None],
        rate,
    )
    shared = lax.all_gather(payload, "seq", axis=0)
    chain = chain_index[None]
    tail, kept_inner, kept_outer, own_decay = tails(
        chain, shared, channels, inner_local, outer_local, columns
    )

    part, local_end, read_rows, decay = block_parts(
        chain,
        tail,
        rows,
        state_rows,
        step,
        rate,
        conv_weight,
        conv_bias[None],
        jnp.repeat(skip_weight, HEAD_DIM)[None],
        chain_size,
    )
    own_ends = rotate(local_end, "seq")

    first = rotate(pick_first(own, table, packets, spread), "req")
    moved_a = rotate(reorder(own, table, spread, 0), "req")
    moved_b = exchange(reorder(own, table, spread, 1), "req")
    entering, final = combine(
        jnp.concatenate([chain, own]), own_decay, own_ends, first
    )
    new_inner, new_outer = settle(first, kept_inner, kept_outer, slots)
    incoming = rotate(entering, "seq")
    mixer_out = finish(
        jnp.stack([start, length, chain_index]),
        part,
        gate_rows[0],
        read_rows,
        decay,
        norm_weight[None],
        incoming,
    )
    states = unpack(own, final, moved_a)
    new_states = unpack_rest(final, moved_b, states).reshape(pool_states.shape)

    return (
        new_states,
        new_inner.transpose(1, 0, 2),
        new_outer.transpose(1, 0, 2),
        mixer_out[None],
    )


def solution(mesh):
    return jax.shard_map(
        device_body,
        mesh=mesh,
        in_specs=(
            P("req", "seq", None, None),
            P("req", None, "seq"),
            P("req", None, "seq"),
            P("req", None),
            P("req"),
            P("req", "seq", None),
            P("req", "seq", None),
            P("req", "seq", None),
            P("req", "seq", None),
            P("req"),
            P(),
            P(),
            P(),
            P(),
            P(),
            P(),
        ),
        out_specs=(
            P("req", "seq", None, None),
            P("req", None, "seq"),
            P("req", None, "seq"),
            P("req", "seq", None),
        ),
        check_vma=False,
    )
```
